32 devices in a mesh: gx: 4 (over x, core), gy: 4 (over z), gz: 2 (over y).
Axes of the slice: x: 2, y: 2, z: 4, core: 2. Of those that a mesh axis runs over, the one named last changes fastest.
Arguments:
- density: float32 [16, 128, 256], P('gx', 'gy', 'gz'), may hold values from 0.5 to 2
- velocity: float32 [3, 16, 128, 256], P(None, 'gx', 'gy', 'gz'), may hold values from -2.5 to 2.5
- pressure: float32 [16, 128, 256], P('gx', 'gy', 'gz'), may hold values from 0.5 to 2
Outputs:
- section_state: float32 [5, 16, 128, 256], P(None, 'gx', 'gy', 'gz')
The draws below stay inside these ranges and needn't reach their ends.
All inputs are finite; a program needn't handle non-finite values.
Results may differ from the reference program's by a relative error of at most 0.0003.
Values sent between devices are 32-bit elements; how exact they have to be, the bound alone decides.
No kernel may reach another device: no remote copies, remote signals or barrier semaphores. Data moves between devices by JAX's collectives and lax.ppermute only.
A program may use at most 64 MiB of HBM per device.

```python
import math
import jax
import jax.numpy as jnp
from jax import lax

CX = 4
NX = 16
NY = 128
NZ = 256


def draw_velocity(key, part):
    growth = 1.0 + 2.0 * jnp.arange(NX, dtype=jnp.float32) / NX
    growth = growth[None, :, None, None]
    sample = jnp.clip(jax.random.normal(key, (3, NX, NY, NZ), jnp.float32), -2.5, 2.5)
    return 0.3 * growth * sample


def shard_levels(stream_key, shape, split, least, high):
    loudness = 1.0
    for position, shards_of in split:
        steps = jax.random.uniform(jax.random.fold_in(jax.random.fold_in(stream_key, 6), position), (shards_of,), jnp.float32, least / len(split), high / len(split))
        loudness = loudness * jnp.repeat(jnp.exp(steps), shape[position] // shards_of).reshape((-1,) + (1,) * (len(shape) - 1 - position))
    return loudness


def setup_inputs(seed: int = 0) -> dict:
    keys = jax.random.split(jax.random.key(seed), 4)
    return {
        "density": jnp.clip(jnp.exp(math.log(2.0) - 1.3862944 * jax.random.uniform(keys[0], (NX, NY, NZ), jnp.float32) ** shard_levels(keys[0], (NX, NY, NZ), ((0, 4), (1, 4), (2, 2)), -0.2, 0.2)), 0.5, 2.0),
        "velocity": draw_velocity(jax.random.fold_in(keys[3], 71), 0),
        "pressure": jnp.clip(jnp.exp(math.log(2.0) - 1.3862944 * jax.random.uniform(keys[2], (NX, NY, NZ), jnp.float32) ** shard_levels(keys[2], (NX, NY, NZ), ((0, 4), (1, 4), (2, 2)), -0.2, 0.2)), 0.5, 2.0),
    }


gamma_gas = 1.4
weno_eps = 1e-06
cfl_number = 0.4

def conserved(density, velocity, pressure):
    momenta = density[None] * velocity
    kinetic = 0.5 * density * lax.optimization_barrier(jnp.sum(velocity * velocity, axis=0))
    energy = pressure / (gamma_gas - 1.0) + kinetic
    return jnp.concatenate([density[None], momenta, energy[None]], axis=0)

def wave_speed(density, velocity, pressure):
    sound = jnp.sqrt(gamma_gas * pressure / density)
    return jnp.max(lax.optimization_barrier(jnp.sum(jnp.abs(velocity), axis=0)) + 3.0 * sound)

def combine(coeffs, arrays):
    total = None
    for coeff, array in zip(coeffs, arrays):
        if isinstance(coeff, float) and coeff == 0.0:
            continue
        term = coeff * array
        total = term if total is None else total + term
    return total

def weno_face(values):
    first, second, third, fourth, fifth = values
    cand_left = (2.0 * first - 7.0 * second + 11.0 * third) / 6.0
    cand_middle = (-second + 5.0 * third + 2.0 * fourth) / 6.0
    cand_right = (2.0 * third + 5.0 * fourth - fifth) / 6.0
    smooth_left = 13.0 / 12.0 * (first - 2.0 * second + third) ** 2 + 0.25 * (first - 4.0 * second + 3.0 * third) ** 2
    smooth_middle = 13.0 / 12.0 * (second - 2.0 * third + fourth) ** 2 + 0.25 * (second - fourth) ** 2
    smooth_right = 13.0 / 12.0 * (third - 2.0 * fourth + fifth) ** 2 + 0.25 * (3.0 * third - 4.0 * fourth + fifth) ** 2
    weight_left = 0.1 / (weno_eps + smooth_left) ** 2
    weight_middle = 0.6 / (weno_eps + smooth_middle) ** 2
    weight_right = 0.3 / (weno_eps + smooth_right) ** 2
    return (weight_left * cand_left + weight_middle * cand_middle + weight_right * cand_right) / (weight_left + weight_middle + weight_right)

def direction_flux(padded, field_dim, normal_comp):
    cells = padded.shape[field_dim + 1] - 6
    faces = cells + 1
    density = padded[0]
    energy = padded[4]
    velocity = [padded[1 + member] / density for member in range(3)]
    speed_sq = velocity[0] * velocity[0] + velocity[1] * velocity[1] + velocity[2] * velocity[2]
    pressure = (gamma_gas - 1.0) * (energy - 0.5 * density * speed_sq)
    sound_sq = gamma_gas * pressure / density
    sound = jnp.sqrt(sound_sq)
    enthalpy = (energy + pressure) / density
    normal_vel = velocity[normal_comp]
    others = [member for member in range(3) if member != normal_comp]
    order = [0, 1 + normal_comp, 1 + others[0], 1 + others[1], 4]
    state_perm = [padded[member] for member in order]
    flux_perm = [density * normal_vel, padded[1 + normal_comp] * normal_vel + pressure, padded[1 + others[0]] * normal_vel, padded[1 + others[1]] * normal_vel, (energy + pressure) * normal_vel]
    signal = jnp.abs(normal_vel) + sound

    def window(array, offset):
        return lax.slice_in_dim(array, offset, offset + faces, axis=field_dim)
    root_left = jnp.sqrt(window(density, 2))
    root_right = jnp.sqrt(window(density, 3))
    share_left = root_left / (root_left + root_right)
    share_right = root_right / (root_left + root_right)
    roe_vel = [share_left * window(member, 2) + share_right * window(member, 3) for member in velocity]
    roe_enth = share_left * window(enthalpy, 2) + share_right * window(enthalpy, 3)
    jump_sq = sum(((window(member, 3) - window(member, 2)) ** 2 for member in velocity))
    roe_sound_sq = share_left * window(sound_sq, 2) + share_right * window(sound_sq, 3) + 0.5 * (gamma_gas - 1.0) * share_left * share_right * jump_sq
    roe_sound = jnp.sqrt(roe_sound_sq)
    normal_roe = roe_vel[normal_comp]
    tang_first = roe_vel[others[0]]
    tang_second = roe_vel[others[1]]
    roe_qsq = normal_roe * normal_roe + tang_first * tang_first + tang_second * tang_second
    b_one = (gamma_gas - 1.0) / roe_sound_sq
    b_two = 0.5 * b_one * roe_qsq
    inv_sound = 1.0 / roe_sound
    left_rows = [[0.5 * (b_two + normal_roe * inv_sound), -0.5 * (b_one * normal_roe + inv_sound), -0.5 * b_one * tang_first, -0.5 * b_one * tang_second, 0.5 * b_one], [1.0 - b_two, b_one * normal_roe, b_one * tang_first, b_one * tang_second, -b_one], [-tang_first, 0.0, 1.0, 0.0, 0.0], [-tang_second, 0.0, 0.0, 1.0, 0.0], [0.5 * (b_two - normal_roe * inv_sound), -0.5 * (b_one * normal_roe - inv_sound), -0.5 * b_one * tang_first, -0.5 * b_one * tang_second, 0.5 * b_one]]
    right_rows = [[1.0, 1.0, 0.0, 0.0, 1.0], [normal_roe - roe_sound, normal_roe, 0.0, 0.0, normal_roe + roe_sound], [tang_first, tang_first, 1.0, 0.0, tang_first], [tang_second, tang_second, 0.0, 1.0, tang_second], [roe_enth - normal_roe * roe_sound, 0.5 * roe_qsq, tang_first, tang_second, roe_enth + normal_roe * roe_sound]]
    alpha = window(signal, 0)
    for offset in range(1, 6):
        alpha = jnp.maximum(alpha, window(signal, offset))
    plus_vals = [[None] * 6 for member in range(5)]
    minus_vals = [[None] * 6 for member in range(5)]
    for offset in range(6):
        state_here = [window(member, offset) for member in state_perm]
        flux_here = [window(member, offset) for member in flux_perm]
        for charac in range(5):
            char_state = combine(left_rows[charac], state_here)
            char_flux = combine(left_rows[charac], flux_here)
            plus_vals[charac][offset] = 0.5 * (char_flux + alpha * char_state)
            minus_vals[charac][offset] = 0.5 * (char_flux - alpha * char_state)
    hats = []
    for charac in range(5):
        upwind = weno_face(plus_vals[charac][0:5])
        downwind = weno_face([minus_vals[charac][5], minus_vals[charac][4], minus_vals[charac][3], minus_vals[charac][2], minus_vals[charac][1]])
        hats.append(upwind + downwind)
    face_flux = [None] * 5
    for member in range(5):
        face_flux[order[member]] = combine(right_rows[member], hats)
    result = [lax.slice_in_dim(member, 1, faces, axis=field_dim) - lax.slice_in_dim(member, 0, faces - 1, axis=field_dim) for member in face_flux]
    return jnp.stack(result, axis=0)

def reference(density, velocity, pressure):
    state = conserved(density, velocity, pressure)
    step = cfl_number / wave_speed(density, velocity, pressure)
    padded = jnp.pad(state, ((0, 0), (3, 3), (3, 3), (3, 3)), mode='wrap')

    def slab_update(start):
        piece = lax.dynamic_slice_in_dim(padded, start, CX + 6, axis=1)
        total = direction_flux(piece[:, :, 3:-3, 3:-3], 0, 0)
        total = total + direction_flux(piece[:, 3:-3, :, 3:-3], 1, 1)
        total = total + direction_flux(piece[:, 3:-3, 3:-3, :], 2, 2)
        return total
    starts = jnp.arange(NX // CX, dtype=jnp.int32) * CX
    slabs = lax.map(slab_update, starts)
    total = jnp.moveaxis(slabs, 0, 1).reshape(5, NX, NY, NZ)
    return state - step * total
```

```python
import functools
import math

import jax
import jax.numpy as jnp
from jax import lax
from jax.experimental import pallas as pl
from jax.experimental.pallas import tpu as pltpu
from jax.sharding import PartitionSpec as P

gamma_gas = 1.4
weno_eps = 1e-06
cfl_number = 0.4
f32 = jnp.float32

KX = math.sqrt(13.0 / 12.0)
KT = 0.5 / KX
KB = 1.0 / (6.0 * KX)
VMEM_LIMIT = 24 * 1024 * 1024


def rup(n, m):
    return (n + m - 1) // m * m


def cell_values(prim, tile, comps):
    rho, p = prim[0], prim[4]
    un, ut, us = (prim[1 + c] for c in comps)
    inv = 1.0 / rho
    mn, mt, ms = rho * un, rho * ut, rho * us
    mnun = mn * un
    energy = 2.5 * p + 0.5 * (mnun + mt * ut + ms * us)
    total = energy + p
    sound = jnp.sqrt(gamma_gas * p * inv)
    state = (rho, mn, mt, ms, energy)
    flux = (mn, mnun + p, mt * un, ms * un, total * un)
    return state, flux, total * inv, jnp.sqrt(rho), jnp.abs(un) + sound


def weno_excess(mid, xa, xb, xc, sign, eps):
    tau_a = xa - xb
    tau_c = xb - xc
    if sign > 0:
        mid_a = mid + KT * tau_a
        mid_c = mid + KT * tau_c
    else:
        mid_a = mid - KT * tau_a
        mid_c = mid - KT * tau_c
    sm_a = mid_a * mid_a + (xa * xa + eps)
    sm_b = mid * mid + (xb * xb + eps)
    sm_c = mid_c * mid_c + (xc * xc + eps)
    ga = 3.0 * (sm_a * sm_a)
    gb = sm_b * sm_b
    gc = sm_c * sm_c
    gc = gc + gc
    num = gb * (tau_a * gc + tau_c * ga)
    den = gb * gc + (ga + ga) * (gb + gc)
    return num / den


def characteristic(v, un, ut, us, qh, b1, ic):
    t = (qh * v[0] - un * v[1]) - (ut * v[2] + us * v[3]) + v[4]
    a = b1 * t
    n = (un * v[0] - v[1]) * ic
    return (a + n, v[0] - a, v[2] - ut * v[0], v[3] - us * v[0], a - n)


def face_values(get_prim, get_aux, get_cx, comps):
    rl, rr = get_aux(1, 2), get_aux(1, 3)
    share = rr / (rl + rr)

    def roe(left, right):
        return left + share * (right - left)

    un, ut, us = (roe(get_prim(1 + c, 2), get_prim(1 + c, 3)) for c in comps)
    enth = roe(get_aux(0, 2), get_aux(0, 3))
    qh = 0.5 * (un * un + ut * ut + us * us)
    c2 = (gamma_gas - 1.0) * (enth - qh)
    ic = lax.rsqrt(c2)
    c = c2 * ic
    b1 = (gamma_gas - 1.0) * (ic * ic)
    alpha = jnp.maximum(jnp.maximum(get_aux(2, 0), get_aux(2, 2)), get_aux(2, 4))

    cu2 = [alpha * get_cx(m, 2) for m in range(5)]
    cu3 = [alpha * get_cx(m, 3) for m in range(5)]
    args = (un, ut, us, qh, b1, ic)
    mid_p = characteristic([get_cx(5 + m, 2) + cu2[m] for m in range(5)], *args)
    mid_m = characteristic([get_cx(5 + m, 3) - cu3[m] for m in range(5)], *args)
    xu = {o: [alpha * get_cx(10 + m, o) for m in range(5)] for o in range(1, 5)}
    xp = {}
    xm = {}
    for o in (1, 2, 3, 4):
        xf = [get_cx(15 + m, o) for m in range(5)]
        if o <= 3:
            xp[o] = characteristic([xf[m] + xu[o][m] for m in range(5)], *args)
        if o >= 2:
            xm[o] = characteristic([xf[m] - xu[o][m] for m in range(5)], *args)
    g = []
    for m in range(5):
        eps = 4.0 * weno_eps if m in (0, 4) else weno_eps
        up = weno_excess(mid_p[m], xp[1][m], xp[2][m], xp[3][m], 1, eps)
        down = weno_excess(mid_m[m], xm[4][m], xm[3][m], xm[2][m], -1, eps)
        g.append(up + down)
    h2, h3, h4 = (g[m] + g[m] for m in (1, 2, 3))
    h15 = g[0] + g[4]
    dh = c * (g[4] - g[0])
    rr = h15 + h2
    upd = (
        rr,
        un * rr + dh,
        ut * rr + h3,
        us * rr + h4,
        enth * h15 + un * dh + qh * h2 + ut * h3 + us * h4,
    )
    return [
        (get_cx(20 + m, 2) + get_cx(20 + m, 3)) + (xu[3][m] - xu[2][m]) + upd[m] for m in range(5)
    ]


def sweep(prim, uf, aux, cx, flux, store, s, cell_tiles, pair_tiles, diff_tiles, face_tiles, out_tiles, comps):
    order = (0, 1 + comps[0], 1 + comps[1], 1 + comps[2], 4)

    def rows(i, offset=0):
        return pl.ds(pl.multiple_of(i * 8, 8) + offset, 8)

    @pl.loop(0, cell_tiles)
    def _(i):
        here = rows(i)
        state, fl, enth, root, sig = cell_values([prim[k, here, :] for k in range(5)], i, comps)
        for m in range(5):
            uf[m, here, :] = state[m]
            uf[5 + m, here, :] = fl[m]
        aux[0, here, :] = enth
        aux[1, here, :] = root
        aux[3, here, :] = sig

    @pl.loop(0, diff_tiles)
    def _(i):
        here = rows(i)
        for m in range(10):
            a, b, c = uf[m, here, :], uf[m, rows(i, s), :], uf[m, rows(i, 2 * s), :]
            both = a + c
            second = (0.5 * both - b) * KX
            cx[m, here, :] = 0.25 * (c - a)
            cx[10 + m, here, :] = second
            if m >= 5:
                cx[15 + m, here, :] = (0.5 / KB) * b - (1.0 / (6.0 * KB * KX)) * second

    @pl.loop(0, pair_tiles)
    def _(i):
        aux[2, rows(i), :] = jnp.maximum(aux[3, rows(i), :], aux[3, rows(i, s), :])

    @pl.loop(0, face_tiles)
    def _(i):
        values = face_values(
            lambda k, o: prim[k, rows(i, o * s), :],
            lambda k, o: aux[k, rows(i, o * s), :],
            lambda k, o: cx[k, rows(i, (o - 1) * s), :],
            comps,
        )
        for m in range(5):
            flux[order[m], rows(i), :] = values[m]

    if store is not None:

        @pl.loop(0, out_tiles)
        def _(i):
            store(i, [flux[k, rows(i, s), :] - flux[k, rows(i), :] for k in range(5)])


def prepare_kernel(nx, ny, nz, xeven, yeven, rho_ref, vel_ref, p_ref, q_ref, qt_ref, xa_ref, xb_ref, y_ref, z_ref, top_ref):
    rows, w = ny, nz
    n = nx * ny
    for k in range(5):
        for x in range(nx):
            src = rho_ref[x] if k == 0 else p_ref[x] if k == 4 else vel_ref[k - 1, x]
            q_ref[k, x * ny : (x + 1) * ny, :] = src
    top = None
    for i in range(n // 8):
        here = slice(8 * i, 8 * i + 8)
        sound = jnp.sqrt(gamma_gas * q_ref[4, here, :] / q_ref[0, here, :])
        speed = jnp.abs(q_ref[1, here, :]) + jnp.abs(q_ref[2, here, :]) + jnp.abs(q_ref[3, here, :]) + 3.0 * sound
        top = speed if top is None else jnp.maximum(top, speed)
    top_ref[...] = top
    width = 3 * ny
    high = (nx - 3) * ny
    if xeven:
        odd = lax.rem(lax.axis_index("gx"), 2)
        start_a = pl.multiple_of((1 - odd) * high, 8)
        start_b = pl.multiple_of(odd * high, 8)
    else:
        start_a, start_b = high, 0
    for k in range(5):
        xa_ref[k * width : (k + 1) * width, :] = q_ref[k, pl.ds(start_a, width), :]
        xb_ref[k * width : (k + 1) * width, :] = q_ref[k, pl.ds(start_b, width), :]
    xa_ref[5 * width : 5 * width + 8, :] = top
    edge = y_ref.shape[1]
    pad = edge - 15 * nx
    if pad:
        y_ref[0, 15 * nx :, :] = jnp.zeros((pad, w), f32)
        y_ref[1, 15 * nx :, :] = jnp.zeros((pad, w), f32)
    for k in range(5):
        for x in range(nx):
            at = (k * nx + x) * 3
            y_ref[0, at : at + 3, :] = q_ref[k, x * ny : x * ny + 3, :]
            y_ref[1, at : at + 3, :] = q_ref[k, (x + 1) * ny - 3 : (x + 1) * ny, :]
    z_ref[...] = jnp.zeros(z_ref.shape, f32)
    for k in range(5):
        qt_ref[k] = q_ref[k].T
        z_ref[0, 3 * k : 3 * k + 3, :] = qt_ref[k, 0:3, :]
        z_ref[1, 3 * k : 3 * k + 3, :] = qt_ref[k, nz - 3 : nz, :]


def x_kernel(nx, ny, xeven, q_ref, a_ref, b_ref, out_ref, prim, uf, aux, cx, flux):
    width = 3 * ny
    n = nx * ny
    far = (nx + 3) * ny
    if xeven:
        odd = lax.rem(lax.axis_index("gx"), 2)
        at_a = pl.multiple_of((1 - odd) * far, 8)
        at_b = pl.multiple_of(odd * far, 8)
    else:
        at_a, at_b = 0, far
    for k in range(5):
        prim[k, pl.ds(at_a, width), :] = a_ref[k * width : (k + 1) * width, :]
        prim[k, pl.ds(at_b, width), :] = b_ref[k * width : (k + 1) * width, :]
        prim[k, width : width + n, :] = q_ref[k]

    def store(i, values):
        for k in range(5):
            out_ref[k, pl.ds(pl.multiple_of(i * 8, 8), 8), :] = values[k]

    t = ny // 8
    sweep(prim, uf, aux, cx, flux, store, ny, (nx + 6) * t, (nx + 5) * t, (nx + 4) * t, (nx + 1) * t, nx * t, (0, 1, 2))


def y_kernel(nx, ny, block, q_ref, lo_ref, hi_ref, out_ref, prim, uf, aux, cx, flux):
    for k in range(5):
        for x in range(nx):
            at = (k * nx + x) * 3
            prim[k, x * block : x * block + 3, :] = lo_ref[at : at + 3, :]
            prim[k, x * block + 3 : x * block + 3 + ny, :] = q_ref[k, x * ny : (x + 1) * ny, :]
            prim[k, x * block + 3 + ny : x * block + 6 + ny, :] = hi_ref[at : at + 3, :]

    tiles = nx * block // 8

    sweep(prim, uf, aux, cx, flux, None, 1, tiles, tiles, tiles, tiles, 0, (1, 0, 2))
    for x in range(nx):
        for k in range(5):
            base = x * block
            out_ref[k, x * ny : (x + 1) * ny, :] = flux[k, base + 1 : base + 1 + ny, :] - flux[k, base : base + ny, :]


def z_kernel(n, nz, qt_ref, lo_ref, hi_ref, out_ref, prim, uf, aux, cx, flux):
    for k in range(5):
        prim[k, 0:3, :] = lo_ref[3 * k : 3 * k + 3, :]
        prim[k, 3 : 3 + nz, :] = qt_ref[k]
        prim[k, 3 + nz : 6 + nz, :] = hi_ref[3 * k : 3 * k + 3, :]
    tiles = rup(nz + 6, 8) // 8
    sweep(prim, uf, aux, cx, flux, None, 1, tiles, tiles, tiles, rup(nz + 1, 8) // 8, 0, (2, 0, 1))
    for k in range(5):
        out_ref[k] = (flux[k, 1 : nz + 1, :] - flux[k, 0:nz, :]).T


def final_kernel(nx, ny, q_ref, tx_ref, ty_ref, tz_ref, top_ref, out_ref):
    step = (cfl_number * KB) / jnp.max(top_ref[...], keepdims=True)
    for x in range(nx):
        here = slice(x * ny, (x + 1) * ny)
        rho, u1, u2, u3, p = (q_ref[k, here, :] for k in range(5))
        m1, m2, m3 = rho * u1, rho * u2, rho * u3
        energy = 2.5 * p + 0.5 * (m1 * u1 + m2 * u2 + m3 * u3)
        for k, value in enumerate((rho, m1, m2, m3, energy)):
            out_ref[k, x] = value - step * (tx_ref[k, here, :] + ty_ref[k, here, :] + tz_ref[k, here, :])


def call(kernel, outs, flops, scratch=()):
    return pl.pallas_call(
        kernel,
        out_shape=outs,
        scratch_shapes=scratch,
        compiler_params=pltpu.CompilerParams(vmem_limit_bytes=VMEM_LIMIT),
        cost_estimate=pl.CostEstimate(flops=flops, bytes_accessed=1000000, transcendentals=0),
    )


def sweep_scratch(rows, w):
    return [
        pltpu.VMEM((5, rows, w), f32),
        pltpu.VMEM((10, rows, w), f32),
        pltpu.VMEM((4, rows, w), f32),
        pltpu.VMEM((25, rows, w), f32),
        pltpu.VMEM((5, rows, w), f32),
    ]


def pairs_a(n):
    return [(i, i ^ 1) for i in range(n)]


def pairs_b(n):
    return [(i, (i + 1) % n if i % 2 else (i - 1) % n) for i in range(n)]


def top_over(top, axis, first):
    n = lax.axis_size(axis)
    if n & (n - 1):
        return lax.pmax(top, axis)
    d = first
    while d < n:
        top = jnp.maximum(top, lax.ppermute(top, axis, [(i, i ^ d) for i in range(n)]))
        d *= 2
    return top


def edge_trade(axis, low, high, top):
    n = lax.axis_size(axis)
    size = low.shape[0]
    if n == 1:
        return high, low, top
    if n == 2:
        got = lax.ppermute(jnp.concatenate([low, high, top]), axis, [(0, 1), (1, 0)])
        return got[size : 2 * size], got[:size], jnp.maximum(top, got[2 * size :])
    if n % 2:
        lower = lax.ppermute(high, axis, [(i, (i + 1) % n) for i in range(n)])
        upper = lax.ppermute(low, axis, [((i + 1) % n, i) for i in range(n)])
        return lower, upper, lax.pmax(top, axis)
    odd = lax.rem(lax.axis_index(axis), 2) == 1
    got_a = lax.ppermute(jnp.concatenate([jnp.where(odd, low, high), top]), axis, pairs_a(n))
    top = jnp.maximum(top, got_a[size:])
    send_b = jnp.where(odd, high, low)
    if n == 4:
        got_b = lax.ppermute(jnp.concatenate([send_b, top]), axis, pairs_b(n))
        top = jnp.maximum(top, got_b[size:])
    else:
        got_b = lax.ppermute(send_b, axis, pairs_b(n))
        top = top_over(top, axis, 2)
    lower = jnp.where(odd, got_a[:size], got_b[:size])
    upper = jnp.where(odd, got_b[:size], got_a[:size])
    return lower, upper, top


def local(density, velocity, pressure):
    nx, ny, nz = density.shape
    n = nx * ny
    gx = lax.axis_size("gx")
    xeven = gx % 2 == 0
    width = 15 * ny
    yrows = rup(15 * nx, 8)
    S = jax.ShapeDtypeStruct
    q, qt, xa, xb, ye, ze, top = call(
        functools.partial(prepare_kernel, nx, ny, nz, xeven, True),
        (
            S((5, n, nz), f32),
            S((5, nz, n), f32),
            S((width + 8, nz), f32),
            S((width, nz), f32),
            S((2, yrows, nz), f32),
            S((2, 16, n), f32),
            S((8, nz), f32),
        ),
        2000000,
    )(density, velocity, pressure)

    if xeven:
        got_b = lax.ppermute(xb, "gx", pairs_b(gx))
        got_a = lax.ppermute(xa, "gx", pairs_a(gx))
        top = jnp.maximum(top, got_a[width:])
    else:
        got_a = lax.ppermute(xa, "gx", [(i, (i + 1) % gx) for i in range(gx)])
        got_b = lax.ppermute(xb, "gx", [((i + 1) % gx, i) for i in range(gx)])
    ztop = top if n == nz else jnp.full((8, n), jnp.max(top))
    zlo, zhi, ztop = edge_trade("gz", ze[0], ze[1], ztop)
    top = ztop if n == nz else jnp.full((8, nz), jnp.max(ztop))
    ylo, yhi, top = edge_trade("gy", ye[0], ye[1], top)
    top = top_over(top, "gx", 2 if xeven else 1)

    sweep_flops = 16000000
    xr = (nx + 6) * ny
    tx = call(
        functools.partial(x_kernel, nx, ny, xeven), S((5, n, nz), f32), sweep_flops, sweep_scratch(xr, nz)
    )(q, got_a, got_b)
    zr = rup(nz + 6, 8) + 16
    tz = call(functools.partial(z_kernel, n, nz), S((5, n, nz), f32), sweep_flops, sweep_scratch(zr, n))(
        qt, zlo, zhi
    )
    block = rup(ny + 6, 8)
    yr = nx * block + 16
    ty = call(
        functools.partial(y_kernel, nx, ny, block), S((5, n, nz), f32), sweep_flops, sweep_scratch(yr, nz)
    )(q, ylo, yhi)
    return call(functools.partial(final_kernel, nx, ny), S((5, nx, ny, nz), f32), 1000000)(q, tx, ty, tz, top)


def solution(mesh):
    in_specs = (P("gx", "gy", "gz"), P(None, "gx", "gy", "gz"), P("gx", "gy", "gz"))
    out_specs = P(None, "gx", "gy", "gz")
    return jax.shard_map(local, mesh=mesh, in_specs=in_specs, out_specs=out_specs, check_vma=False)
```

```python
import functools
import math

import jax
import jax.numpy as jnp
from jax import lax
from jax.experimental import pallas as pl
from jax.experimental.pallas import tpu as pltpu
from jax.sharding import PartitionSpec as P

gamma_gas = 1.4
weno_eps = 1e-06
cfl_number = 0.4
f32 = jnp.float32

KX = math.sqrt(13.0 / 12.0)
KT = 0.5 / KX
KB = 1.0 / (6.0 * KX)
VMEM_LIMIT = 24 * 1024 * 1024


def rup(n, m):
    return (n + m - 1) // m * m


def rows(i, offset=0):
    return pl.ds(pl.multiple_of(i * 8, 8) + offset, 8)


def over(count, unroll, body):
    whole = count // unroll
    if whole:

        @pl.loop(0, whole)
        def _(j):
            for u in range(unroll):
                body(j * unroll + u)

    for i in range(whole * unroll, count):
        body(i)


def cell_pass(prim, uf, aux, count, comps):
    def body(i):
        here = rows(i)
        rho, p = prim[0, here, :], prim[4, here, :]
        un, ut, us = (prim[1 + c, here, :] for c in comps)
        inv = 1.0 / rho
        mn, mt, ms = rho * un, rho * ut, rho * us
        mnun = mn * un
        energy = 2.5 * p + 0.5 * (mnun + mt * ut + ms * us)
        total = energy + p
        values = (rho, mn, mt, ms, energy, mn, mnun + p, mt * un, ms * un, total * un)
        for m in range(10):
            uf[m, here, :] = values[m]
        aux[0, here, :] = total * inv
        aux[1, here, :] = jnp.sqrt(rho)
        aux[3, here, :] = jnp.abs(un) + jnp.sqrt(gamma_gas * p * inv)

    over(count, 4, body)


def diff_pass(uf, aux, cx, count, pairs, s):
    def body(i):
        here = rows(i)
        for m in range(10):
            a, b, c = uf[m, here, :], uf[m, rows(i, s), :], uf[m, rows(i, 2 * s), :]
            second = (0.5 * (a + c) - b) * KX
            cx[m, here, :] = 0.25 * (c - a)
            cx[10 + m, here, :] = second
            if m >= 5:
                cx[15 + m, here, :] = (0.5 / KB) * b - (1.0 / (6.0 * KB * KX)) * second

    def pair(i):
        aux[2, rows(i), :] = jnp.maximum(aux[3, rows(i), :], aux[3, rows(i, s), :])

    over(count, 2, body)
    over(pairs, 8, pair)


def weno_excess(mid, xa, xb, xc, sign, eps):
    tau_a = xa - xb
    tau_c = xb - xc
    if sign > 0:
        mid_a = mid + KT * tau_a
        mid_c = mid + KT * tau_c
    else:
        mid_a = mid - KT * tau_a
        mid_c = mid - KT * tau_c
    sm_a = mid_a * mid_a + (xa * xa + eps)
    sm_b = mid * mid + (xb * xb + eps)
    sm_c = mid_c * mid_c + (xc * xc + eps)
    ga = 3.0 * (sm_a * sm_a)
    gb = sm_b * sm_b
    gc = sm_c * sm_c
    gc = gc + gc
    num = gb * (tau_a * gc + tau_c * ga)
    den = gb * gc + (ga + ga) * (gb + gc)
    return num / den


def characteristic(v, un, ut, us, qh, b1, ic):
    t = (qh * v[0] - un * v[1]) - (ut * v[2] + us * v[3]) + v[4]
    a = b1 * t
    n = (un * v[0] - v[1]) * ic
    return (a + n, v[0] - a, v[2] - ut * v[0], v[3] - us * v[0], a - n)


def face_average(prim, aux, i, s, comps):
    def at(ref, k, o):
        return ref[k, rows(i, o * s), :]

    rl, rr = at(aux, 1, 2), at(aux, 1, 3)
    share = rr / (rl + rr)

    def roe(ref, k):
        left, right = at(ref, k, 2), at(ref, k, 3)
        return left + share * (right - left)

    un, ut, us = (roe(prim, 1 + c) for c in comps)
    enth = roe(aux, 0)
    qh = 0.5 * (un * un + ut * ut + us * us)
    c2 = (gamma_gas - 1.0) * (enth - qh)
    ic = lax.rsqrt(c2)
    b1 = (gamma_gas - 1.0) * (ic * ic)
    alpha = jnp.maximum(jnp.maximum(at(aux, 2, 0), at(aux, 2, 2)), at(aux, 2, 4))
    return un, ut, us, enth, qh, c2 * ic, ic, b1, alpha


def face_values(get_cx, average):
    un, ut, us, enth, qh, c, ic, b1, alpha = average
    args = (un, ut, us, qh, b1, ic)
    mid_p = characteristic([get_cx(5 + m, 2) + alpha * get_cx(m, 2) for m in range(5)], *args)
    mid_m = characteristic([get_cx(5 + m, 3) - alpha * get_cx(m, 3) for m in range(5)], *args)
    xu = {o: [alpha * get_cx(10 + m, o) for m in range(5)] for o in range(1, 5)}
    xp = {}
    xm = {}
    for o in (1, 2, 3, 4):
        xf = [get_cx(15 + m, o) for m in range(5)]
        if o <= 3:
            xp[o] = characteristic([xf[m] + xu[o][m] for m in range(5)], *args)
        if o >= 2:
            xm[o] = characteristic([xf[m] - xu[o][m] for m in range(5)], *args)
    g = []
    for m in range(5):
        eps = 4.0 * weno_eps if m in (0, 4) else weno_eps
        up = weno_excess(mid_p[m], xp[1][m], xp[2][m], xp[3][m], 1, eps)
        down = weno_excess(mid_m[m], xm[4][m], xm[3][m], xm[2][m], -1, eps)
        g.append(up + down)
    h2, h3, h4 = (g[m] + g[m] for m in (1, 2, 3))
    h15 = g[0] + g[4]
    dh = c * (g[4] - g[0])
    rr = h15 + h2
    upd = (
        rr,
        un * rr + dh,
        ut * rr + h3,
        us * rr + h4,
        enth * h15 + un * dh + qh * h2 + ut * h3 + us * h4,
    )
    return [
        (get_cx(20 + m, 2) + get_cx(20 + m, 3)) + (xu[3][m] - xu[2][m]) + upd[m] for m in range(5)
    ]


def face_pass(prim, aux, cx, count, s, comps, put):
    order = (0, 1 + comps[0], 1 + comps[1], 1 + comps[2], 4)

    def step(i, average):
        ahead = face_average(prim, aux, i + 1, s, comps)
        values = face_values(lambda k, o: cx[k, rows(i, (o - 1) * s), :], average)
        for m in range(5):
            put(order[m], i, values[m])
        return ahead

    lax.fori_loop(0, count, step, face_average(prim, aux, 0, s, comps))


def prepare_kernel(nx, ny, nz, xeven, rho, vel, p, q_ref, qt_ref, xa_ref, xb_ref, y_ref, z_ref, top_ref, sems):
    n = nx * ny
    sources = (rho, vel.at[0], vel.at[1], vel.at[2], p)
    copies = [
        pltpu.make_async_copy(src, q_ref.at[k, pl.ds(0, n), :], sems.at[k])
        for k, src in enumerate(sources)
    ]
    for copy in copies:
        copy.start()
    for copy in copies:
        copy.wait()
    top = None
    for i in range(n // 8):
        here = slice(8 * i, 8 * i + 8)
        sound = jnp.sqrt(gamma_gas * q_ref[4, here, :] / q_ref[0, here, :])
        speed = (jnp.abs(q_ref[1, here, :]) + jnp.abs(q_ref[2, here, :])) + (
            jnp.abs(q_ref[3, here, :]) + 3.0 * sound
        )
        top = speed if top is None else jnp.maximum(top, speed)
    top_ref[...] = top
    width = 3 * ny
    high = (nx - 3) * ny
    if xeven:
        odd = lax.rem(lax.axis_index("gx"), 2)
        start_a = pl.multiple_of((1 - odd) * high, 8)
        start_b = pl.multiple_of(odd * high, 8)
    else:
        start_a, start_b = high, 0
    for k in range(5):
        xa_ref[k * width : (k + 1) * width, :] = q_ref[k, pl.ds(start_a, width), :]
        xb_ref[k * width : (k + 1) * width, :] = q_ref[k, pl.ds(start_b, width), :]
    xa_ref[5 * width : 5 * width + 8, :] = top
    pad = y_ref.shape[1] - 15 * nx
    for side in (0, 1):
        if pad:
            y_ref[side, 15 * nx :, :] = jnp.zeros((pad, nz), f32)
        for k in range(5):
            for e in range(3):
                at = (3 * k + e) * nx
                row = e + side * (ny - 3)
                y_ref[side, at : at + nx, :] = q_ref[k, pl.ds(row, nx, stride=ny), :]
    z_ref[...] = jnp.zeros(z_ref.shape, f32)
    for k in range(5):
        qt_ref[k, 0:nz, :] = q_ref[k, 0:n, :].T
        z_ref[0, 3 * k : 3 * k + 3, :] = qt_ref[k, 0:3, :]
        z_ref[1, 3 * k : 3 * k + 3, :] = qt_ref[k, nz - 3 : nz, :]


def x_kernel(nx, ny, xeven, q_ref, a_ref, b_ref, after, out_ref, prim, uf, aux, cx, flux):
    width = 3 * ny
    n = nx * ny
    far = (nx + 3) * ny
    if xeven:
        odd = lax.rem(lax.axis_index("gx"), 2)
        at_a = pl.multiple_of((1 - odd) * far, 8)
        at_b = pl.multiple_of(odd * far, 8)
    else:
        at_a, at_b = 0, far
    for k in range(5):
        prim[k, pl.ds(at_a, width), :] = a_ref[k * width : (k + 1) * width, :]
        prim[k, pl.ds(at_b, width), :] = b_ref[k * width : (k + 1) * width, :]
        prim[k, width : width + n, :] = q_ref[k, 0:n, :]
    t = ny // 8
    comps = (0, 1, 2)
    cell_pass(prim, uf, aux, (nx + 6) * t, comps)
    diff_pass(uf, aux, cx, (nx + 4) * t, (nx + 5) * t, ny)

    def put(k, i, value):
        flux[k, rows(i), :] = value

    face_pass(prim, aux, cx, (nx + 1) * t, ny, comps, put)
    for k in range(5):
        out_ref[k] = flux[k, ny : ny + n, :] - flux[k, 0:n, :]


def inner_kernel(count, length, block, comps, q_ref, after, out_ref, uf, aux, cx):
    cell_pass(q_ref, uf, aux, count, comps)
    diff_pass(uf, aux, cx, count, count, 1)
    tiles = length // 8

    def put(k, i, value):
        if block:
            i = lax.div(i, tiles) * (block // 8) + lax.rem(i, tiles)
        out_ref[k, rows(i, 3), :] = value

    face_pass(q_ref, aux, cx, count, 1, comps, put)


def edge_kernel(nx, ny, nz, block, q_ref, qt_ref, ylo, yhi, zlo, zhi, fy_ref, fz_ref, after, out_ref, prim, uf, aux, cx, flux, fy, fz):
    n = nx * ny
    sb = rup(2 * nx, 8)
    for k in range(5):
        for e in range(8):
            if e < 3:
                low = ylo[(3 * k + e) * nx : (3 * k + e + 1) * nx, :]
            else:
                low = q_ref[k, pl.ds(e - 3, nx, stride=ny), :]
            if e < 5:
                high = q_ref[k, pl.ds(ny - 5 + e, nx, stride=ny), :]
            else:
                high = yhi[(3 * k + e - 5) * nx : (3 * k + e - 4) * nx, :]
            prim[k, e * sb : e * sb + nx, :] = low
            prim[k, e * sb + nx : e * sb + 2 * nx, :] = high
    t = sb // 8
    comps = (1, 0, 2)
    cell_pass(prim, uf, aux, 8 * t, comps)
    diff_pass(uf, aux, cx, 6 * t, 7 * t, sb)

    def put(k, i, value):
        flux[k, rows(i), :] = value

    face_pass(prim, aux, cx, 3 * t, sb, comps, put)
    for k in range(5):
        fy[k, 0 : nx * block, :] = fy_ref[k, 0 : nx * block, :]
        for f in range(3):
            fy[k, pl.ds(f, nx, stride=block), :] = flux[k, f * sb : f * sb + nx, :]
            fy[k, pl.ds(ny - 2 + f, nx, stride=block), :] = flux[k, f * sb + nx : f * sb + 2 * nx, :]
    for k in range(5):
        prim[k, 0:3, :] = zlo[3 * k : 3 * k + 3, :]
        prim[k, 3:8, :] = qt_ref[k, 0:5, :]
        prim[k, 8:13, :] = qt_ref[k, nz - 5 : nz, :]
        prim[k, 13:16, :] = zhi[3 * k : 3 * k + 3, :]
    comps = (2, 0, 1)
    cell_pass(prim, uf, aux, 2, comps)
    diff_pass(uf, aux, cx, 2, 2, 1)
    face_pass(prim, aux, cx, 2, 1, comps, put)
    for k in range(5):
        fz[k, 0 : nz + 8, :] = fz_ref[k, 0 : nz + 8, :]
        fz[k, 0:3, :] = flux[k, 0:3, :]
        fz[k, nz - 2 : nz + 1, :] = flux[k, 8:11, :]
    for k in range(5):
        across = (fz[k, 1 : nz + 1, :] - fz[k, 0:nz, :]).T
        for x in range(nx):
            at = x * block
            out_ref[k, x * ny : (x + 1) * ny, :] = across[x * ny : (x + 1) * ny, :] + (
                fy[k, at + 1 : at + 1 + ny, :] - fy[k, at : at + ny, :]
            )


def final_kernel(nx, ny, q_ref, tx_ref, t_ref, top_ref, out_ref):
    step = (cfl_number * KB) / jnp.max(top_ref[...], keepdims=True)
    for x in range(nx):
        here = slice(x * ny, (x + 1) * ny)
        rho, u1, u2, u3, p = (q_ref[k, here, :] for k in range(5))
        m1, m2, m3 = rho * u1, rho * u2, rho * u3
        energy = 2.5 * p + 0.5 * (m1 * u1 + m2 * u2 + m3 * u3)
        for k, value in enumerate((rho, m1, m2, m3, energy)):
            out_ref[k, x] = value - step * (tx_ref[k, here, :] + t_ref[k, here, :])


VMEM = pl.BlockSpec(memory_space=pltpu.VMEM)
HBM = pl.BlockSpec(memory_space=pltpu.HBM)
ANY = pl.BlockSpec(memory_space=pl.ANY)


def call(kernel, outs, flops, scratch=(), in_specs=None):
    extra = {} if in_specs is None else {"in_specs": in_specs}
    return pl.pallas_call(
        kernel,
        out_shape=outs,
        scratch_shapes=scratch,
        compiler_params=pltpu.CompilerParams(vmem_limit_bytes=VMEM_LIMIT),
        cost_estimate=pl.CostEstimate(flops=flops, bytes_accessed=1000000, transcendentals=0),
        **extra,
    )


def fields(*counts, r, w):
    return [pltpu.VMEM((count, r, w), f32) for count in counts]


def pairs_a(n):
    return [(i, i ^ 1) for i in range(n)]


def pairs_b(n):
    return [(i, (i + 1) % n if i % 2 else (i - 1) % n) for i in range(n)]


def top_over(top, axis, first):
    n = lax.axis_size(axis)
    if n & (n - 1):
        return lax.pmax(top, axis)
    d = first
    while d < n:
        top = jnp.maximum(top, lax.ppermute(top, axis, [(i, i ^ d) for i in range(n)]))
        d *= 2
    return top


def edge_trade(axis, low, high, top, mids=None):
    n = lax.axis_size(axis)
    size = low.shape[0]
    if n == 1:
        return high, low, top
    if n == 2:
        got = lax.ppermute(jnp.concatenate([low, high, top]), axis, [(0, 1), (1, 0)])
        return got[size : 2 * size], got[:size], jnp.maximum(top, got[2 * size :])
    if n % 2:
        lower = lax.ppermute(high, axis, [(i, (i + 1) % n) for i in range(n)])
        upper = lax.ppermute(low, axis, [((i + 1) % n, i) for i in range(n)])
        return lower, upper, lax.pmax(top, axis)
    odd = lax.rem(lax.axis_index(axis), 2) == 1
    got_a = lax.ppermute(jnp.concatenate([jnp.where(odd, low, high), top]), axis, pairs_a(n))
    top = jnp.maximum(top, got_a[size:])
    if mids is not None:
        mids.append(top)
    send_b = jnp.where(odd, high, low)
    if n == 4:
        got_b = lax.ppermute(jnp.concatenate([send_b, top]), axis, pairs_b(n))
        top = jnp.maximum(top, got_b[size:])
    else:
        got_b = lax.ppermute(send_b, axis, pairs_b(n))
        top = top_over(top, axis, 2)
    lower = jnp.where(odd, got_a[:size], got_b[:size])
    upper = jnp.where(odd, got_b[:size], got_a[:size])
    return lower, upper, top


def local(density, velocity, pressure):
    nx, ny, nz = density.shape
    n = nx * ny
    gx = lax.axis_size("gx")
    xeven = gx % 2 == 0
    width = 15 * ny
    S = jax.ShapeDtypeStruct
    q, qt, xa, xb, ye, ze, top = call(
        functools.partial(prepare_kernel, nx, ny, nz, xeven),
        (
            S((5, n + 16, nz), f32),
            S((5, nz + 16, n), f32),
            S((width + 8, nz), f32),
            S((width, nz), f32),
            S((2, rup(15 * nx, 8), nz), f32),
            S((2, 16, n), f32),
            S((8, nz), f32),
        ),
        2000000,
        [pltpu.SemaphoreType.DMA((5,))],
        [HBM] * 3,
    )(density.reshape(n, nz), velocity.reshape(3, n, nz), pressure.reshape(n, nz))

    sweep_flops = 16000000

    def inner(source, rows_in, lanes, length, block, comps, rows_out, after):
        return call(
            functools.partial(inner_kernel, rows_in // 8, length, block, comps),
            S((5, rows_out, lanes), f32),
            sweep_flops,
            fields(10, 4, 25, r=rows_in + 16, w=lanes),
            [VMEM, ANY],
        )(source, after)

    if xeven:
        got_b = lax.ppermute(xb, "gx", pairs_b(gx))
        got_a = lax.ppermute(xa, "gx", pairs_a(gx))
        top = jnp.maximum(top, got_a[width:])
    else:
        got_a = lax.ppermute(xa, "gx", [(i, (i + 1) % gx) for i in range(gx)])
        got_b = lax.ppermute(xb, "gx", [((i + 1) % gx, i) for i in range(gx)])
    ztop = top if n == nz else jnp.full((8, n), jnp.max(top))
    fz = inner(qt, nz, n, nz, 0, (2, 0, 1), nz + 16, ztop)
    zlo, zhi, ztop = edge_trade("gz", ze[0], ze[1], ztop)
    top = ztop if n == nz else jnp.full((8, nz), jnp.max(ztop))
    block = rup(ny + 6, 8)
    fy = inner(q, n, nz, ny, block, (1, 0, 2), nx * block + 16, top)
    mids = []
    ylo, yhi, top = edge_trade("gy", ye[0], ye[1], top, mids)
    tx = call(
        functools.partial(x_kernel, nx, ny, xeven),
        S((5, n, nz), f32),
        sweep_flops,
        fields(5, 10, 4, 25, 5, r=(nx + 6) * ny, w=nz),
        [VMEM] * 3 + [ANY],
    )(q, got_a, got_b, mids[0] if mids else top)
    near = 8 * rup(2 * nx, 8) + 16
    lanes = max(n, nz)
    t = call(
        functools.partial(edge_kernel, nx, ny, nz, block),
        S((5, n, nz), f32),
        sweep_flops // 2,
        fields(5, 10, 4, 25, 5, r=near, w=lanes)
        + [pltpu.VMEM((5, nx * block + 16, nz), f32), pltpu.VMEM((5, nz + 16, n), f32)],
        [VMEM] * 8 + [ANY],
    )(q, qt, ylo, yhi, zlo, zhi, fy, fz, top)
    top = top_over(top, "gx", 2 if xeven else 1)
    return call(functools.partial(final_kernel, nx, ny), S((5, nx, ny, nz), f32), 1000000)(q, tx, t, top)


def solution(mesh):
    in_specs = (P("gx", "gy", "gz"), P(None, "gx", "gy", "gz"), P("gx", "gy", "gz"))
    out_specs = P(None, "gx", "gy", "gz")
    return jax.shard_map(local, mesh=mesh, in_specs=in_specs, out_specs=out_specs, check_vma=False)
```

```python
import functools
import math

import jax
import jax.numpy as jnp
from jax import lax
from jax.experimental import pallas as pl
from jax.experimental.pallas import tpu as pltpu
from jax.sharding import PartitionSpec as P


gamma_gas = 1.4
weno_eps = 1e-06
cfl_number = 0.4
f32 = jnp.float32

KX = math.sqrt(13.0 / 12.0)
KT = 0.5 / KX
KB = 1.0 / (6.0 * KX)
VMEM_LIMIT = 24 * 1024 * 1024


def rup(n, m):
    return (n + m - 1) // m * m


def rows(i, offset=0):
    return pl.ds(pl.multiple_of(i * 8, 8) + offset, 8)


def over(count, unroll, body):
    whole = count // unroll
    if whole:

        @pl.loop(0, whole)
        def _(j):
            for u in range(unroll):
                body(j * unroll + u)

    for i in range(whole * unroll, count):
        body(i)


def cell_pass(prim, uf, aux, count, comps):
    def body(i):
        here = rows(i)
        rho, p = prim[0, here, :], prim[4, here, :]
        un, ut, us = (prim[1 + c, here, :] for c in comps)
        inv = 1.0 / rho
        mn, mt, ms = rho * un, rho * ut, rho * us
        mnun = mn * un
        energy = 2.5 * p + 0.5 * (mnun + mt * ut + ms * us)
        total = energy + p
        values = (rho, mn, mt, ms, energy, mn, mnun + p, mt * un, ms * un, total * un)
        for m in range(10):
            uf[m, here, :] = values[m]
        aux[0, here, :] = total * inv
        aux[1, here, :] = jnp.sqrt(rho)
        aux[3, here, :] = jnp.abs(un) + jnp.sqrt(gamma_gas * p * inv)

    over(count, 4, body)


def diff_pass(uf, aux, cx, count, pairs, s):
    def body(i):
        here = rows(i)
        for m in range(10):
            a, b, c = uf[m, here, :], uf[m, rows(i, s), :], uf[m, rows(i, 2 * s), :]
            second = (0.5 * (a + c) - b) * KX
            cx[m, here, :] = 0.25 * (c - a)
            cx[10 + m, here, :] = second
            if m >= 5:
                cx[15 + m, here, :] = (0.5 / KB) * b - (1.0 / (6.0 * KB * KX)) * second

    def pair(i):
        aux[2, rows(i), :] = jnp.maximum(aux[3, rows(i), :], aux[3, rows(i, s), :])

    over(count, 2, body)
    over(pairs, 8, pair)


def weno_excess(mid, xa, xb, xc, sign, eps):
    tau_a = xa - xb
    tau_c = xb - xc
    if sign > 0:
        mid_a = mid + KT * tau_a
        mid_c = mid + KT * tau_c
    else:
        mid_a = mid - KT * tau_a
        mid_c = mid - KT * tau_c
    sm_a = mid_a * mid_a + (xa * xa + eps)
    sm_b = mid * mid + (xb * xb + eps)
    sm_c = mid_c * mid_c + (xc * xc + eps)
    ga = 3.0 * (sm_a * sm_a)
    gb = sm_b * sm_b
    gc = sm_c * sm_c
    gc = gc + gc
    num = gb * (tau_a * gc + tau_c * ga)
    den = gb * gc + (ga + ga) * (gb + gc)
    return num / den


def characteristic(v, un, ut, us, qh, b1, ic):
    t = (qh * v[0] - un * v[1]) - (ut * v[2] + us * v[3]) + v[4]
    a = b1 * t
    n = (un * v[0] - v[1]) * ic
    return (a + n, v[0] - a, v[2] - ut * v[0], v[3] - us * v[0], a - n)


def face_average(prim, aux, i, s, comps):
    def at(ref, k, o):
        return ref[k, rows(i, o * s), :]

    rl, rr = at(aux, 1, 2), at(aux, 1, 3)
    share = rr / (rl + rr)

    def roe(ref, k):
        left, right = at(ref, k, 2), at(ref, k, 3)
        return left + share * (right - left)

    un, ut, us = (roe(prim, 1 + c) for c in comps)
    enth = roe(aux, 0)
    qh = 0.5 * (un * un + ut * ut + us * us)
    c2 = (gamma_gas - 1.0) * (enth - qh)
    ic = lax.rsqrt(c2)
    b1 = (gamma_gas - 1.0) * (ic * ic)
    alpha = jnp.maximum(jnp.maximum(at(aux, 2, 0), at(aux, 2, 2)), at(aux, 2, 4))
    return un, ut, us, enth, qh, c2 * ic, ic, b1, alpha


def face_values(get_cx, average):
    un, ut, us, enth, qh, c, ic, b1, alpha = average
    args = (un, ut, us, qh, b1, ic)
    mid_p = characteristic([get_cx(5 + m, 2) + alpha * get_cx(m, 2) for m in range(5)], *args)
    mid_m = characteristic([get_cx(5 + m, 3) - alpha * get_cx(m, 3) for m in range(5)], *args)
    xu = {o: [alpha * get_cx(10 + m, o) for m in range(5)] for o in range(1, 5)}
    xp = {}
    xm = {}
    for o in (1, 2, 3, 4):
        xf = [get_cx(15 + m, o) for m in range(5)]
        if o <= 3:
            xp[o] = characteristic([xf[m] + xu[o][m] for m in range(5)], *args)
        if o >= 2:
            xm[o] = characteristic([xf[m] - xu[o][m] for m in range(5)], *args)
    g = []
    for m in range(5):
        eps = 4.0 * weno_eps if m in (0, 4) else weno_eps
        up = weno_excess(mid_p[m], xp[1][m], xp[2][m], xp[3][m], 1, eps)
        down = weno_excess(mid_m[m], xm[4][m], xm[3][m], xm[2][m], -1, eps)
        g.append(up + down)
    h2, h3, h4 = (g[m] + g[m] for m in (1, 2, 3))
    h15 = g[0] + g[4]
    dh = c * (g[4] - g[0])
    rr = h15 + h2
    upd = (
        rr,
        un * rr + dh,
        ut * rr + h3,
        us * rr + h4,
        enth * h15 + un * dh + qh * h2 + ut * h3 + us * h4,
    )
    return [
        (get_cx(20 + m, 2) + get_cx(20 + m, 3)) + (xu[3][m] - xu[2][m]) + upd[m] for m in range(5)
    ]


def face_pass(prim, aux, cx, count, s, comps, put):
    order = (0, 1 + comps[0], 1 + comps[1], 1 + comps[2], 4)

    def step(i, average):
        ahead = face_average(prim, aux, i + 1, s, comps)
        values = face_values(lambda k, o: cx[k, rows(i, (o - 1) * s), :], average)
        for m in range(5):
            put(order[m], i, values[m])
        return ahead

    lax.fori_loop(0, count, step, face_average(prim, aux, 0, s, comps))


def prepare_kernel(nx, ny, nz, xeven, rho, vel, p, q_ref, qt_ref, xa_ref, xb_ref, y_ref, z_ref, top_ref, sems):
    n = nx * ny
    sources = (rho, vel.at[0], vel.at[1], vel.at[2], p)
    copies = [
        pltpu.make_async_copy(src, q_ref.at[k, pl.ds(0, n), :], sems.at[k])
        for k, src in enumerate(sources)
    ]
    for copy in copies:
        copy.start()
    for copy in copies:
        copy.wait()
    top = None
    for i in range(n // 8):
        here = slice(8 * i, 8 * i + 8)
        sound = jnp.sqrt(gamma_gas * q_ref[4, here, :] / q_ref[0, here, :])
        speed = (jnp.abs(q_ref[1, here, :]) + jnp.abs(q_ref[2, here, :])) + (
            jnp.abs(q_ref[3, here, :]) + 3.0 * sound
        )
        top = speed if top is None else jnp.maximum(top, speed)
    top_ref[...] = top
    width = 3 * ny
    high = (nx - 3) * ny
    if xeven:
        odd = lax.rem(lax.axis_index("gx"), 2)
        start_a = pl.multiple_of((1 - odd) * high, 8)
        start_b = pl.multiple_of(odd * high, 8)
    else:
        start_a, start_b = high, 0
    for k in range(5):
        xa_ref[k * width : (k + 1) * width, :] = q_ref[k, pl.ds(start_a, width), :]
        xb_ref[k * width : (k + 1) * width, :] = q_ref[k, pl.ds(start_b, width), :]
    xa_ref[5 * width : 5 * width + 8, :] = top
    pad = y_ref.shape[1] - 15 * nx
    for side in (0, 1):
        if pad:
            y_ref[side, 15 * nx :, :] = jnp.zeros((pad, nz), f32)
        for k in range(5):
            for e in range(3):
                at = (3 * k + e) * nx
                row = e + side * (ny - 3)
                y_ref[side, at : at + nx, :] = q_ref[k, pl.ds(row, nx, stride=ny), :]
    z_ref[...] = jnp.zeros(z_ref.shape, f32)
    for k in range(5):
        qt_ref[k, 0:nz, :] = q_ref[k, 0:n, :].T
        z_ref[0, 3 * k : 3 * k + 3, :] = qt_ref[k, 0:3, :]
        z_ref[1, 3 * k : 3 * k + 3, :] = qt_ref[k, nz - 3 : nz, :]


def x_kernel(nx, ny, xeven, q_ref, a_ref, b_ref, after, out_ref, prim, uf, aux, cx, flux):
    width = 3 * ny
    n = nx * ny
    far = (nx + 3) * ny
    if xeven:
        odd = lax.rem(lax.axis_index("gx"), 2)
        at_a = pl.multiple_of((1 - odd) * far, 8)
        at_b = pl.multiple_of(odd * far, 8)
    else:
        at_a, at_b = 0, far
    for k in range(5):
        prim[k, pl.ds(at_a, width), :] = a_ref[k * width : (k + 1) * width, :]
        prim[k, pl.ds(at_b, width), :] = b_ref[k * width : (k + 1) * width, :]
        prim[k, width : width + n, :] = q_ref[k, 0:n, :]
    t = ny // 8
    comps = (0, 1, 2)
    cell_pass(prim, uf, aux, (nx + 6) * t, comps)
    diff_pass(uf, aux, cx, (nx + 4) * t, (nx + 5) * t, ny)

    def put(k, i, value):
        flux[k, rows(i), :] = value

    face_pass(prim, aux, cx, (nx + 1) * t, ny, comps, put)
    for k in range(5):
        out_ref[k] = flux[k, ny : ny + n, :] - flux[k, 0:n, :]


def inner_kernel(count, length, block, comps, q_ref, after, out_ref, uf, aux, cx):
    cell_pass(q_ref, uf, aux, count, comps)
    diff_pass(uf, aux, cx, count, count, 1)
    tiles = length // 8

    def put(k, i, value):
        if block:
            i = lax.div(i, tiles) * (block // 8) + lax.rem(i, tiles)
        out_ref[k, rows(i, 3), :] = value

    face_pass(q_ref, aux, cx, count, 1, comps, put)


def edge_kernel(nx, ny, nz, block, q_ref, qt_ref, ylo, yhi, zlo, zhi, fy_ref, fz_ref, after, out_ref, prim, uf, aux, cx, flux, fy, fz):
    sb = rup(2 * nx, 8)
    for k in range(5):
        for e in range(8):
            if e < 3:
                low = ylo[(3 * k + e) * nx : (3 * k + e + 1) * nx, :]
            else:
                low = q_ref[k, pl.ds(e - 3, nx, stride=ny), :]
            if e < 5:
                high = q_ref[k, pl.ds(ny - 5 + e, nx, stride=ny), :]
            else:
                high = yhi[(3 * k + e - 5) * nx : (3 * k + e - 4) * nx, :]
            prim[k, e * sb : e * sb + nx, :] = low
            prim[k, e * sb + nx : e * sb + 2 * nx, :] = high
    t = sb // 8
    comps = (1, 0, 2)
    cell_pass(prim, uf, aux, 8 * t, comps)
    diff_pass(uf, aux, cx, 6 * t, 7 * t, sb)

    def put(k, i, value):
        flux[k, rows(i), :] = value

    face_pass(prim, aux, cx, 3 * t, sb, comps, put)
    for k in range(5):
        fy[k, 0 : nx * block, :] = fy_ref[k, 0 : nx * block, :]
        for f in range(3):
            fy[k, pl.ds(f, nx, stride=block), :] = flux[k, f * sb : f * sb + nx, :]
            fy[k, pl.ds(ny - 2 + f, nx, stride=block), :] = flux[k, f * sb + nx : f * sb + 2 * nx, :]
    for k in range(5):
        prim[k, 0:3, :] = zlo[3 * k : 3 * k + 3, :]
        prim[k, 3:8, :] = qt_ref[k, 0:5, :]
        prim[k, 8:13, :] = qt_ref[k, nz - 5 : nz, :]
        prim[k, 13:16, :] = zhi[3 * k : 3 * k + 3, :]
    comps = (2, 0, 1)
    cell_pass(prim, uf, aux, 2, comps)
    diff_pass(uf, aux, cx, 2, 2, 1)
    face_pass(prim, aux, cx, 2, 1, comps, put)
    for k in range(5):
        fz[k, 0 : nz + 8, :] = fz_ref[k, 0 : nz + 8, :]
        fz[k, 0:3, :] = flux[k, 0:3, :]
        fz[k, nz - 2 : nz + 1, :] = flux[k, 8:11, :]
    for k in range(5):
        across = (fz[k, 1 : nz + 1, :] - fz[k, 0:nz, :]).T
        for x in range(nx):
            at = x * block
            out_ref[k, x * ny : (x + 1) * ny, :] = across[x * ny : (x + 1) * ny, :] + (
                fy[k, at + 1 : at + 1 + ny, :] - fy[k, at : at + ny, :]
            )


def final_kernel(nx, ny, q_ref, tx_ref, t_ref, top_ref, out_ref):
    step = (cfl_number * KB) / jnp.max(top_ref[...], keepdims=True)
    for x in range(nx):
        here = slice(x * ny, (x + 1) * ny)
        rho, u1, u2, u3, p = (q_ref[k, here, :] for k in range(5))
        m1, m2, m3 = rho * u1, rho * u2, rho * u3
        energy = 2.5 * p + 0.5 * (m1 * u1 + m2 * u2 + m3 * u3)
        for k, value in enumerate((rho, m1, m2, m3, energy)):
            out_ref[k, x] = value - step * (tx_ref[k, here, :] + t_ref[k, here, :])


VMEM = pl.BlockSpec(memory_space=pltpu.VMEM)
HBM = pl.BlockSpec(memory_space=pltpu.HBM)
ANY = pl.BlockSpec(memory_space=pl.ANY)


def call(kernel, outs, flops, scratch=(), in_specs=None):
    extra = {} if in_specs is None else {"in_specs": in_specs}
    return pl.pallas_call(
        kernel,
        out_shape=outs,
        scratch_shapes=scratch,
        compiler_params=pltpu.CompilerParams(vmem_limit_bytes=VMEM_LIMIT),
        cost_estimate=pl.CostEstimate(flops=flops, bytes_accessed=1000000, transcendentals=0),
        **extra,
    )


def fields(*counts, r, w):
    return [pltpu.VMEM((count, r, w), f32) for count in counts]


def pairs_a(n):
    return [(i, i ^ 1) for i in range(n)]


def pairs_b(n):
    return [(i, (i + 1) % n if i % 2 else (i - 1) % n) for i in range(n)]


def top_over(top, axis, first):
    n = lax.axis_size(axis)
    if n & (n - 1):
        return lax.pmax(top, axis)
    d = first
    while d < n:
        top = jnp.maximum(top, lax.ppermute(top, axis, [(i, i ^ d) for i in range(n)]))
        d *= 2
    return top


def edge_trade(axis, low, high, top, mids=None):
    n = lax.axis_size(axis)
    size = low.shape[0]
    if n == 1:
        return high, low, top
    if n == 2:
        got = lax.ppermute(jnp.concatenate([low, high, top]), axis, [(0, 1), (1, 0)])
        return got[size : 2 * size], got[:size], jnp.maximum(top, got[2 * size :])
    if n % 2:
        lower = lax.ppermute(high, axis, [(i, (i + 1) % n) for i in range(n)])
        upper = lax.ppermute(low, axis, [((i + 1) % n, i) for i in range(n)])
        return lower, upper, lax.pmax(top, axis)
    odd = lax.rem(lax.axis_index(axis), 2) == 1
    got_a = lax.ppermute(jnp.concatenate([jnp.where(odd, low, high), top]), axis, pairs_a(n))
    top = jnp.maximum(top, got_a[size:])
    if mids is not None:
        mids.append(top)
    send_b = jnp.where(odd, high, low)
    if n == 4:
        got_b = lax.ppermute(jnp.concatenate([send_b, top]), axis, pairs_b(n))
        top = jnp.maximum(top, got_b[size:])
    else:
        got_b = lax.ppermute(send_b, axis, pairs_b(n))
        top = top_over(top, axis, 2)
    lower = jnp.where(odd, got_a[:size], got_b[:size])
    upper = jnp.where(odd, got_b[:size], got_a[:size])
    return lower, upper, top


def local(density, velocity, pressure):
    nx, ny, nz = density.shape
    n = nx * ny
    gx = lax.axis_size("gx")
    xeven = gx % 2 == 0
    width = 15 * ny
    S = jax.ShapeDtypeStruct
    density, velocity, pressure = (
        pltpu.with_memory_space_constraint(a, pltpu.HBM)
        for a in (density.reshape(n, nz), velocity.reshape(3, n, nz), pressure.reshape(n, nz))
    )
    q, qt, xa, xb, ye, ze, top = call(
        functools.partial(prepare_kernel, nx, ny, nz, xeven),
        (
            S((5, n + 16, nz), f32),
            S((5, nz + 16, n), f32),
            S((width + 8, nz), f32),
            S((width, nz), f32),
            S((2, rup(15 * nx, 8), nz), f32),
            S((2, 16, n), f32),
            S((8, nz), f32),
        ),
        2000000,
        [pltpu.SemaphoreType.DMA((5,))],
        [HBM] * 3,
    )(density, velocity, pressure)

    sweep_flops = 16000000

    def inner(source, rows_in, lanes, length, block, comps, rows_out, after):
        return call(
            functools.partial(inner_kernel, rows_in // 8, length, block, comps),
            S((5, rows_out, lanes), f32),
            sweep_flops,
            fields(10, 4, 25, r=rows_in + 16, w=lanes),
            [VMEM, ANY],
        )(source, after)

    if xeven:
        got_b = lax.ppermute(xb, "gx", pairs_b(gx))
        got_a = lax.ppermute(xa, "gx", pairs_a(gx))
        top = jnp.maximum(top, got_a[width:])
    else:
        got_a = lax.ppermute(xa, "gx", [(i, (i + 1) % gx) for i in range(gx)])
        got_b = lax.ppermute(xb, "gx", [((i + 1) % gx, i) for i in range(gx)])
    ztop = top if n == nz else jnp.full((8, n), jnp.max(top))
    fz = inner(qt, nz, n, nz, 0, (2, 0, 1), nz + 16, ztop)
    zlo, zhi, ztop = edge_trade("gz", ze[0], ze[1], ztop)
    top = ztop if n == nz else jnp.full((8, nz), jnp.max(ztop))
    block = rup(ny + 6, 8)
    fy = inner(q, n, nz, ny, block, (1, 0, 2), nx * block + 16, top)
    mids = []
    ylo, yhi, top = edge_trade("gy", ye[0], ye[1], top, mids)
    tx = call(
        functools.partial(x_kernel, nx, ny, xeven),
        S((5, n, nz), f32),
        sweep_flops,
        fields(5, 10, 4, 25, 5, r=(nx + 6) * ny, w=nz),
        [VMEM] * 3 + [ANY],
    )(q, got_a, got_b, mids[0] if mids else top)
    near = 8 * rup(2 * nx, 8) + 16
    lanes = max(n, nz)
    t = call(
        functools.partial(edge_kernel, nx, ny, nz, block),
        S((5, n, nz), f32),
        sweep_flops // 2,
        fields(5, 10, 4, 25, 5, r=near, w=lanes)
        + [pltpu.VMEM((5, nx * block + 16, nz), f32), pltpu.VMEM((5, nz + 16, n), f32)],
        [VMEM] * 8 + [ANY],
    )(q, qt, ylo, yhi, zlo, zhi, fy, fz, top)
    top = top_over(top, "gx", 2 if xeven else 1)
    return call(functools.partial(final_kernel, nx, ny), S((5, nx, ny, nz), f32), 1000000)(q, tx, t, top)


def solution(mesh):
    in_specs = (P("gx", "gy", "gz"), P(None, "gx", "gy", "gz"), P("gx", "gy", "gz"))
    out_specs = P(None, "gx", "gy", "gz")

    return jax.shard_map(local, mesh=mesh, in_specs=in_specs, out_specs=out_specs, check_vma=False)
```

```python
import functools
import math

import jax
import jax.numpy as jnp
from jax import lax
from jax.experimental import pallas as pl
from jax.experimental.pallas import tpu as pltpu
from jax.sharding import PartitionSpec as P


gamma_gas = 1.4
weno_eps = 1e-06
cfl_number = 0.4
f32 = jnp.float32

KX = math.sqrt(13.0 / 12.0)
KT = 0.5 / KX
KB = 1.0 / (6.0 * KX)
VMEM_LIMIT = 24 * 1024 * 1024


def rup(n, m):
    return (n + m - 1) // m * m


def rows(i, offset=0):
    return pl.ds(pl.multiple_of(i * 8, 8) + offset, 8)


def over(count, unroll, body):
    whole = count // unroll
    if whole:

        @pl.loop(0, whole)
        def _(j):
            for u in range(unroll):
                body(j * unroll + u)

    for i in range(whole * unroll, count):
        body(i)


def cell_pass(prim, uf, aux, count, comps):
    def body(i):
        here = rows(i)
        rho, p = prim[0, here, :], prim[4, here, :]
        un, ut, us = (prim[1 + c, here, :] for c in comps)
        inv = 1.0 / rho
        mn, mt, ms = rho * un, rho * ut, rho * us
        mnun = mn * un
        energy = 2.5 * p + 0.5 * (mnun + mt * ut + ms * us)
        total = energy + p
        values = (rho, mn, mt, ms, energy, mn, mnun + p, mt * un, ms * un, total * un)
        for m in range(10):
            uf[m, here, :] = values[m]
        aux[0, here, :] = total * inv
        aux[1, here, :] = jnp.sqrt(rho)
        aux[3, here, :] = jnp.abs(un) + jnp.sqrt(gamma_gas * p * inv)

    over(count, 4, body)


def diff_pass(uf, aux, cx, count, pairs, s):
    def body(i):
        here = rows(i)
        for m in range(10):
            a, b, c = uf[m, here, :], uf[m, rows(i, s), :], uf[m, rows(i, 2 * s), :]
            second = (0.5 * (a + c) - b) * KX
            cx[m, here, :] = 0.25 * (c - a)
            cx[10 + m, here, :] = second
            if m >= 5:
                cx[15 + m, here, :] = (0.5 / KB) * b - (1.0 / (6.0 * KB * KX)) * second

    def pair(i):
        aux[2, rows(i), :] = jnp.maximum(aux[3, rows(i), :], aux[3, rows(i, s), :])

    over(count, 2, body)
    over(pairs, 8, pair)


def weno_excess(mid, xa, xb, xc, sign, eps):
    tau_a = xa - xb
    tau_c = xb - xc
    if sign > 0:
        mid_a = mid + KT * tau_a
        mid_c = mid + KT * tau_c
    else:
        mid_a = mid - KT * tau_a
        mid_c = mid - KT * tau_c
    sm_a = mid_a * mid_a + (xa * xa + eps)
    sm_b = mid * mid + (xb * xb + eps)
    sm_c = mid_c * mid_c + (xc * xc + eps)
    ga = 3.0 * (sm_a * sm_a)
    gb = sm_b * sm_b
    gc = sm_c * sm_c
    gc = gc + gc
    num = gb * (tau_a * gc + tau_c * ga)
    den = gb * gc + (ga + ga) * (gb + gc)
    return num / den


def characteristic(v, un, ut, us, qh, b1, ic):
    t = (qh * v[0] - un * v[1]) - (ut * v[2] + us * v[3]) + v[4]
    a = b1 * t
    n = (un * v[0] - v[1]) * ic
    return (a + n, v[0] - a, v[2] - ut * v[0], v[3] - us * v[0], a - n)


def face_average(prim, aux, i, s, comps):
    def at(ref, k, o):
        return ref[k, rows(i, o * s), :]

    rl, rr = at(aux, 1, 2), at(aux, 1, 3)
    share = rr / (rl + rr)

    def roe(ref, k):
        left, right = at(ref, k, 2), at(ref, k, 3)
        return left + share * (right - left)

    un, ut, us = (roe(prim, 1 + c) for c in comps)
    enth = roe(aux, 0)
    qh = 0.5 * (un * un + ut * ut + us * us)
    c2 = (gamma_gas - 1.0) * (enth - qh)
    ic = lax.rsqrt(c2)
    b1 = (gamma_gas - 1.0) * (ic * ic)
    alpha = jnp.maximum(jnp.maximum(at(aux, 2, 0), at(aux, 2, 2)), at(aux, 2, 4))
    return un, ut, us, enth, qh, c2 * ic, ic, b1, alpha


def face_values(get_cx, average):
    un, ut, us, enth, qh, c, ic, b1, alpha = average
    args = (un, ut, us, qh, b1, ic)
    mid_p = characteristic([get_cx(5 + m, 2) + alpha * get_cx(m, 2) for m in range(5)], *args)
    mid_m = characteristic([get_cx(5 + m, 3) - alpha * get_cx(m, 3) for m in range(5)], *args)
    xu = {o: [alpha * get_cx(10 + m, o) for m in range(5)] for o in range(1, 5)}
    xp = {}
    xm = {}
    for o in (1, 2, 3, 4):
        xf = [get_cx(15 + m, o) for m in range(5)]
        if o <= 3:
            xp[o] = characteristic([xf[m] + xu[o][m] for m in range(5)], *args)
        if o >= 2:
            xm[o] = characteristic([xf[m] - xu[o][m] for m in range(5)], *args)
    g = []
    for m in range(5):
        eps = 4.0 * weno_eps if m in (0, 4) else weno_eps
        up = weno_excess(mid_p[m], xp[1][m], xp[2][m], xp[3][m], 1, eps)
        down = weno_excess(mid_m[m], xm[4][m], xm[3][m], xm[2][m], -1, eps)
        g.append(up + down)
    h2, h3, h4 = (g[m] + g[m] for m in (1, 2, 3))
    h15 = g[0] + g[4]
    dh = c * (g[4] - g[0])
    rr = h15 + h2
    upd = (
        rr,
        un * rr + dh,
        ut * rr + h3,
        us * rr + h4,
        enth * h15 + un * dh + qh * h2 + ut * h3 + us * h4,
    )
    return [
        (get_cx(20 + m, 2) + get_cx(20 + m, 3)) + (xu[3][m] - xu[2][m]) + upd[m] for m in range(5)
    ]


def face_pass(prim, aux, cx, count, s, comps, put):
    order = (0, 1 + comps[0], 1 + comps[1], 1 + comps[2], 4)

    def step(i, average):
        ahead = face_average(prim, aux, i + 1, s, comps)
        values = face_values(lambda k, o: cx[k, rows(i, (o - 1) * s), :], average)
        for m in range(5):
            put(order[m], i, values[m])
        return ahead

    lax.fori_loop(0, count, step, face_average(prim, aux, 0, s, comps))


def prepare_kernel(nx, ny, nz, xeven, rho, vel, p, q_ref, qt_ref, xa_ref, xb_ref, y_ref, z_ref, top_ref, sems):
    n = nx * ny
    sources = (rho, vel.at[0], vel.at[1], vel.at[2], p)
    copies = [
        pltpu.make_async_copy(src, q_ref.at[k, pl.ds(0, n), :], sems.at[k])
        for k, src in enumerate(sources)
    ]
    for copy in copies:
        copy.start()
    for copy in copies:
        copy.wait()
    top = None
    for i in range(n // 8):
        here = slice(8 * i, 8 * i + 8)
        sound = jnp.sqrt(gamma_gas * q_ref[4, here, :] / q_ref[0, here, :])
        speed = (jnp.abs(q_ref[1, here, :]) + jnp.abs(q_ref[2, here, :])) + (
            jnp.abs(q_ref[3, here, :]) + 3.0 * sound
        )
        top = speed if top is None else jnp.maximum(top, speed)
    top = jnp.broadcast_to(jnp.max(top, keepdims=True), (8, nz))
    top_ref[...] = top
    width = 3 * ny
    high = (nx - 3) * ny
    if xeven:
        odd = lax.rem(lax.axis_index("gx"), 2)
        start_a = pl.multiple_of((1 - odd) * high, 8)
        start_b = pl.multiple_of(odd * high, 8)
    else:
        start_a, start_b = high, 0
    for k in range(5):
        xa_ref[k * width : (k + 1) * width, :] = q_ref[k, pl.ds(start_a, width), :]
        xb_ref[k * width : (k + 1) * width, :] = q_ref[k, pl.ds(start_b, width), :]
    xa_ref[5 * width : 5 * width + 8, :] = top
    pad = y_ref.shape[1] - 15 * nx
    for side in (0, 1):
        if pad:
            y_ref[side, 15 * nx :, :] = jnp.zeros((pad, nz), f32)
        for k in range(5):
            for e in range(3):
                at = (3 * k + e) * nx
                row = e + side * (ny - 3)
                y_ref[side, at : at + nx, :] = q_ref[k, pl.ds(row, nx, stride=ny), :]
    z_ref[...] = jnp.zeros(z_ref.shape, f32)
    for k in range(5):
        qt_ref[k, 0:nz, :] = q_ref[k, 0:n, :].T
        z_ref[0, 3 * k : 3 * k + 3, :] = qt_ref[k, 0:3, :]
        z_ref[1, 3 * k : 3 * k + 3, :] = qt_ref[k, nz - 3 : nz, :]


def x_kernel(nx, ny, xeven, q_ref, a_ref, b_ref, after, out_ref, prim, uf, aux, cx, flux):
    width = 3 * ny
    n = nx * ny
    far = (nx + 3) * ny
    if xeven:
        odd = lax.rem(lax.axis_index("gx"), 2)
        at_a = pl.multiple_of((1 - odd) * far, 8)
        at_b = pl.multiple_of(odd * far, 8)
    else:
        at_a, at_b = 0, far
    for k in range(5):
        prim[k, pl.ds(at_a, width), :] = a_ref[k * width : (k + 1) * width, :]
        prim[k, pl.ds(at_b, width), :] = b_ref[k * width : (k + 1) * width, :]
        prim[k, width : width + n, :] = q_ref[k, 0:n, :]
    t = ny // 8
    comps = (0, 1, 2)
    cell_pass(prim, uf, aux, (nx + 6) * t, comps)
    diff_pass(uf, aux, cx, (nx + 4) * t, (nx + 5) * t, ny)

    def put(k, i, value):
        flux[k, rows(i), :] = value

    face_pass(prim, aux, cx, (nx + 1) * t, ny, comps, put)
    for k in range(5):
        out_ref[k] = flux[k, ny : ny + n, :] - flux[k, 0:n, :]


def inner_kernel(count, length, block, comps, q_ref, after, out_ref, uf, aux, cx):
    cell_pass(q_ref, uf, aux, count, comps)
    diff_pass(uf, aux, cx, count, count, 1)
    tiles = length // 8

    def put(k, i, value):
        if block:
            i = lax.div(i, tiles) * (block // 8) + lax.rem(i, tiles)
        out_ref[k, rows(i, 3), :] = value

    face_pass(q_ref, aux, cx, count, 1, comps, put)


def edge_kernel(nx, ny, nz, block, q_ref, qt_ref, ylo, yhi, zlo, zhi, fy_ref, fz_ref, after, out_ref, prim, uf, aux, cx, flux, fy, fz):
    sb = rup(2 * nx, 8)
    for k in range(5):
        for e in range(8):
            if e < 3:
                low = ylo[(3 * k + e) * nx : (3 * k + e + 1) * nx, :]
            else:
                low = q_ref[k, pl.ds(e - 3, nx, stride=ny), :]
            if e < 5:
                high = q_ref[k, pl.ds(ny - 5 + e, nx, stride=ny), :]
            else:
                high = yhi[(3 * k + e - 5) * nx : (3 * k + e - 4) * nx, :]
            prim[k, e * sb : e * sb + nx, :] = low
            prim[k, e * sb + nx : e * sb + 2 * nx, :] = high
    t = sb // 8
    comps = (1, 0, 2)
    cell_pass(prim, uf, aux, 8 * t, comps)
    diff_pass(uf, aux, cx, 6 * t, 7 * t, sb)

    def put(k, i, value):
        flux[k, rows(i), :] = value

    face_pass(prim, aux, cx, 3 * t, sb, comps, put)
    for k in range(5):
        fy[k, 0 : nx * block, :] = fy_ref[k, 0 : nx * block, :]
        for f in range(3):
            fy[k, pl.ds(f, nx, stride=block), :] = flux[k, f * sb : f * sb + nx, :]
            fy[k, pl.ds(ny - 2 + f, nx, stride=block), :] = flux[k, f * sb + nx : f * sb + 2 * nx, :]
    for k in range(5):
        prim[k, 0:3, :] = zlo[3 * k : 3 * k + 3, :]
        prim[k, 3:8, :] = qt_ref[k, 0:5, :]
        prim[k, 8:13, :] = qt_ref[k, nz - 5 : nz, :]
        prim[k, 13:16, :] = zhi[3 * k : 3 * k + 3, :]
    comps = (2, 0, 1)
    cell_pass(prim, uf, aux, 2, comps)
    diff_pass(uf, aux, cx, 2, 2, 1)
    face_pass(prim, aux, cx, 2, 1, comps, put)
    for k in range(5):
        fz[k, 0 : nz + 8, :] = fz_ref[k, 0 : nz + 8, :]
        fz[k, 0:3, :] = flux[k, 0:3, :]
        fz[k, nz - 2 : nz + 1, :] = flux[k, 8:11, :]
    for k in range(5):
        across = (fz[k, 1 : nz + 1, :] - fz[k, 0:nz, :]).T
        for x in range(nx):
            at = x * block
            out_ref[k, x * ny : (x + 1) * ny, :] = across[x * ny : (x + 1) * ny, :] + (
                fy[k, at + 1 : at + 1 + ny, :] - fy[k, at : at + ny, :]
            )


def final_kernel(nx, ny, q_ref, tx_ref, t_ref, top_ref, out_ref):
    step = (cfl_number * KB) / top_ref[0:1, :]
    for x in range(nx):
        here = slice(x * ny, (x + 1) * ny)
        rho, u1, u2, u3, p = (q_ref[k, here, :] for k in range(5))
        m1, m2, m3 = rho * u1, rho * u2, rho * u3
        energy = 2.5 * p + 0.5 * (m1 * u1 + m2 * u2 + m3 * u3)
        for k, value in enumerate((rho, m1, m2, m3, energy)):
            out_ref[k, x] = value - step * (tx_ref[k, here, :] + t_ref[k, here, :])


VMEM = pl.BlockSpec(memory_space=pltpu.VMEM)
HBM = pl.BlockSpec(memory_space=pltpu.HBM)
ANY = pl.BlockSpec(memory_space=pl.ANY)


def call(kernel, outs, flops, scratch=(), in_specs=None):
    extra = {} if in_specs is None else {"in_specs": in_specs}
    return pl.pallas_call(
        kernel,
        out_shape=outs,
        scratch_shapes=scratch,
        compiler_params=pltpu.CompilerParams(vmem_limit_bytes=VMEM_LIMIT),
        cost_estimate=pl.CostEstimate(flops=flops, bytes_accessed=1000000, transcendentals=0),
        **extra,
    )


def fields(*counts, r, w):
    return [pltpu.VMEM((count, r, w), f32) for count in counts]


def pairs_a(n):
    return [(i, i ^ 1) for i in range(n)]


def pairs_b(n):
    return [(i, (i + 1) % n if i % 2 else (i - 1) % n) for i in range(n)]


def top_over(top, axis, first, leads):
    n = lax.axis_size(axis)
    if n & (n - 1):
        return lax.pmax(top, axis)
    d = first
    while d < n:
        got = lead_permute(top, axis, [(i, i ^ d) for i in range(n)], leads)
        top = jnp.maximum(top, got)
        d *= 2
    return top


def lead_permute(value, axis, pairs, leads):
    gx = lax.axis_size("gx")
    if axis == "gx":
        return lax.ppermute(value, "gx", [(i, j) for i, j in pairs if leads(i)])
    n = lax.axis_size(axis)
    return lax.ppermute(
        value, ("gx", axis), [(g * n + i, g * n + j) for g in range(gx) if leads(g) for i, j in pairs]
    )


def with_top(edges, used, top):
    row = lax.broadcasted_iota(jnp.int32, edges.shape, 0)
    return jnp.where(row >= used, top[0:1], edges)


def got_top(top, got, row):
    return jnp.maximum(top, got[row : row + 1])


def edge_trade(axis, low, high, used, top, lead, leads, mids=None):
    n = lax.axis_size(axis)
    size = low.shape[0]

    def both(bare, pairs, top):
        led = lead_permute(with_top(bare, bare.shape[0] - size + used, top), axis, pairs, leads)
        if lead is None:
            return led, led
        rest = lead_permute(bare, axis, pairs, lambda i: not leads(i))
        return led, jnp.where(lead, led, rest)

    if n == 1:
        return high, low, top
    if n == 2:
        led, got = both(jnp.concatenate([low, high]), [(0, 1), (1, 0)], top)
        return got[size:], got[:size], got_top(top, led, size + used)
    if n % 2:
        lower = lax.ppermute(high, axis, [(i, (i + 1) % n) for i in range(n)])
        upper = lax.ppermute(low, axis, [((i + 1) % n, i) for i in range(n)])
        return lower, upper, lax.pmax(top, axis)
    odd = lax.rem(lax.axis_index(axis), 2) == 1
    led, got_a = both(jnp.where(odd, low, high), pairs_a(n), top)
    top = got_top(top, led, used)
    if mids is not None:
        mids.append(top)
    led, got_b = both(jnp.where(odd, high, low), pairs_b(n), top)
    if n == 4:
        top = got_top(top, led, used)
    else:
        top = top_over(top, axis, 2, leads)
    lower = jnp.where(odd, got_a, got_b)
    upper = jnp.where(odd, got_b, got_a)
    return lower, upper, top


def local(density, velocity, pressure):
    nx, ny, nz = density.shape
    n = nx * ny
    gx = lax.axis_size("gx")
    xeven = gx % 2 == 0
    width = 15 * ny
    S = jax.ShapeDtypeStruct
    density, velocity, pressure = (
        pltpu.with_memory_space_constraint(a, pltpu.HBM)
        for a in (density.reshape(n, nz), velocity.reshape(3, n, nz), pressure.reshape(n, nz))
    )
    q, qt, xa, xb, ye, ze, top = call(
        functools.partial(prepare_kernel, nx, ny, nz, xeven),
        (
            S((5, n + 16, nz), f32),
            S((5, nz + 16, n), f32),
            S((width + 8, nz), f32),
            S((width, nz), f32),
            S((2, rup(15 * nx + 1, 8), nz), f32),
            S((2, 16, n), f32),
            S((8, nz), f32),
        ),
        2000000,
        [pltpu.SemaphoreType.DMA((5,))],
        [HBM] * 3,
    )(density, velocity, pressure)

    sweep_flops = 16000000

    def inner(source, rows_in, lanes, length, block, comps, rows_out, after):
        return call(
            functools.partial(inner_kernel, rows_in // 8, length, block, comps),
            S((5, rows_out, lanes), f32),
            sweep_flops,
            fields(10, 4, 25, r=rows_in + 16, w=lanes),
            [VMEM, ANY],
        )(source, after)

    if xeven:
        got_b = lax.ppermute(xb, "gx", pairs_b(gx))
        got_a = lax.ppermute(xa, "gx", pairs_a(gx))
        top = jnp.maximum(top, got_a[width:])
    else:
        got_a = lax.ppermute(xa, "gx", [(i, (i + 1) % gx) for i in range(gx)])
        got_b = lax.ppermute(xb, "gx", [((i + 1) % gx, i) for i in range(gx)])
    ztop = top if n == nz else jnp.full((8, n), jnp.max(top))
    fz = inner(qt, nz, n, nz, 0, (2, 0, 1), nz + 16, ztop)
    lead, leads = None, lambda i: True
    if xeven:
        lead, leads = lax.rem(lax.axis_index("gx"), 2) == 1, lambda i: i % 2 == 1
    zlo, zhi, ztop = edge_trade("gz", ze[0], ze[1], 15, ztop, lead, leads)
    top = ztop if n == nz else jnp.full((8, nz), jnp.max(ztop))
    block = rup(ny + 6, 8)
    fy = inner(q, n, nz, ny, block, (1, 0, 2), nx * block + 16, top)
    mids = []
    ylo, yhi, top = edge_trade("gy", ye[0], ye[1], 15 * nx, top, lead, leads, mids)
    tx = call(
        functools.partial(x_kernel, nx, ny, xeven),
        S((5, n, nz), f32),
        sweep_flops,
        fields(5, 10, 4, 25, 5, r=(nx + 6) * ny, w=nz),
        [VMEM] * 3 + [ANY],
    )(q, got_a, got_b, mids[0] if mids else top)
    near = 8 * rup(2 * nx, 8) + 16
    lanes = max(n, nz)
    t = call(
        functools.partial(edge_kernel, nx, ny, nz, block),
        S((5, n, nz), f32),
        sweep_flops // 2,
        fields(5, 10, 4, 25, 5, r=near, w=lanes)
        + [pltpu.VMEM((5, nx * block + 16, nz), f32), pltpu.VMEM((5, nz + 16, n), f32)],
        [VMEM] * 8 + [ANY],
    )(q, qt, ylo, yhi, zlo, zhi, fy, fz, top)
    top = top_over(top, "gx", 2 if xeven else 1, leads)
    if xeven:
        top = jnp.maximum(top, lax.ppermute(top, "gx", [(i + 1, i) for i in range(0, gx, 2)]))
    return call(functools.partial(final_kernel, nx, ny), S((5, nx, ny, nz), f32), 1000000)(q, tx, t, top)


def solution(mesh):
    in_specs = (P("gx", "gy", "gz"), P(None, "gx", "gy", "gz"), P("gx", "gy", "gz"))
    out_specs = P(None, "gx", "gy", "gz")

    return jax.shard_map(local, mesh=mesh, in_specs=in_specs, out_specs=out_specs, check_vma=False)
```

```python
import functools
import math

import jax
import jax.numpy as jnp
from jax import lax
from jax.experimental import pallas as pl
from jax.experimental.pallas import tpu as pltpu
from jax.sharding import PartitionSpec as P


gamma_gas = 1.4
weno_eps = 1e-06
cfl_number = 0.4
f32 = jnp.float32

KX = math.sqrt(13.0 / 12.0)
KT = 0.5 / KX
KB = 1.0 / (6.0 * KX)
VMEM_LIMIT = 24 * 1024 * 1024


def rup(n, m):
    return (n + m - 1) // m * m


def rows(i, offset=0):
    return pl.ds(pl.multiple_of(i * 8, 8) + offset, 8)


def over(count, unroll, body):
    whole = count // unroll
    if whole:

        @pl.loop(0, whole)
        def _(j):
            for u in range(unroll):
                body(j * unroll + u)

    for i in range(whole * unroll, count):
        body(i)


def cell_pass(prim, uf, aux, count, comps):
    def body(i):
        here = rows(i)
        rho, p = prim[0, here, :], prim[4, here, :]
        un, ut, us = (prim[1 + c, here, :] for c in comps)
        inv = 1.0 / rho
        mn, mt, ms = rho * un, rho * ut, rho * us
        mnun = mn * un
        energy = 2.5 * p + 0.5 * (mnun + mt * ut + ms * us)
        total = energy + p
        values = (rho, mn, mt, ms, energy, mn, mnun + p, mt * un, ms * un, total * un)
        for m in range(10):
            uf[m, here, :] = values[m]
        aux[0, here, :] = total * inv
        aux[1, here, :] = jnp.sqrt(rho)
        aux[3, here, :] = jnp.abs(un) + jnp.sqrt(gamma_gas * p * inv)

    over(count, 4, body)


def diff_pass(uf, aux, cx, count, pairs, s):
    def body(i):
        here = rows(i)
        for m in range(10):
            a, b, c = uf[m, here, :], uf[m, rows(i, s), :], uf[m, rows(i, 2 * s), :]
            second = (0.5 * (a + c) - b) * KX
            cx[m, here, :] = 0.25 * (c - a)
            cx[10 + m, here, :] = second
            if m >= 5:
                cx[15 + m, here, :] = (0.5 / KB) * b - (1.0 / (6.0 * KB * KX)) * second

    def pair(i):
        aux[2, rows(i), :] = jnp.maximum(aux[3, rows(i), :], aux[3, rows(i, s), :])

    over(count, 2, body)
    over(pairs, 8, pair)


def weno_excess(mid, xa, xb, xc, sign, eps):
    tau_a = xa - xb
    tau_c = xb - xc
    if sign > 0:
        mid_a = mid + KT * tau_a
        mid_c = mid + KT * tau_c
    else:
        mid_a = mid - KT * tau_a
        mid_c = mid - KT * tau_c
    sm_a = mid_a * mid_a + (xa * xa + eps)
    sm_b = mid * mid + (xb * xb + eps)
    sm_c = mid_c * mid_c + (xc * xc + eps)
    ga = 3.0 * (sm_a * sm_a)
    gb = sm_b * sm_b
    gc = sm_c * sm_c
    gc = gc + gc
    num = gb * (tau_a * gc + tau_c * ga)
    den = gb * gc + (ga + ga) * (gb + gc)
    return num / den


def characteristic(v, un, ut, us, qh, b1, ic):
    t = (qh * v[0] - un * v[1]) - (ut * v[2] + us * v[3]) + v[4]
    a = b1 * t
    n = (un * v[0] - v[1]) * ic
    return (a + n, v[0] - a, v[2] - ut * v[0], v[3] - us * v[0], a - n)


def face_average(prim, aux, i, s, comps):
    def at(ref, k, o):
        return ref[k, rows(i, o * s), :]

    rl, rr = at(aux, 1, 2), at(aux, 1, 3)
    share = rr / (rl + rr)

    def roe(ref, k):
        left, right = at(ref, k, 2), at(ref, k, 3)
        return left + share * (right - left)

    un, ut, us = (roe(prim, 1 + c) for c in comps)
    enth = roe(aux, 0)
    qh = 0.5 * (un * un + ut * ut + us * us)
    c2 = (gamma_gas - 1.0) * (enth - qh)
    ic = lax.rsqrt(c2)
    b1 = (gamma_gas - 1.0) * (ic * ic)
    alpha = jnp.maximum(jnp.maximum(at(aux, 2, 0), at(aux, 2, 2)), at(aux, 2, 4))
    return un, ut, us, enth, qh, c2 * ic, ic, b1, alpha


def face_values(get_cx, average):
    un, ut, us, enth, qh, c, ic, b1, alpha = average
    args = (un, ut, us, qh, b1, ic)
    mid_p = characteristic([get_cx(5 + m, 2) + alpha * get_cx(m, 2) for m in range(5)], *args)
    mid_m = characteristic([get_cx(5 + m, 3) - alpha * get_cx(m, 3) for m in range(5)], *args)
    xu = {o: [alpha * get_cx(10 + m, o) for m in range(5)] for o in range(1, 5)}
    xp = {}
    xm = {}
    for o in (1, 2, 3, 4):
        xf = [get_cx(15 + m, o) for m in range(5)]
        if o <= 3:
            xp[o] = characteristic([xf[m] + xu[o][m] for m in range(5)], *args)
        if o >= 2:
            xm[o] = characteristic([xf[m] - xu[o][m] for m in range(5)], *args)
    g = []
    for m in range(5):
        eps = 4.0 * weno_eps if m in (0, 4) else weno_eps
        up = weno_excess(mid_p[m], xp[1][m], xp[2][m], xp[3][m], 1, eps)
        down = weno_excess(mid_m[m], xm[4][m], xm[3][m], xm[2][m], -1, eps)
        g.append(up + down)
    h2, h3, h4 = (g[m] + g[m] for m in (1, 2, 3))
    h15 = g[0] + g[4]
    dh = c * (g[4] - g[0])
    rr = h15 + h2
    upd = (
        rr,
        un * rr + dh,
        ut * rr + h3,
        us * rr + h4,
        enth * h15 + un * dh + qh * h2 + ut * h3 + us * h4,
    )
    return [
        (get_cx(20 + m, 2) + get_cx(20 + m, 3)) + (xu[3][m] - xu[2][m]) + upd[m] for m in range(5)
    ]


def face_pass(prim, aux, cx, count, s, comps, put):
    order = (0, 1 + comps[0], 1 + comps[1], 1 + comps[2], 4)

    def step(i, average):
        ahead = face_average(prim, aux, i + 1, s, comps)
        values = face_values(lambda k, o: cx[k, rows(i, (o - 1) * s), :], average)
        for m in range(5):
            put(order[m], i, values[m])
        return ahead

    lax.fori_loop(0, count, step, face_average(prim, aux, 0, s, comps))


def prepare_kernel(nx, ny, nz, xeven, rho, vel, p, q_ref, qt_ref, xa_ref, xb_ref, y_ref, z_ref, top_ref, sems):
    n = nx * ny
    sources = (rho, vel.at[0], vel.at[1], vel.at[2], p)
    copies = [
        pltpu.make_async_copy(src, q_ref.at[k, pl.ds(0, n), :], sems.at[k])
        for k, src in enumerate(sources)
    ]
    for copy in copies:
        copy.start()
    for copy in copies:
        copy.wait()
    top = None
    for i in range(n // 8):
        here = slice(8 * i, 8 * i + 8)
        sound = jnp.sqrt(gamma_gas * q_ref[4, here, :] / q_ref[0, here, :])
        speed = (jnp.abs(q_ref[1, here, :]) + jnp.abs(q_ref[2, here, :])) + (
            jnp.abs(q_ref[3, here, :]) + 3.0 * sound
        )
        top = speed if top is None else jnp.maximum(top, speed)
    top = jnp.broadcast_to(jnp.max(top, keepdims=True), (8, nz))
    top_ref[...] = top
    width = 3 * ny
    high = (nx - 3) * ny
    if xeven:
        odd = lax.rem(lax.axis_index("gx"), 2)
        start_a = pl.multiple_of((1 - odd) * high, 8)
        start_b = pl.multiple_of(odd * high, 8)
    else:
        start_a, start_b = high, 0
    for k in range(5):
        xa_ref[k * width : (k + 1) * width, :] = q_ref[k, pl.ds(start_a, width), :]
        xb_ref[k * width : (k + 1) * width, :] = q_ref[k, pl.ds(start_b, width), :]
    xa_ref[5 * width : 5 * width + 8, :] = top
    pad = y_ref.shape[1] - 15 * nx
    for side in (0, 1):
        if pad:
            y_ref[side, 15 * nx :, :] = jnp.zeros((pad, nz), f32)
        for k in range(5):
            for e in range(3):
                at = (3 * k + e) * nx
                row = e + side * (ny - 3)
                y_ref[side, at : at + nx, :] = q_ref[k, pl.ds(row, nx, stride=ny), :]
    z_ref[...] = jnp.zeros(z_ref.shape, f32)
    for k in range(5):
        qt_ref[k, 0:nz, :] = q_ref[k, 0:n, :].T
        z_ref[0, 3 * k : 3 * k + 3, :] = qt_ref[k, 0:3, :]
        z_ref[1, 3 * k : 3 * k + 3, :] = qt_ref[k, nz - 3 : nz, :]


def x_kernel(nx, ny, first, ys, xeven, q_ref, a_ref, b_ref, after, out_ref, prim, uf, aux, cx, flux):
    far = (nx + 3) * ys
    if xeven:
        odd = lax.rem(lax.axis_index("gx"), 2)
        at_a = pl.multiple_of((1 - odd) * far, 8)
        at_b = pl.multiple_of(odd * far, 8)
    else:
        at_a, at_b = 0, far
    for k in range(5):
        for e in range(3):
            row = (3 * k + e) * ny + first
            prim[k, pl.ds(pl.multiple_of(at_a + e * ys, 8), ys), :] = a_ref[row : row + ys, :]
            prim[k, pl.ds(pl.multiple_of(at_b + e * ys, 8), ys), :] = b_ref[row : row + ys, :]
        for x in range(nx):
            row = x * ny + first
            prim[k, (3 + x) * ys : (4 + x) * ys, :] = q_ref[k, row : row + ys, :]
    t = ys // 8
    comps = (0, 1, 2)
    cell_pass(prim, uf, aux, (nx + 6) * t, comps)
    diff_pass(uf, aux, cx, (nx + 4) * t, (nx + 5) * t, ys)

    def put(k, i, value):
        flux[k, rows(i), :] = value

    face_pass(prim, aux, cx, (nx + 1) * t, ys, comps, put)
    n = nx * ys
    for k in range(5):
        out_ref[k] = flux[k, ys : ys + n, :] - flux[k, 0:n, :]


def inner_kernel(count, length, block, comps, q_ref, after, out_ref, uf, aux, cx):
    cell_pass(q_ref, uf, aux, count, comps)
    diff_pass(uf, aux, cx, count, count, 1)
    tiles = length // 8

    def put(k, i, value):
        if block:
            i = lax.div(i, tiles) * (block // 8) + lax.rem(i, tiles)
        out_ref[k, rows(i, 3), :] = value

    face_pass(q_ref, aux, cx, count, 1, comps, put)


def edge_kernel(nx, ny, nz, block, q_ref, qt_ref, ylo, yhi, zlo, zhi, fy_ref, fz_ref, after, out_ref, prim, uf, aux, cx, flux, fy, fz):
    sb = rup(2 * nx, 8)
    for k in range(5):
        for e in range(8):
            if e < 3:
                low = ylo[(3 * k + e) * nx : (3 * k + e + 1) * nx, :]
            else:
                low = q_ref[k, pl.ds(e - 3, nx, stride=ny), :]
            if e < 5:
                high = q_ref[k, pl.ds(ny - 5 + e, nx, stride=ny), :]
            else:
                high = yhi[(3 * k + e - 5) * nx : (3 * k + e - 4) * nx, :]
            prim[k, e * sb : e * sb + nx, :] = low
            prim[k, e * sb + nx : e * sb + 2 * nx, :] = high
    t = sb // 8
    comps = (1, 0, 2)
    cell_pass(prim, uf, aux, 8 * t, comps)
    diff_pass(uf, aux, cx, 6 * t, 7 * t, sb)

    def put(k, i, value):
        flux[k, rows(i), :] = value

    face_pass(prim, aux, cx, 3 * t, sb, comps, put)
    for k in range(5):
        fy[k, 0 : nx * block, :] = fy_ref[k, 0 : nx * block, :]
        for f in range(3):
            fy[k, pl.ds(f, nx, stride=block), :] = flux[k, f * sb : f * sb + nx, :]
            fy[k, pl.ds(ny - 2 + f, nx, stride=block), :] = flux[k, f * sb + nx : f * sb + 2 * nx, :]
    for k in range(5):
        prim[k, 0:3, :] = zlo[3 * k : 3 * k + 3, :]
        prim[k, 3:8, :] = qt_ref[k, 0:5, :]
        prim[k, 8:13, :] = qt_ref[k, nz - 5 : nz, :]
        prim[k, 13:16, :] = zhi[3 * k : 3 * k + 3, :]
    comps = (2, 0, 1)
    cell_pass(prim, uf, aux, 2, comps)
    diff_pass(uf, aux, cx, 2, 2, 1)
    face_pass(prim, aux, cx, 2, 1, comps, put)
    for k in range(5):
        fz[k, 0 : nz + 8, :] = fz_ref[k, 0 : nz + 8, :]
        fz[k, 0:3, :] = flux[k, 0:3, :]
        fz[k, nz - 2 : nz + 1, :] = flux[k, 8:11, :]
    for k in range(5):
        across = (fz[k, 1 : nz + 1, :] - fz[k, 0:nz, :]).T
        for x in range(nx):
            at = x * block
            out_ref[k, x * ny : (x + 1) * ny, :] = across[x * ny : (x + 1) * ny, :] + (
                fy[k, at + 1 : at + 1 + ny, :] - fy[k, at : at + ny, :]
            )


def final_kernel(nx, ny, split, q_ref, tx_ref, rest_ref, t_ref, top_ref, out_ref):
    step = (cfl_number * KB) / top_ref[0:1, :]
    for x in range(nx):
        for lo, hi, part in ((0, split, tx_ref), (split, ny, rest_ref)):
            here = slice(x * ny + lo, x * ny + hi)
            there = slice(x * (hi - lo), (x + 1) * (hi - lo))
            rho, u1, u2, u3, p = (q_ref[k, here, :] for k in range(5))
            m1, m2, m3 = rho * u1, rho * u2, rho * u3
            energy = 2.5 * p + 0.5 * (m1 * u1 + m2 * u2 + m3 * u3)
            for k, value in enumerate((rho, m1, m2, m3, energy)):
                out_ref[k, x, lo:hi] = value - step * (part[k, there, :] + t_ref[k, here, :])


VMEM = pl.BlockSpec(memory_space=pltpu.VMEM)
HBM = pl.BlockSpec(memory_space=pltpu.HBM)
ANY = pl.BlockSpec(memory_space=pl.ANY)


def call(kernel, outs, flops, scratch=(), in_specs=None):
    extra = {} if in_specs is None else {"in_specs": in_specs}
    return pl.pallas_call(
        kernel,
        out_shape=outs,
        scratch_shapes=scratch,
        compiler_params=pltpu.CompilerParams(vmem_limit_bytes=VMEM_LIMIT),
        cost_estimate=pl.CostEstimate(flops=flops, bytes_accessed=1000000, transcendentals=0),
        **extra,
    )


def permute(value, axis, pairs):
    return lax.ppermute(value, axis, pairs)


def fields(*counts, r, w):
    return [pltpu.VMEM((count, r, w), f32) for count in counts]


def pairs_a(n):
    return [(i, i ^ 1) for i in range(n)]


def pairs_b(n):
    return [(i, (i + 1) % n if i % 2 else (i - 1) % n) for i in range(n)]


def top_over(top, axis, first):
    n = lax.axis_size(axis)
    if n & (n - 1):
        return lax.pmax(top, axis)
    d = first
    while d < n:
        top = jnp.maximum(top, permute(top, axis, [(i, i ^ d) for i in range(n)]))
        d *= 2
    return top


def with_top(edges, used, top):
    row = lax.broadcasted_iota(jnp.int32, edges.shape, 0)
    return jnp.where(row >= used, top[0:1], edges)


def got_top(top, got, row):
    return jnp.maximum(top, got[row : row + 1])


def edge_trade(axis, low, high, used, top, mids=None):
    n = lax.axis_size(axis)
    size = low.shape[0]
    if n == 1:
        return high, low, top
    if n == 2:
        got = permute(with_top(jnp.concatenate([low, high]), size + used, top), axis, [(0, 1), (1, 0)])
        return got[size:], got[:size], got_top(top, got, size + used)
    if n % 2:
        lower = permute(high, axis, [(i, (i + 1) % n) for i in range(n)])
        upper = permute(low, axis, [((i + 1) % n, i) for i in range(n)])
        return lower, upper, lax.pmax(top, axis)
    odd = lax.rem(lax.axis_index(axis), 2) == 1
    got_a = permute(with_top(jnp.where(odd, low, high), used, top), axis, pairs_a(n))
    top = got_top(top, got_a, used)
    if mids is not None:
        mids.append(top)
    got_b = permute(with_top(jnp.where(odd, high, low), used, top), axis, pairs_b(n))
    if n == 4:
        top = got_top(top, got_b, used)
    else:
        top = top_over(top, axis, 2)
    lower = jnp.where(odd, got_a, got_b)
    upper = jnp.where(odd, got_b, got_a)
    return lower, upper, top


def local(density, velocity, pressure):
    nx, ny, nz = density.shape
    n = nx * ny
    gx = lax.axis_size("gx")
    xeven = gx % 2 == 0
    width = 15 * ny
    S = jax.ShapeDtypeStruct
    density, velocity, pressure = (
        pltpu.with_memory_space_constraint(a, pltpu.HBM)
        for a in (density.reshape(n, nz), velocity.reshape(3, n, nz), pressure.reshape(n, nz))
    )
    q, qt, xa, xb, ye, ze, top = call(
        functools.partial(prepare_kernel, nx, ny, nz, xeven),
        (
            S((5, n + 16, nz), f32),
            S((5, nz + 16, n), f32),
            S((width + 8, nz), f32),
            S((width, nz), f32),
            S((2, rup(15 * nx + 1, 8), nz), f32),
            S((2, 16, n), f32),
            S((8, nz), f32),
        ),
        2000000,
        [pltpu.SemaphoreType.DMA((5,))],
        [HBM] * 3,
    )(density, velocity, pressure)

    sweep_flops = 16000000

    def inner(source, rows_in, lanes, length, block, comps, rows_out, after):
        return call(
            functools.partial(inner_kernel, rows_in // 8, length, block, comps),
            S((5, rows_out, lanes), f32),
            sweep_flops,
            fields(10, 4, 25, r=rows_in + 16, w=lanes),
            [VMEM, ANY],
        )(source, after)

    if xeven:
        got_b = permute(xb, "gx", pairs_b(gx))
        got_a = permute(xa, "gx", pairs_a(gx))
        top = jnp.maximum(top, got_a[width:])
    else:
        got_a = permute(xa, "gx", [(i, (i + 1) % gx) for i in range(gx)])
        got_b = permute(xb, "gx", [((i + 1) % gx, i) for i in range(gx)])
    ztop = top if n == nz else jnp.full((8, n), jnp.max(top))
    fz = inner(qt, nz, n, nz, 0, (2, 0, 1), nz + 16, ztop)
    zlo, zhi, ztop = edge_trade("gz", ze[0], ze[1], 15, ztop)
    top = ztop if n == nz else jnp.full((8, nz), jnp.max(ztop))
    block = rup(ny + 6, 8)
    fy = inner(q, n, nz, ny, block, (1, 0, 2), nx * block + 16, top)
    mids = []
    ylo, yhi, top = edge_trade("gy", ye[0], ye[1], 15 * nx, top, mids)

    def along_x(first, ys, after):
        return call(
            functools.partial(x_kernel, nx, ny, first, ys, xeven),
            S((5, nx * ys, nz), f32),
            sweep_flops,
            fields(5, 10, 4, 25, 5, r=(nx + 6) * ys + 16, w=nz),
            [VMEM] * 3 + [ANY],
        )(q, got_a, got_b, after)

    split = rup(3 * ny // 4, 8)
    tx = along_x(0, split, mids[0] if mids else top)
    tx_rest = along_x(split, ny - split, top)
    near = 8 * rup(2 * nx, 8) + 16
    lanes = max(n, nz)
    t = call(
        functools.partial(edge_kernel, nx, ny, nz, block),
        S((5, n, nz), f32),
        sweep_flops // 2,
        fields(5, 10, 4, 25, 5, r=near, w=lanes)
        + [pltpu.VMEM((5, nx * block + 16, nz), f32), pltpu.VMEM((5, nz + 16, n), f32)],
        [VMEM] * 8 + [ANY],
    )(q, qt, ylo, yhi, zlo, zhi, fy, fz, top)
    top = top_over(top, "gx", 2 if xeven else 1)
    return call(functools.partial(final_kernel, nx, ny, split), S((5, nx, ny, nz), f32), 1000000)(
        q, tx, tx_rest, t, top
    )


def solution(mesh):
    in_specs = (P("gx", "gy", "gz"), P(None, "gx", "gy", "gz"), P("gx", "gy", "gz"))
    out_specs = P(None, "gx", "gy", "gz")

    return jax.shard_map(local, mesh=mesh, in_specs=in_specs, out_specs=out_specs, check_vma=False)
```

```python
import functools
import math

import jax
import jax.numpy as jnp
from jax import lax
from jax.experimental import pallas as pl
from jax.experimental.pallas import tpu as pltpu
from jax.sharding import PartitionSpec as P


gamma_gas = 1.4
weno_eps = 1e-06
cfl_number = 0.4
f32 = jnp.float32

KX = math.sqrt(13.0 / 12.0)
KT = 0.5 / KX
KB = 1.0 / (6.0 * KX)
VMEM_LIMIT = 24 * 1024 * 1024


def rup(n, m):
    return (n + m - 1) // m * m


def rows(i, offset=0):
    return pl.ds(pl.multiple_of(i * 8, 8) + offset, 8)


def over(count, unroll, body):
    whole = count // unroll
    if whole:

        @pl.loop(0, whole)
        def _(j):
            for u in range(unroll):
                body(j * unroll + u)

    for i in range(whole * unroll, count):
        body(i)


def cell_pass(prim, uf, aux, count, comps, first=0):
    def body(i):
        here, there = rows(i), rows(i + first)
        rho, p = prim[0, there, :], prim[4, there, :]
        un, ut, us = (prim[1 + c, there, :] for c in comps)
        inv = 1.0 / rho
        mn, mt, ms = rho * un, rho * ut, rho * us
        mnun = mn * un
        energy = 2.5 * p + 0.5 * (mnun + mt * ut + ms * us)
        total = energy + p
        values = (rho, mn, mt, ms, energy, mn, mnun + p, mt * un, ms * un, total * un)
        for m in range(10):
            uf[m, here, :] = values[m]
        aux[0, here, :] = total * inv
        aux[1, here, :] = jnp.sqrt(rho)
        aux[3, here, :] = jnp.abs(un) + jnp.sqrt(gamma_gas * p * inv)

    over(count, 4, body)


def diff_pass(uf, aux, cx, count, pairs, s):
    def body(i):
        here = rows(i)
        for m in range(10):
            a, b, c = uf[m, here, :], uf[m, rows(i, s), :], uf[m, rows(i, 2 * s), :]
            second = (0.5 * (a + c) - b) * KX
            cx[m, here, :] = 0.25 * (c - a)
            cx[10 + m, here, :] = second
            if m >= 5:
                cx[15 + m, here, :] = (0.5 / KB) * b - (1.0 / (6.0 * KB * KX)) * second

    def pair(i):
        aux[2, rows(i), :] = jnp.maximum(aux[3, rows(i), :], aux[3, rows(i, s), :])

    over(count, 2, body)
    over(pairs, 8, pair)


def weno_excess(mid, xa, xb, xc, sign, eps):
    tau_a = xa - xb
    tau_c = xb - xc
    if sign > 0:
        mid_a = mid + KT * tau_a
        mid_c = mid + KT * tau_c
    else:
        mid_a = mid - KT * tau_a
        mid_c = mid - KT * tau_c
    sm_a = mid_a * mid_a + (xa * xa + eps)
    sm_b = mid * mid + (xb * xb + eps)
    sm_c = mid_c * mid_c + (xc * xc + eps)
    ga = 3.0 * (sm_a * sm_a)
    gb = sm_b * sm_b
    gc = sm_c * sm_c
    gc = gc + gc
    num = gb * (tau_a * gc + tau_c * ga)
    den = gb * gc + (ga + ga) * (gb + gc)
    return num / den


def characteristic(v, un, ut, us, qh, b1, ic):
    t = (qh * v[0] - un * v[1]) - (ut * v[2] + us * v[3]) + v[4]
    a = b1 * t
    n = (un * v[0] - v[1]) * ic
    return (a + n, v[0] - a, v[2] - ut * v[0], v[3] - us * v[0], a - n)


def face_average(prim, aux, i, s, comps, first):
    def at(ref, k, o):
        return ref[k, rows(i if ref is aux else i + first, o * s), :]

    rl, rr = at(aux, 1, 2), at(aux, 1, 3)
    share = rr / (rl + rr)

    def roe(ref, k):
        left, right = at(ref, k, 2), at(ref, k, 3)
        return left + share * (right - left)

    un, ut, us = (roe(prim, 1 + c) for c in comps)
    enth = roe(aux, 0)
    qh = 0.5 * (un * un + ut * ut + us * us)
    c2 = (gamma_gas - 1.0) * (enth - qh)
    ic = lax.rsqrt(c2)
    b1 = (gamma_gas - 1.0) * (ic * ic)
    alpha = jnp.maximum(jnp.maximum(at(aux, 2, 0), at(aux, 2, 2)), at(aux, 2, 4))
    return un, ut, us, enth, qh, c2 * ic, ic, b1, alpha


def face_values(get_cx, average):
    un, ut, us, enth, qh, c, ic, b1, alpha = average
    args = (un, ut, us, qh, b1, ic)
    mid_p = characteristic([get_cx(5 + m, 2) + alpha * get_cx(m, 2) for m in range(5)], *args)
    mid_m = characteristic([get_cx(5 + m, 3) - alpha * get_cx(m, 3) for m in range(5)], *args)
    xu = {o: [alpha * get_cx(10 + m, o) for m in range(5)] for o in range(1, 5)}
    xp = {}
    xm = {}
    for o in (1, 2, 3, 4):
        xf = [get_cx(15 + m, o) for m in range(5)]
        if o <= 3:
            xp[o] = characteristic([xf[m] + xu[o][m] for m in range(5)], *args)
        if o >= 2:
            xm[o] = characteristic([xf[m] - xu[o][m] for m in range(5)], *args)
    g = []
    for m in range(5):
        eps = 4.0 * weno_eps if m in (0, 4) else weno_eps
        up = weno_excess(mid_p[m], xp[1][m], xp[2][m], xp[3][m], 1, eps)
        down = weno_excess(mid_m[m], xm[4][m], xm[3][m], xm[2][m], -1, eps)
        g.append(up + down)
    h2, h3, h4 = (g[m] + g[m] for m in (1, 2, 3))
    h15 = g[0] + g[4]
    dh = c * (g[4] - g[0])
    rr = h15 + h2
    upd = (
        rr,
        un * rr + dh,
        ut * rr + h3,
        us * rr + h4,
        enth * h15 + un * dh + qh * h2 + ut * h3 + us * h4,
    )
    return [
        (get_cx(20 + m, 2) + get_cx(20 + m, 3)) + (xu[3][m] - xu[2][m]) + upd[m] for m in range(5)
    ]


def face_pass(prim, aux, cx, count, s, comps, put, first=0):
    order = (0, 1 + comps[0], 1 + comps[1], 1 + comps[2], 4)

    def step(i, average):
        ahead = face_average(prim, aux, i + 1, s, comps, first)
        values = face_values(lambda k, o: cx[k, rows(i, (o - 1) * s), :], average)
        for m in range(5):
            put(order[m], i, values[m])
        return ahead

    lax.fori_loop(0, count, step, face_average(prim, aux, 0, s, comps, first))


def prepare_kernel(nx, ny, nz, xeven, rho, vel, p, q_ref, xa_ref, top_ref, sems):
    n = nx * ny
    sources = (rho, vel.at[0], vel.at[1], vel.at[2], p)
    copies = [
        pltpu.make_async_copy(src, q_ref.at[k, pl.ds(0, n), :], sems.at[k])
        for k, src in enumerate(sources)
    ]
    for copy in copies:
        copy.start()
    for copy in copies:
        copy.wait()
    top = None
    for i in range(n // 8):
        here = slice(8 * i, 8 * i + 8)
        sound = jnp.sqrt(gamma_gas * q_ref[4, here, :] / q_ref[0, here, :])
        speed = (jnp.abs(q_ref[1, here, :]) + jnp.abs(q_ref[2, here, :])) + (
            jnp.abs(q_ref[3, here, :]) + 3.0 * sound
        )
        top = speed if top is None else jnp.maximum(top, speed)
    top = jnp.broadcast_to(jnp.max(top, keepdims=True), (8, nz))
    top_ref[...] = top
    width = 3 * ny
    start, _ = edge_starts(nx, ny, xeven)
    for k in range(5):
        xa_ref[k * width : (k + 1) * width, :] = q_ref[k, pl.ds(start, width), :]
    xa_ref[5 * width : 5 * width + 8, :] = top


def edge_starts(nx, ny, xeven):
    high = (nx - 3) * ny
    if not xeven:
        return high, 0
    odd = lax.rem(lax.axis_index("gx"), 2)
    return pl.multiple_of((1 - odd) * high, 8), pl.multiple_of(odd * high, 8)


def turn_kernel(nx, ny, nz, xeven, q_ref, after, qt_ref, xb_ref, y_ref, z_ref):
    n = nx * ny
    for k in range(5):
        qt_ref[k, 0:nz, :] = q_ref[k, 0:n, :].T
    pad = y_ref.shape[1] - 15 * nx
    for side in (0, 1):
        if pad:
            y_ref[side, 15 * nx :, :] = jnp.zeros((pad, nz), f32)
        for k in range(5):
            for e in range(3):
                at = (3 * k + e) * nx
                row = e + side * (ny - 3)
                y_ref[side, at : at + nx, :] = q_ref[k, pl.ds(row, nx, stride=ny), :]
    width = 3 * ny
    _, start = edge_starts(nx, ny, xeven)
    for k in range(5):
        xb_ref[k * width : (k + 1) * width, :] = q_ref[k, pl.ds(start, width), :]
    z_ref[...] = jnp.zeros(z_ref.shape, f32)
    for k in range(5):
        z_ref[0, 3 * k : 3 * k + 3, :] = qt_ref[k, 0:3, :]
        z_ref[1, 3 * k : 3 * k + 3, :] = qt_ref[k, nz - 3 : nz, :]


def x_kernel(nx, ny, first, ys, xeven, q_ref, a_ref, b_ref, after, out_ref, prim, uf, aux, cx, flux):
    far = (nx + 3) * ys
    if xeven:
        odd = lax.rem(lax.axis_index("gx"), 2)
        at_a = pl.multiple_of((1 - odd) * far, 8)
        at_b = pl.multiple_of(odd * far, 8)
    else:
        at_a, at_b = 0, far
    for k in range(5):
        for e in range(3):
            row = (3 * k + e) * ny + first
            prim[k, pl.ds(pl.multiple_of(at_a + e * ys, 8), ys), :] = a_ref[row : row + ys, :]
            prim[k, pl.ds(pl.multiple_of(at_b + e * ys, 8), ys), :] = b_ref[row : row + ys, :]
        for x in range(nx):
            row = x * ny + first
            prim[k, (3 + x) * ys : (4 + x) * ys, :] = q_ref[k, row : row + ys, :]
    t = ys // 8
    comps = (0, 1, 2)
    cell_pass(prim, uf, aux, (nx + 6) * t, comps)
    diff_pass(uf, aux, cx, (nx + 4) * t, (nx + 5) * t, ys)

    def put(k, i, value):
        flux[k, rows(i), :] = value

    face_pass(prim, aux, cx, (nx + 1) * t, ys, comps, put)
    n = nx * ys
    for k in range(5):
        out_ref[k] = flux[k, ys : ys + n, :] - flux[k, 0:n, :]


def inner_kernel(first, count, more, length, block, comps, q_ref, after, out_ref, uf, aux, cx):
    cell_pass(q_ref, uf, aux, count + more, comps, first)
    diff_pass(uf, aux, cx, count + more, count + more, 1)
    tiles = length // 8

    def put(k, i, value):
        if block:
            i = lax.div(i, tiles) * (block // 8) + lax.rem(i, tiles)
        out_ref[k, rows(i, 3), :] = value

    face_pass(q_ref, aux, cx, count, 1, comps, put, first)


def edge_kernel(nx, ny, nz, block, q_ref, qt_ref, ylo, yhi, zlo, zhi, fy_ref, fz_ref, fz2_ref, after, out_ref, prim, uf, aux, cx, flux, fy, fz):
    sb = rup(2 * nx, 8)
    for k in range(5):
        for e in range(8):
            if e < 3:
                low = ylo[(3 * k + e) * nx : (3 * k + e + 1) * nx, :]
            else:
                low = q_ref[k, pl.ds(e - 3, nx, stride=ny), :]
            if e < 5:
                high = q_ref[k, pl.ds(ny - 5 + e, nx, stride=ny), :]
            else:
                high = yhi[(3 * k + e - 5) * nx : (3 * k + e - 4) * nx, :]
            prim[k, e * sb : e * sb + nx, :] = low
            prim[k, e * sb + nx : e * sb + 2 * nx, :] = high
    t = sb // 8
    comps = (1, 0, 2)
    cell_pass(prim, uf, aux, 8 * t, comps)
    diff_pass(uf, aux, cx, 6 * t, 7 * t, sb)

    def put(k, i, value):
        flux[k, rows(i), :] = value

    face_pass(prim, aux, cx, 3 * t, sb, comps, put)
    for k in range(5):
        fy[k, 0 : nx * block, :] = fy_ref[k, 0 : nx * block, :]
        for f in range(3):
            fy[k, pl.ds(f, nx, stride=block), :] = flux[k, f * sb : f * sb + nx, :]
            fy[k, pl.ds(ny - 2 + f, nx, stride=block), :] = flux[k, f * sb + nx : f * sb + 2 * nx, :]
    for k in range(5):
        prim[k, 0:3, :] = zlo[3 * k : 3 * k + 3, :]
        prim[k, 3:8, :] = qt_ref[k, 0:5, :]
        prim[k, 8:13, :] = qt_ref[k, nz - 5 : nz, :]
        prim[k, 13:16, :] = zhi[3 * k : 3 * k + 3, :]
    comps = (2, 0, 1)
    cell_pass(prim, uf, aux, 2, comps)
    diff_pass(uf, aux, cx, 2, 2, 1)
    face_pass(prim, aux, cx, 2, 1, comps, put)
    for k in range(5):
        part = fz_ref.shape[1] - 8
        fz[k, 3 : part + 3, :] = fz_ref[k, 3 : part + 3, :]
        fz[k, part + 3 : nz + 3, :] = fz2_ref[k, 3 : nz - part + 3, :]
        fz[k, 0:3, :] = flux[k, 0:3, :]
        fz[k, nz - 2 : nz + 1, :] = flux[k, 8:11, :]
    for k in range(5):
        across = (fz[k, 1 : nz + 1, :] - fz[k, 0:nz, :]).T
        for x in range(nx):
            at = x * block
            out_ref[k, x * ny : (x + 1) * ny, :] = across[x * ny : (x + 1) * ny, :] + (
                fy[k, at + 1 : at + 1 + ny, :] - fy[k, at : at + ny, :]
            )


def final_kernel(nx, ny, split, q_ref, tx_ref, rest_ref, t_ref, top_ref, out_ref):
    step = (cfl_number * KB) / top_ref[0:1, :]
    for x in range(nx):
        for lo, hi, part in ((0, split, tx_ref), (split, ny, rest_ref)):
            here = slice(x * ny + lo, x * ny + hi)
            there = slice(x * (hi - lo), (x + 1) * (hi - lo))
            rho, u1, u2, u3, p = (q_ref[k, here, :] for k in range(5))
            m1, m2, m3 = rho * u1, rho * u2, rho * u3
            energy = 2.5 * p + 0.5 * (m1 * u1 + m2 * u2 + m3 * u3)
            for k, value in enumerate((rho, m1, m2, m3, energy)):
                out_ref[k, x, lo:hi] = value - step * (part[k, there, :] + t_ref[k, here, :])


VMEM = pl.BlockSpec(memory_space=pltpu.VMEM)
HBM = pl.BlockSpec(memory_space=pltpu.HBM)
ANY = pl.BlockSpec(memory_space=pl.ANY)


def call(kernel, outs, flops, scratch=(), in_specs=None):
    extra = {} if in_specs is None else {"in_specs": in_specs}
    return pl.pallas_call(
        kernel,
        out_shape=outs,
        scratch_shapes=scratch,
        compiler_params=pltpu.CompilerParams(vmem_limit_bytes=VMEM_LIMIT),
        cost_estimate=pl.CostEstimate(flops=flops, bytes_accessed=1000000, transcendentals=0),
        **extra,
    )


def permute(value, axis, pairs):
    return lax.ppermute(value, axis, pairs)


def fields(*counts, r, w):
    return [pltpu.VMEM((count, r, w), f32) for count in counts]


def pairs_a(n):
    return [(i, i ^ 1) for i in range(n)]


def pairs_b(n):
    return [(i, (i + 1) % n if i % 2 else (i - 1) % n) for i in range(n)]


def top_over(top, axis, first):
    n = lax.axis_size(axis)
    if n & (n - 1):
        return lax.pmax(top, axis)
    d = first
    while d < n:
        top = jnp.maximum(top, permute(top, axis, [(i, i ^ d) for i in range(n)]))
        d *= 2
    return top


def with_top(edges, used, top):
    row = lax.broadcasted_iota(jnp.int32, edges.shape, 0)
    return jnp.where(row >= used, top[0:1], edges)


def got_top(top, got, row):
    return jnp.maximum(top, got[row : row + 1])


def edge_trade(axis, low, high, used, top, mids=None):
    n = lax.axis_size(axis)
    size = low.shape[0]
    if n == 1:
        return high, low, top
    if n == 2:
        got = permute(with_top(jnp.concatenate([low, high]), size + used, top), axis, [(0, 1), (1, 0)])
        return got[size:], got[:size], got_top(top, got, size + used)
    if n % 2:
        lower = permute(high, axis, [(i, (i + 1) % n) for i in range(n)])
        upper = permute(low, axis, [((i + 1) % n, i) for i in range(n)])
        return lower, upper, lax.pmax(top, axis)
    odd = lax.rem(lax.axis_index(axis), 2) == 1
    got_a = permute(with_top(jnp.where(odd, low, high), used, top), axis, pairs_a(n))
    top = got_top(top, got_a, used)
    if mids is not None:
        mids.append(top)
    got_b = permute(with_top(jnp.where(odd, high, low), used, top), axis, pairs_b(n))
    if n == 4:
        top = got_top(top, got_b, used)
    else:
        top = top_over(top, axis, 2)
    lower = jnp.where(odd, got_a, got_b)
    upper = jnp.where(odd, got_b, got_a)
    return lower, upper, top


def local(density, velocity, pressure):
    nx, ny, nz = density.shape
    n = nx * ny
    gx = lax.axis_size("gx")
    xeven = gx % 2 == 0
    width = 15 * ny
    S = jax.ShapeDtypeStruct
    density, velocity, pressure = (
        pltpu.with_memory_space_constraint(a, pltpu.HBM)
        for a in (density.reshape(n, nz), velocity.reshape(3, n, nz), pressure.reshape(n, nz))
    )
    q, xa, top = call(
        functools.partial(prepare_kernel, nx, ny, nz, xeven),
        (S((5, n + 16, nz), f32), S((width + 8, nz), f32), S((8, nz), f32)),
        2000000,
        [pltpu.SemaphoreType.DMA((5,))],
        [HBM] * 3,
    )(density, velocity, pressure)
    qt, xb, ye, ze = call(
        functools.partial(turn_kernel, nx, ny, nz, xeven),
        (
            S((5, nz + 16, n), f32),
            S((width, nz), f32),
            S((2, rup(15 * nx + 1, 8), nz), f32),
            S((2, 16, n), f32),
        ),
        2000000,
        (),
        [VMEM, ANY],
    )(q, top)

    sweep_flops = 16000000

    def inner(source, first, count, more, lanes, length, block, comps, rows_out, after):
        return call(
            functools.partial(inner_kernel, first, count, more, length, block, comps),
            S((5, rows_out, lanes), f32),
            sweep_flops,
            fields(10, 4, 25, r=8 * (count + more) + 16, w=lanes),
            [VMEM, ANY],
        )(source, after)

    if xeven:
        got_b = permute(xb, "gx", pairs_b(gx))
        got_a = permute(xa, "gx", pairs_a(gx))
        top = jnp.maximum(top, got_a[width:])
    else:
        got_a = permute(xa, "gx", [(i, (i + 1) % gx) for i in range(gx)])
        got_b = permute(xb, "gx", [((i + 1) % gx, i) for i in range(gx)])
    ztop = top if n == nz else jnp.full((8, n), jnp.max(top))
    zt = nz // 8
    half = zt // 2
    fz = [
        inner(qt, 0, half, 1, n, nz, 0, (2, 0, 1), 8 * half + 8, ye),
        inner(qt, half, zt - half, 0, n, nz, 0, (2, 0, 1), 8 * (zt - half) + 8, ztop),
    ]
    zlo, zhi, ztop = edge_trade("gz", ze[0], ze[1], 15, ztop)
    top = ztop if n == nz else jnp.full((8, nz), jnp.max(ztop))
    block = rup(ny + 6, 8)
    fy = inner(q, 0, n // 8, 0, nz, ny, block, (1, 0, 2), nx * block + 16, top)
    mids = []
    ylo, yhi, top = edge_trade("gy", ye[0], ye[1], 15 * nx, top, mids)

    def along_x(first, ys, after):
        return call(
            functools.partial(x_kernel, nx, ny, first, ys, xeven),
            S((5, nx * ys, nz), f32),
            sweep_flops,
            fields(5, 10, 4, 25, 5, r=(nx + 6) * ys + 16, w=nz),
            [VMEM] * 3 + [ANY],
        )(q, got_a, got_b, after)

    split = rup(3 * ny // 4, 8)
    tx = along_x(0, split, mids[0] if mids else top)
    tx_rest = along_x(split, ny - split, top)
    near = 8 * rup(2 * nx, 8) + 16
    lanes = max(n, nz)
    t = call(
        functools.partial(edge_kernel, nx, ny, nz, block),
        S((5, n, nz), f32),
        sweep_flops // 2,
        fields(5, 10, 4, 25, 5, r=near, w=lanes)
        + [pltpu.VMEM((5, nx * block + 16, nz), f32), pltpu.VMEM((5, nz + 16, n), f32)],
        [VMEM] * 9 + [ANY],
    )(q, qt, ylo, yhi, zlo, zhi, fy, *fz, top)
    top = top_over(top, "gx", 2 if xeven else 1)
    return call(functools.partial(final_kernel, nx, ny, split), S((5, nx, ny, nz), f32), 1000000)(
        q, tx, tx_rest, t, top
    )


def solution(mesh):
    in_specs = (P("gx", "gy", "gz"), P(None, "gx", "gy", "gz"), P("gx", "gy", "gz"))
    out_specs = P(None, "gx", "gy", "gz")

    return jax.shard_map(local, mesh=mesh, in_specs=in_specs, out_specs=out_specs, check_vma=False)
```

```python
import functools
import math

import jax
import jax.numpy as jnp
from jax import lax
from jax.experimental import pallas as pl
from jax.experimental.pallas import tpu as pltpu
from jax.sharding import PartitionSpec as P


gamma_gas = 1.4
weno_eps = 1e-06
cfl_number = 0.4
f32 = jnp.float32

KX = math.sqrt(13.0 / 12.0)
KT = 0.5 / KX
KB = 1.0 / (6.0 * KX)
VMEM_LIMIT = 24 * 1024 * 1024


def rup(n, m):
    return (n + m - 1) // m * m


def rows(i, offset=0):
    return pl.ds(pl.multiple_of(i * 8, 8) + offset, 8)


def over(count, unroll, body):
    whole = count // unroll
    if whole:

        @pl.loop(0, whole)
        def _(j):
            for u in range(unroll):
                body(j * unroll + u)

    for i in range(whole * unroll, count):
        body(i)


def cell_pass(prim, uf, aux, count, comps, first=0):
    def body(i):
        here, there = rows(i), rows(i + first)
        rho, p = prim[0, there, :], prim[4, there, :]
        un, ut, us = (prim[1 + c, there, :] for c in comps)
        inv = 1.0 / rho
        mn, mt, ms = rho * un, rho * ut, rho * us
        mnun = mn * un
        energy = 2.5 * p + 0.5 * (mnun + mt * ut + ms * us)
        total = energy + p
        values = (rho, mn, mt, ms, energy, mn, mnun + p, mt * un, ms * un, total * un)
        for m in range(10):
            uf[m, here, :] = values[m]
        aux[0, here, :] = total * inv
        aux[1, here, :] = jnp.sqrt(rho)
        aux[3, here, :] = jnp.abs(un) + jnp.sqrt(gamma_gas * p * inv)

    over(count, 4, body)


def diff_pass(uf, aux, cx, count, pairs, s):
    def body(i):
        here = rows(i)
        for m in range(10):
            a, b, c = uf[m, here, :], uf[m, rows(i, s), :], uf[m, rows(i, 2 * s), :]
            second = (0.5 * (a + c) - b) * KX
            cx[m, here, :] = 0.25 * (c - a)
            cx[10 + m, here, :] = second
            if m >= 5:
                cx[15 + m, here, :] = (0.5 / KB) * b - (1.0 / (6.0 * KB * KX)) * second

    def pair(i):
        aux[2, rows(i), :] = jnp.maximum(aux[3, rows(i), :], aux[3, rows(i, s), :])

    over(count, 2, body)
    over(pairs, 8, pair)


def weno_excess(mid, xa, xb, xc, sign, eps):
    tau_a = xa - xb
    tau_c = xb - xc
    if sign > 0:
        mid_a = mid + KT * tau_a
        mid_c = mid + KT * tau_c
    else:
        mid_a = mid - KT * tau_a
        mid_c = mid - KT * tau_c
    sm_a = mid_a * mid_a + (xa * xa + eps)
    sm_b = mid * mid + (xb * xb + eps)
    sm_c = mid_c * mid_c + (xc * xc + eps)
    ga = 3.0 * (sm_a * sm_a)
    gb = sm_b * sm_b
    gc = sm_c * sm_c
    gc = gc + gc
    num = gb * (tau_a * gc + tau_c * ga)
    den = gb * gc + (ga + ga) * (gb + gc)
    return num / den


def characteristic(v, un, ut, us, qh, b1, ic):
    t = (qh * v[0] - un * v[1]) - (ut * v[2] + us * v[3]) + v[4]
    a = b1 * t
    n = (un * v[0] - v[1]) * ic
    return (a + n, v[0] - a, v[2] - ut * v[0], v[3] - us * v[0], a - n)


def face_average(prim, aux, i, s, comps, first):
    def at(ref, k, o):
        return ref[k, rows(i if ref is aux else i + first, o * s), :]

    rl, rr = at(aux, 1, 2), at(aux, 1, 3)
    share = rr / (rl + rr)

    def roe(ref, k):
        left, right = at(ref, k, 2), at(ref, k, 3)
        return left + share * (right - left)

    un, ut, us = (roe(prim, 1 + c) for c in comps)
    enth = roe(aux, 0)
    qh = 0.5 * (un * un + ut * ut + us * us)
    c2 = (gamma_gas - 1.0) * (enth - qh)
    ic = lax.rsqrt(c2)
    b1 = (gamma_gas - 1.0) * (ic * ic)
    alpha = jnp.maximum(jnp.maximum(at(aux, 2, 0), at(aux, 2, 2)), at(aux, 2, 4))
    return un, ut, us, enth, qh, c2 * ic, ic, b1, alpha


def face_values(get_cx, average):
    un, ut, us, enth, qh, c, ic, b1, alpha = average
    args = (un, ut, us, qh, b1, ic)
    mid_p = characteristic([get_cx(5 + m, 2) + alpha * get_cx(m, 2) for m in range(5)], *args)
    mid_m = characteristic([get_cx(5 + m, 3) - alpha * get_cx(m, 3) for m in range(5)], *args)
    xu = {o: [alpha * get_cx(10 + m, o) for m in range(5)] for o in range(1, 5)}
    xp = {}
    xm = {}
    for o in (1, 2, 3, 4):
        xf = [get_cx(15 + m, o) for m in range(5)]
        if o <= 3:
            xp[o] = characteristic([xf[m] + xu[o][m] for m in range(5)], *args)
        if o >= 2:
            xm[o] = characteristic([xf[m] - xu[o][m] for m in range(5)], *args)
    g = []
    for m in range(5):
        eps = 4.0 * weno_eps if m in (0, 4) else weno_eps
        up = weno_excess(mid_p[m], xp[1][m], xp[2][m], xp[3][m], 1, eps)
        down = weno_excess(mid_m[m], xm[4][m], xm[3][m], xm[2][m], -1, eps)
        g.append(up + down)
    h2, h3, h4 = (g[m] + g[m] for m in (1, 2, 3))
    h15 = g[0] + g[4]
    dh = c * (g[4] - g[0])
    rr = h15 + h2
    upd = (
        rr,
        un * rr + dh,
        ut * rr + h3,
        us * rr + h4,
        enth * h15 + un * dh + qh * h2 + ut * h3 + us * h4,
    )
    return [
        (get_cx(20 + m, 2) + get_cx(20 + m, 3)) + (xu[3][m] - xu[2][m]) + upd[m] for m in range(5)
    ]


def face_pass(prim, aux, cx, count, s, comps, put, first=0):
    order = (0, 1 + comps[0], 1 + comps[1], 1 + comps[2], 4)

    def step(i, average):
        ahead = face_average(prim, aux, i + 1, s, comps, first)
        values = face_values(lambda k, o: cx[k, rows(i, (o - 1) * s), :], average)
        for m in range(5):
            put(order[m], i, values[m])
        return ahead

    lax.fori_loop(0, count, step, face_average(prim, aux, 0, s, comps, first))


def prepare_kernel(nx, ny, nz, xeven, rho, vel, p, q_ref, xa_ref, top_ref, sems):
    n = nx * ny
    sources = (rho, vel.at[0], vel.at[1], vel.at[2], p)
    copies = [
        pltpu.make_async_copy(src, q_ref.at[k, pl.ds(0, n), :], sems.at[k])
        for k, src in enumerate(sources)
    ]
    for copy in copies:
        copy.start()
    for copy in copies:
        copy.wait()
    top = None
    for i in range(n // 8):
        here = slice(8 * i, 8 * i + 8)
        sound = jnp.sqrt(gamma_gas * q_ref[4, here, :] / q_ref[0, here, :])
        speed = (jnp.abs(q_ref[1, here, :]) + jnp.abs(q_ref[2, here, :])) + (
            jnp.abs(q_ref[3, here, :]) + 3.0 * sound
        )
        top = speed if top is None else jnp.maximum(top, speed)
    top = jnp.broadcast_to(jnp.max(top, keepdims=True), (8, nz))
    top_ref[...] = top
    width = 3 * ny
    start, _ = edge_starts(nx, ny, xeven)
    for k in range(5):
        xa_ref[k * width : (k + 1) * width, :] = q_ref[k, pl.ds(start, width), :]
    xa_ref[5 * width : 5 * width + 8, :] = top


def edge_starts(nx, ny, xeven):
    high = (nx - 3) * ny
    if not xeven:
        return high, 0
    odd = lax.rem(lax.axis_index("gx"), 2)
    return pl.multiple_of((1 - odd) * high, 8), pl.multiple_of(odd * high, 8)


def turn_kernel(nx, ny, nz, xeven, q_ref, after, qt_ref, xb_ref, y_ref, z_ref):
    n = nx * ny
    for k in range(5):
        qt_ref[k, 0:nz, :] = q_ref[k, 0:n, :].T
    pad = y_ref.shape[1] - 15 * nx
    for side in (0, 1):
        if pad:
            y_ref[side, 15 * nx :, :] = jnp.zeros((pad, nz), f32)
        for k in range(5):
            for e in range(3):
                at = (3 * k + e) * nx
                row = e + side * (ny - 3)
                y_ref[side, at : at + nx, :] = q_ref[k, pl.ds(row, nx, stride=ny), :]
    width = 3 * ny
    _, start = edge_starts(nx, ny, xeven)
    for k in range(5):
        xb_ref[k * width : (k + 1) * width, :] = q_ref[k, pl.ds(start, width), :]
    z_ref[...] = jnp.zeros(z_ref.shape, f32)
    for k in range(5):
        z_ref[0, 3 * k : 3 * k + 3, :] = qt_ref[k, 0:3, :]
        z_ref[1, 3 * k : 3 * k + 3, :] = qt_ref[k, nz - 3 : nz, :]


def x_kernel(nx, ny, first, ys, xeven, q_ref, a_ref, b_ref, after, out_ref, prim, uf, aux, cx, flux):
    far = (nx + 3) * ys
    if xeven:
        odd = lax.rem(lax.axis_index("gx"), 2)
        at_a = pl.multiple_of((1 - odd) * far, 8)
        at_b = pl.multiple_of(odd * far, 8)
    else:
        at_a, at_b = 0, far
    for k in range(5):
        for e in range(3):
            row = (3 * k + e) * ny + first
            prim[k, pl.ds(pl.multiple_of(at_a + e * ys, 8), ys), :] = a_ref[row : row + ys, :]
            prim[k, pl.ds(pl.multiple_of(at_b + e * ys, 8), ys), :] = b_ref[row : row + ys, :]
        for x in range(nx):
            row = x * ny + first
            prim[k, (3 + x) * ys : (4 + x) * ys, :] = q_ref[k, row : row + ys, :]
    t = ys // 8
    comps = (0, 1, 2)
    cell_pass(prim, uf, aux, (nx + 6) * t, comps)
    diff_pass(uf, aux, cx, (nx + 4) * t, (nx + 5) * t, ys)

    def put(k, i, value):
        flux[k, rows(i), :] = value

    face_pass(prim, aux, cx, (nx + 1) * t, ys, comps, put)
    n = nx * ys
    for k in range(5):
        out_ref[k] = flux[k, ys : ys + n, :] - flux[k, 0:n, :]


def inner_kernel(first, count, more, length, block, comps, q_ref, after, out_ref, uf, aux, cx):
    cell_pass(q_ref, uf, aux, count + more, comps, first)
    diff_pass(uf, aux, cx, count + more, count + more, 1)
    tiles = length // 8

    def put(k, i, value):
        if block:
            i = lax.div(i, tiles) * (block // 8) + lax.rem(i, tiles)
        out_ref[k, rows(i, 3), :] = value

    face_pass(q_ref, aux, cx, count, 1, comps, put, first)


def z_ends_kernel(nz, qt_ref, lo, hi, fz_ref, fz2_ref, after, out_ref, prim, uf, aux, cx, flux, fz):
    for k in range(5):
        prim[k] = jnp.ones(prim.shape[1:], f32)
        for j in range(6):
            if j < 3:
                prim[k, 8 * j : 8 * j + 3 - j, :] = lo[3 * k + j : 3 * k + 3, :]
            if j > 0:
                prim[k, 8 * j + max(3 - j, 0) : 8 * j + 3, :] = qt_ref[k, max(j - 3, 0) : j, :]
            if j < 5:
                prim[k, 8 * j + 3 : 8 * j + 3 + min(5 - j, 3), :] = qt_ref[k, nz - 5 + j : nz - 5 + j + min(5 - j, 3), :]
            if j > 2:
                prim[k, 8 * j + 8 - j : 8 * j + 6, :] = hi[3 * k : 3 * k + j - 2, :]

    def put(k, i, value):
        flux[k, rows(i), :] = value

    comps = (2, 0, 1)
    cell_pass(prim, uf, aux, 6, comps)
    diff_pass(uf, aux, cx, 4, 5, 8)
    face_pass(prim, aux, cx, 1, 8, comps, put)
    part = fz_ref.shape[1] - 8
    for k in range(5):
        fz[k, 3 : part + 3, :] = fz_ref[k, 3 : part + 3, :]
        fz[k, part + 3 : nz + 3, :] = fz2_ref[k, 3 : nz - part + 3, :]
        fz[k, 0:3, :] = flux[k, 0:3, :]
        fz[k, nz - 2 : nz + 1, :] = flux[k, 3:6, :]
        out_ref[k] = (fz[k, 1 : nz + 1, :] - fz[k, 0:nz, :]).T


def y_ends_kernel(nx, ny, block, q_ref, lo, hi, fy_ref, tz_ref, after, out_ref, prim, uf, aux, cx, flux, fy):
    sb = rup(2 * nx, 8)
    for k in range(5):
        for e in range(8):
            if e < 3:
                low = lo[(3 * k + e) * nx : (3 * k + e + 1) * nx, :]
            else:
                low = q_ref[k, pl.ds(e - 3, nx, stride=ny), :]
            if e < 5:
                high = q_ref[k, pl.ds(ny - 5 + e, nx, stride=ny), :]
            else:
                high = hi[(3 * k + e - 5) * nx : (3 * k + e - 4) * nx, :]
            prim[k, e * sb : e * sb + nx, :] = low
            prim[k, e * sb + nx : e * sb + 2 * nx, :] = high
    t = sb // 8
    comps = (1, 0, 2)
    cell_pass(prim, uf, aux, 8 * t, comps)
    diff_pass(uf, aux, cx, 6 * t, 7 * t, sb)

    def put(k, i, value):
        flux[k, rows(i), :] = value

    face_pass(prim, aux, cx, 3 * t, sb, comps, put)
    for k in range(5):
        fy[k, 0 : nx * block, :] = fy_ref[k, 0 : nx * block, :]
        for f in range(3):
            fy[k, pl.ds(f, nx, stride=block), :] = flux[k, f * sb : f * sb + nx, :]
            fy[k, pl.ds(ny - 2 + f, nx, stride=block), :] = flux[k, f * sb + nx : f * sb + 2 * nx, :]
        for x in range(nx):
            at = x * block
            here = slice(x * ny, (x + 1) * ny)
            out_ref[k, here, :] = tz_ref[k, here, :] + (fy[k, at + 1 : at + 1 + ny, :] - fy[k, at : at + ny, :])


def final_kernel(nx, ny, split, q_ref, tx_ref, rest_ref, t_ref, top_ref, out_ref):
    step = (cfl_number * KB) / top_ref[0:1, :]
    for x in range(nx):
        for lo, hi, part in ((0, split, tx_ref), (split, ny, rest_ref)):
            here = slice(x * ny + lo, x * ny + hi)
            there = slice(x * (hi - lo), (x + 1) * (hi - lo))
            rho, u1, u2, u3, p = (q_ref[k, here, :] for k in range(5))
            m1, m2, m3 = rho * u1, rho * u2, rho * u3
            energy = 2.5 * p + 0.5 * (m1 * u1 + m2 * u2 + m3 * u3)
            for k, value in enumerate((rho, m1, m2, m3, energy)):
                out_ref[k, x, lo:hi] = value - step * (part[k, there, :] + t_ref[k, here, :])


VMEM = pl.BlockSpec(memory_space=pltpu.VMEM)
HBM = pl.BlockSpec(memory_space=pltpu.HBM)
ANY = pl.BlockSpec(memory_space=pl.ANY)


def call(kernel, outs, flops, scratch=(), in_specs=None):
    extra = {} if in_specs is None else {"in_specs": in_specs}
    return pl.pallas_call(
        kernel,
        out_shape=outs,
        scratch_shapes=scratch,
        compiler_params=pltpu.CompilerParams(vmem_limit_bytes=VMEM_LIMIT),
        cost_estimate=pl.CostEstimate(flops=flops, bytes_accessed=1000000, transcendentals=0),
        **extra,
    )


def permute(value, axis, pairs):
    return lax.ppermute(value, axis, pairs)


def fields(*counts, r, w):
    return [pltpu.VMEM((count, r, w), f32) for count in counts]


def pairs_a(n):
    return [(i, i ^ 1) for i in range(n)]


def pairs_b(n):
    return [(i, (i + 1) % n if i % 2 else (i - 1) % n) for i in range(n)]


def top_over(top, axis, first):
    n = lax.axis_size(axis)
    if n & (n - 1):
        return lax.pmax(top, axis)
    d = first
    while d < n:
        top = jnp.maximum(top, permute(top, axis, [(i, i ^ d) for i in range(n)]))
        d *= 2
    return top


def with_top(edges, used, top):
    row = lax.broadcasted_iota(jnp.int32, edges.shape, 0)
    return jnp.where(row >= used, top[0:1], edges)


def got_top(top, got, row):
    return jnp.maximum(top, got[row : row + 1])


def edge_trade(axis, low, high, used, top, mids=None):
    n = lax.axis_size(axis)
    size = low.shape[0]
    if n == 1:
        return high, low, top
    if n == 2:
        got = permute(with_top(jnp.concatenate([low, high]), size + used, top), axis, [(0, 1), (1, 0)])
        return got[size:], got[:size], got_top(top, got, size + used)
    if n % 2:
        lower = permute(high, axis, [(i, (i + 1) % n) for i in range(n)])
        upper = permute(low, axis, [((i + 1) % n, i) for i in range(n)])
        return lower, upper, lax.pmax(top, axis)
    odd = lax.rem(lax.axis_index(axis), 2) == 1
    got_a = permute(with_top(jnp.where(odd, low, high), used, top), axis, pairs_a(n))
    top = got_top(top, got_a, used)
    if mids is not None:
        mids.append(top)
    got_b = permute(with_top(jnp.where(odd, high, low), used, top), axis, pairs_b(n))
    if n == 4:
        top = got_top(top, got_b, used)
    else:
        top = top_over(top, axis, 2)
    lower = jnp.where(odd, got_a, got_b)
    upper = jnp.where(odd, got_b, got_a)
    return lower, upper, top


def local(density, velocity, pressure):
    nx, ny, nz = density.shape
    n = nx * ny
    gx = lax.axis_size("gx")
    xeven = gx % 2 == 0
    width = 15 * ny
    S = jax.ShapeDtypeStruct
    density, velocity, pressure = (
        pltpu.with_memory_space_constraint(a, pltpu.HBM)
        for a in (density.reshape(n, nz), velocity.reshape(3, n, nz), pressure.reshape(n, nz))
    )
    q, xa, top = call(
        functools.partial(prepare_kernel, nx, ny, nz, xeven),
        (S((5, n + 16, nz), f32), S((width + 8, nz), f32), S((8, nz), f32)),
        2000000,
        [pltpu.SemaphoreType.DMA((5,))],
        [HBM] * 3,
    )(density, velocity, pressure)
    qt, xb, ye, ze = call(
        functools.partial(turn_kernel, nx, ny, nz, xeven),
        (
            S((5, nz + 16, n), f32),
            S((width, nz), f32),
            S((2, rup(15 * nx + 1, 8), nz), f32),
            S((2, 16, n), f32),
        ),
        2000000,
        (),
        [VMEM, ANY],
    )(q, top)

    sweep_flops = 16000000

    def inner(source, first, count, more, lanes, length, block, comps, rows_out, after):
        return call(
            functools.partial(inner_kernel, first, count, more, length, block, comps),
            S((5, rows_out, lanes), f32),
            sweep_flops,
            fields(10, 4, 25, r=8 * (count + more) + 16, w=lanes),
            [VMEM, ANY],
        )(source, after)

    if xeven:
        got_b = permute(xb, "gx", pairs_b(gx))
        got_a = permute(xa, "gx", pairs_a(gx))
        top = jnp.maximum(top, got_a[width:])
    else:
        got_a = permute(xa, "gx", [(i, (i + 1) % gx) for i in range(gx)])
        got_b = permute(xb, "gx", [((i + 1) % gx, i) for i in range(gx)])
    ztop = top if n == nz else jnp.full((8, n), jnp.max(top))
    zt = nz // 8
    half = zt // 2
    fz = [
        inner(qt, 0, half, 1, n, nz, 0, (2, 0, 1), 8 * half + 8, ye),
        inner(qt, half, zt - half, 0, n, nz, 0, (2, 0, 1), 8 * (zt - half) + 8, ztop),
    ]
    zlo, zhi, ztop = edge_trade("gz", ze[0], ze[1], 15, ztop)
    top = ztop if n == nz else jnp.full((8, nz), jnp.max(ztop))
    block = rup(ny + 6, 8)
    ytop = top
    fy = inner(q, 0, n // 8, 0, nz, ny, block, (1, 0, 2), nx * block + 16, top)
    mids = []
    ylo, yhi, top = edge_trade("gy", ye[0], ye[1], 15 * nx, top, mids)

    def along_x(first, ys, after):
        return call(
            functools.partial(x_kernel, nx, ny, first, ys, xeven),
            S((5, nx * ys, nz), f32),
            sweep_flops,
            fields(5, 10, 4, 25, 5, r=(nx + 6) * ys + 16, w=nz),
            [VMEM] * 3 + [ANY],
        )(q, got_a, got_b, after)

    split = rup(ny // 2, 8)
    tx = along_x(0, split, mids[0] if mids else top)
    tx_rest = along_x(split, ny - split, top)
    tz = call(
        functools.partial(z_ends_kernel, nz),
        S((5, n, nz), f32),
        sweep_flops // 4,
        fields(5, 10, 4, 25, 5, r=64, w=n) + [pltpu.VMEM((5, nz + 16, n), f32)],
        [VMEM] * 5 + [ANY],
    )(qt, zlo, zhi, *fz, ytop)
    t = call(
        functools.partial(y_ends_kernel, nx, ny, block),
        S((5, n, nz), f32),
        sweep_flops // 4,
        fields(5, 10, 4, 25, 5, r=8 * rup(2 * nx, 8) + 16, w=nz) + [pltpu.VMEM((5, nx * block + 16, nz), f32)],
        [VMEM] * 5 + [ANY],
    )(q, ylo, yhi, fy, tz, top)
    top = top_over(top, "gx", 2 if xeven else 1)
    return call(functools.partial(final_kernel, nx, ny, split), S((5, nx, ny, nz), f32), 1000000)(
        q, tx, tx_rest, t, top
    )


def solution(mesh):
    in_specs = (P("gx", "gy", "gz"), P(None, "gx", "gy", "gz"), P("gx", "gy", "gz"))
    out_specs = P(None, "gx", "gy", "gz")

    return jax.shard_map(local, mesh=mesh, in_specs=in_specs, out_specs=out_specs, check_vma=False)
```

```python
import functools
import math

import jax
import jax.numpy as jnp
from jax import lax
from jax.experimental import pallas as pl
from jax.experimental.pallas import tpu as pltpu
from jax.sharding import PartitionSpec as P


gamma_gas = 1.4
weno_eps = 1e-06
cfl_number = 0.4
f32 = jnp.float32

KX = math.sqrt(13.0 / 12.0)
KT = 0.5 / KX
KB = 1.0 / (6.0 * KX)
VMEM_LIMIT = 24 * 1024 * 1024


def rup(n, m):
    return (n + m - 1) // m * m


def rows(i, offset=0):
    return pl.ds(pl.multiple_of(i * 8, 8) + offset, 8)


def over(count, unroll, body):
    whole = count // unroll
    if whole:

        @pl.loop(0, whole)
        def _(j):
            for u in range(unroll):
                body(j * unroll + u)

    for i in range(whole * unroll, count):
        body(i)


def cell_pass(prim, uf, aux, count, comps, first=0):
    def body(i):
        here, there = rows(i), rows(i + first)
        rho, p = prim[0, there, :], prim[4, there, :]
        un, ut, us = (prim[1 + c, there, :] for c in comps)
        inv = 1.0 / rho
        mn, mt, ms = rho * un, rho * ut, rho * us
        mnun = mn * un
        energy = 2.5 * p + 0.5 * (mnun + mt * ut + ms * us)
        total = energy + p
        values = (rho, mn, mt, ms, energy, mn, mnun + p, mt * un, ms * un, total * un)
        for m in range(10):
            uf[m, here, :] = values[m]
        aux[0, here, :] = total * inv
        aux[1, here, :] = jnp.sqrt(rho)
        aux[3, here, :] = jnp.abs(un) + jnp.sqrt(gamma_gas * p * inv)

    over(count, 4, body)


def diff_pass(uf, aux, cx, count, pairs, s):
    def body(i):
        here = rows(i)
        for m in range(10):
            a, b, c = uf[m, here, :], uf[m, rows(i, s), :], uf[m, rows(i, 2 * s), :]
            second = (0.5 * (a + c) - b) * KX
            cx[m, here, :] = 0.25 * (c - a)
            cx[10 + m, here, :] = second
            if m >= 5:
                cx[15 + m, here, :] = (0.5 / KB) * b - (1.0 / (6.0 * KB * KX)) * second

    def pair(i):
        aux[2, rows(i), :] = jnp.maximum(aux[3, rows(i), :], aux[3, rows(i, s), :])

    over(count, 2, body)
    over(pairs, 8, pair)


def weno_excess(mid, xa, xb, xc, sign, eps):
    tau_a = xa - xb
    tau_c = xb - xc
    if sign > 0:
        mid_a = mid + KT * tau_a
        mid_c = mid + KT * tau_c
    else:
        mid_a = mid - KT * tau_a
        mid_c = mid - KT * tau_c
    sm_a = mid_a * mid_a + (xa * xa + eps)
    sm_b = mid * mid + (xb * xb + eps)
    sm_c = mid_c * mid_c + (xc * xc + eps)
    ga = 3.0 * (sm_a * sm_a)
    gb = sm_b * sm_b
    gc = sm_c * sm_c
    gc = gc + gc
    num = gb * (tau_a * gc + tau_c * ga)
    den = gb * gc + (ga + ga) * (gb + gc)
    return num / den


def characteristic(v, un, ut, us, qh, b1, ic):
    t = (qh * v[0] - un * v[1]) - (ut * v[2] + us * v[3]) + v[4]
    a = b1 * t
    n = (un * v[0] - v[1]) * ic
    return (a + n, v[0] - a, v[2] - ut * v[0], v[3] - us * v[0], a - n)


def face_average(prim, aux, i, s, comps, first):
    def at(ref, k, o):
        return ref[k, rows(i if ref is aux else i + first, o * s), :]

    rl, rr = at(aux, 1, 2), at(aux, 1, 3)
    share = rr / (rl + rr)

    def roe(ref, k):
        left, right = at(ref, k, 2), at(ref, k, 3)
        return left + share * (right - left)

    un, ut, us = (roe(prim, 1 + c) for c in comps)
    enth = roe(aux, 0)
    qh = 0.5 * (un * un + ut * ut + us * us)
    c2 = (gamma_gas - 1.0) * (enth - qh)
    ic = lax.rsqrt(c2)
    b1 = (gamma_gas - 1.0) * (ic * ic)
    alpha = jnp.maximum(jnp.maximum(at(aux, 2, 0), at(aux, 2, 2)), at(aux, 2, 4))
    return un, ut, us, enth, qh, c2 * ic, ic, b1, alpha


def face_values(get_cx, average):
    un, ut, us, enth, qh, c, ic, b1, alpha = average
    args = (un, ut, us, qh, b1, ic)
    mid_p = characteristic([get_cx(5 + m, 2) + alpha * get_cx(m, 2) for m in range(5)], *args)
    mid_m = characteristic([get_cx(5 + m, 3) - alpha * get_cx(m, 3) for m in range(5)], *args)
    xu = {o: [alpha * get_cx(10 + m, o) for m in range(5)] for o in range(1, 5)}
    xp = {}
    xm = {}
    for o in (1, 2, 3, 4):
        xf = [get_cx(15 + m, o) for m in range(5)]
        if o <= 3:
            xp[o] = characteristic([xf[m] + xu[o][m] for m in range(5)], *args)
        if o >= 2:
            xm[o] = characteristic([xf[m] - xu[o][m] for m in range(5)], *args)
    g = []
    for m in range(5):
        eps = 4.0 * weno_eps if m in (0, 4) else weno_eps
        up = weno_excess(mid_p[m], xp[1][m], xp[2][m], xp[3][m], 1, eps)
        down = weno_excess(mid_m[m], xm[4][m], xm[3][m], xm[2][m], -1, eps)
        g.append(up + down)
    h2, h3, h4 = (g[m] + g[m] for m in (1, 2, 3))
    h15 = g[0] + g[4]
    dh = c * (g[4] - g[0])
    rr = h15 + h2
    upd = (
        rr,
        un * rr + dh,
        ut * rr + h3,
        us * rr + h4,
        enth * h15 + un * dh + qh * h2 + ut * h3 + us * h4,
    )
    return [
        (get_cx(20 + m, 2) + get_cx(20 + m, 3)) + (xu[3][m] - xu[2][m]) + upd[m] for m in range(5)
    ]


def face_pass(prim, aux, cx, count, s, comps, put, first=0):
    order = (0, 1 + comps[0], 1 + comps[1], 1 + comps[2], 4)

    def step(i, average):
        ahead = face_average(prim, aux, i + 1, s, comps, first)
        values = face_values(lambda k, o: cx[k, rows(i, (o - 1) * s), :], average)
        for m in range(5):
            put(order[m], i, values[m])
        return ahead

    lax.fori_loop(0, count, step, face_average(prim, aux, 0, s, comps, first))


def prepare_kernel(nx, ny, nz, rho, vel, p, q_ref, top_ref, sems):
    n = nx * ny
    sources = (rho, vel.at[0], vel.at[1], vel.at[2], p)
    copies = [
        pltpu.make_async_copy(src, q_ref.at[k, pl.ds(0, n), :], sems.at[k])
        for k, src in enumerate(sources)
    ]
    for copy in copies:
        copy.start()
    for copy in copies:
        copy.wait()
    top = None
    for i in range(n // 8):
        here = slice(8 * i, 8 * i + 8)
        sound = jnp.sqrt(gamma_gas * q_ref[4, here, :] / q_ref[0, here, :])
        speed = (jnp.abs(q_ref[1, here, :]) + jnp.abs(q_ref[2, here, :])) + (
            jnp.abs(q_ref[3, here, :]) + 3.0 * sound
        )
        top = speed if top is None else jnp.maximum(top, speed)
    top = jnp.broadcast_to(jnp.max(top, keepdims=True), (8, nz))
    top_ref[...] = top


def edge_starts(nx, ny, xeven):
    high = (nx - 3) * ny
    if not xeven:
        return high, 0
    odd = lax.rem(lax.axis_index("gx"), 2)
    return pl.multiple_of((1 - odd) * high, 8), pl.multiple_of(odd * high, 8)


def turn_kernel(nx, ny, nz, xeven, q_ref, after, qt_ref, xa_ref, xb_ref, y_ref, z_ref):
    n = nx * ny
    for k in range(5):
        qt_ref[k, 0:nz, :] = q_ref[k, 0:n, :].T
    pad = y_ref.shape[1] - 15 * nx
    for side in (0, 1):
        if pad:
            y_ref[side, 15 * nx :, :] = jnp.zeros((pad, nz), f32)
        for k in range(5):
            for e in range(3):
                at = (3 * k + e) * nx
                row = e + side * (ny - 3)
                y_ref[side, at : at + nx, :] = q_ref[k, pl.ds(row, nx, stride=ny), :]
    width = 3 * ny
    start_a, start_b = edge_starts(nx, ny, xeven)
    for k in range(5):
        xa_ref[k * width : (k + 1) * width, :] = q_ref[k, pl.ds(start_a, width), :]
        xb_ref[k * width : (k + 1) * width, :] = q_ref[k, pl.ds(start_b, width), :]
    z_ref[...] = jnp.zeros(z_ref.shape, f32)
    for k in range(5):
        z_ref[0, 3 * k : 3 * k + 3, :] = qt_ref[k, 0:3, :]
        z_ref[1, 3 * k : 3 * k + 3, :] = qt_ref[k, nz - 3 : nz, :]


def x_kernel(nx, ny, first, ys, xeven, q_ref, a_ref, b_ref, after, out_ref, prim, uf, aux, cx, flux):
    far = (nx + 3) * ys
    if xeven:
        odd = lax.rem(lax.axis_index("gx"), 2)
        at_a = pl.multiple_of((1 - odd) * far, 8)
        at_b = pl.multiple_of(odd * far, 8)
    else:
        at_a, at_b = 0, far
    for k in range(5):
        for e in range(3):
            row = (3 * k + e) * ny + first
            prim[k, pl.ds(pl.multiple_of(at_a + e * ys, 8), ys), :] = a_ref[row : row + ys, :]
            prim[k, pl.ds(pl.multiple_of(at_b + e * ys, 8), ys), :] = b_ref[row : row + ys, :]
        for x in range(nx):
            row = x * ny + first
            prim[k, (3 + x) * ys : (4 + x) * ys, :] = q_ref[k, row : row + ys, :]
    t = ys // 8
    comps = (0, 1, 2)
    cell_pass(prim, uf, aux, (nx + 6) * t, comps)
    diff_pass(uf, aux, cx, (nx + 4) * t, (nx + 5) * t, ys)

    def put(k, i, value):
        flux[k, rows(i), :] = value

    face_pass(prim, aux, cx, (nx + 1) * t, ys, comps, put)
    n = nx * ys
    for k in range(5):
        out_ref[k] = flux[k, ys : ys + n, :] - flux[k, 0:n, :]


def inner_kernel(first, count, more, length, block, comps, q_ref, after, out_ref, uf, aux, cx):
    cell_pass(q_ref, uf, aux, count + more, comps, first)
    diff_pass(uf, aux, cx, count + more, count + more, 1)
    tiles = length // 8

    def put(k, i, value):
        if block:
            i = lax.div(i, tiles) * (block // 8) + lax.rem(i, tiles)
        out_ref[k, rows(i, 3), :] = value

    face_pass(q_ref, aux, cx, count, 1, comps, put, first)


def z_ends_kernel(nz, qt_ref, lo, hi, fz_ref, fz2_ref, after, out_ref, prim, uf, aux, cx, flux, fz):
    for k in range(5):
        prim[k] = jnp.ones(prim.shape[1:], f32)
        for j in range(6):
            if j < 3:
                prim[k, 8 * j : 8 * j + 3 - j, :] = lo[3 * k + j : 3 * k + 3, :]
            if j > 0:
                prim[k, 8 * j + max(3 - j, 0) : 8 * j + 3, :] = qt_ref[k, max(j - 3, 0) : j, :]
            if j < 5:
                prim[k, 8 * j + 3 : 8 * j + 3 + min(5 - j, 3), :] = qt_ref[k, nz - 5 + j : nz - 5 + j + min(5 - j, 3), :]
            if j > 2:
                prim[k, 8 * j + 8 - j : 8 * j + 6, :] = hi[3 * k : 3 * k + j - 2, :]

    def put(k, i, value):
        flux[k, rows(i), :] = value

    comps = (2, 0, 1)
    cell_pass(prim, uf, aux, 6, comps)
    diff_pass(uf, aux, cx, 4, 5, 8)
    face_pass(prim, aux, cx, 1, 8, comps, put)
    part = fz_ref.shape[1] - 8
    for k in range(5):
        fz[k, 3 : part + 3, :] = fz_ref[k, 3 : part + 3, :]
        fz[k, part + 3 : nz + 3, :] = fz2_ref[k, 3 : nz - part + 3, :]
        fz[k, 0:3, :] = flux[k, 0:3, :]
        fz[k, nz - 2 : nz + 1, :] = flux[k, 3:6, :]
        out_ref[k] = (fz[k, 1 : nz + 1, :] - fz[k, 0:nz, :]).T


def y_ends_kernel(nx, ny, block, q_ref, lo, hi, fy_ref, tz_ref, after, out_ref, prim, uf, aux, cx, flux, fy):
    sb = rup(2 * nx, 8)
    for k in range(5):
        for e in range(8):
            if e < 3:
                low = lo[(3 * k + e) * nx : (3 * k + e + 1) * nx, :]
            else:
                low = q_ref[k, pl.ds(e - 3, nx, stride=ny), :]
            if e < 5:
                high = q_ref[k, pl.ds(ny - 5 + e, nx, stride=ny), :]
            else:
                high = hi[(3 * k + e - 5) * nx : (3 * k + e - 4) * nx, :]
            prim[k, e * sb : e * sb + nx, :] = low
            prim[k, e * sb + nx : e * sb + 2 * nx, :] = high
    t = sb // 8
    comps = (1, 0, 2)
    cell_pass(prim, uf, aux, 8 * t, comps)
    diff_pass(uf, aux, cx, 6 * t, 7 * t, sb)

    def put(k, i, value):
        flux[k, rows(i), :] = value

    face_pass(prim, aux, cx, 3 * t, sb, comps, put)
    for k in range(5):
        fy[k, 0 : nx * block, :] = fy_ref[k, 0 : nx * block, :]
        for f in range(3):
            fy[k, pl.ds(f, nx, stride=block), :] = flux[k, f * sb : f * sb + nx, :]
            fy[k, pl.ds(ny - 2 + f, nx, stride=block), :] = flux[k, f * sb + nx : f * sb + 2 * nx, :]
        for x in range(nx):
            at = x * block
            here = slice(x * ny, (x + 1) * ny)
            out_ref[k, here, :] = tz_ref[k, here, :] + (fy[k, at + 1 : at + 1 + ny, :] - fy[k, at : at + ny, :])


def final_kernel(nx, ny, split, q_ref, tx_ref, rest_ref, t_ref, top_ref, out_ref, held, sems):
    step = (cfl_number * KB) / top_ref[7:8, :]
    copies = []
    for x in range(nx):
        for lo, hi, part in ((0, split, tx_ref), (split, ny, rest_ref)):
            here = slice(x * ny + lo, x * ny + hi)
            there = slice(x * (hi - lo), (x + 1) * (hi - lo))
            rho, u1, u2, u3, p = (q_ref[k, here, :] for k in range(5))
            m1, m2, m3 = rho * u1, rho * u2, rho * u3
            energy = 2.5 * p + 0.5 * (m1 * u1 + m2 * u2 + m3 * u3)
            for k, value in enumerate((rho, m1, m2, m3, energy)):
                held[k, x, lo:hi] = value - step * (part[k, there, :] + t_ref[k, here, :])
        copies.append(pltpu.make_async_copy(held.at[:, x], out_ref.at[:, x], sems.at[x]))
        copies[-1].start()
    for copy in copies:
        copy.wait()


VMEM = pl.BlockSpec(memory_space=pltpu.VMEM)
HBM = pl.BlockSpec(memory_space=pltpu.HBM)
ANY = pl.BlockSpec(memory_space=pl.ANY)


def call(kernel, outs, flops, scratch=(), in_specs=None, out_specs=None):
    extra = {} if in_specs is None else {"in_specs": in_specs}
    if out_specs is not None:
        extra["out_specs"] = out_specs
    return pl.pallas_call(
        kernel,
        out_shape=outs,
        scratch_shapes=scratch,
        compiler_params=pltpu.CompilerParams(vmem_limit_bytes=VMEM_LIMIT),
        cost_estimate=pl.CostEstimate(flops=flops, bytes_accessed=1000000, transcendentals=0),
        **extra,
    )


def permute(value, axis, pairs):
    return lax.ppermute(value, axis, pairs)


def fields(*counts, r, w):
    return [pltpu.VMEM((count, r, w), f32) for count in counts]


def pairs_a(n):
    return [(i, i ^ 1) for i in range(n)]


def pairs_b(n):
    return [(i, (i + 1) % n if i % 2 else (i - 1) % n) for i in range(n)]


def top_over(top, axis, first):
    n = lax.axis_size(axis)
    if n & (n - 1):
        return lax.pmax(top, axis)
    d = first
    while d < n:
        top = jnp.maximum(top, permute(top, axis, [(i, i ^ d) for i in range(n)]))
        d *= 2
    return top


def with_top(edges, used, top):
    tiles = edges.reshape(-1, 8, edges.shape[1])
    row = 8 * lax.broadcasted_iota(jnp.int32, tiles.shape, 0) + lax.broadcasted_iota(jnp.int32, tiles.shape, 1)
    return jnp.where(row >= used, top[None], tiles).reshape(edges.shape)


def got_top(top, got):
    return jnp.maximum(top, got[got.shape[0] - 8 :])


def edge_trade(axis, low, high, used, top, mids=None):
    n = lax.axis_size(axis)
    size = low.shape[0]
    if n == 1:
        return high, low, top
    if n == 2:
        got = permute(with_top(jnp.concatenate([low, high]), size + used, top), axis, [(0, 1), (1, 0)])
        return got[size:], got[:size], got_top(top, got)
    if n % 2:
        lower = permute(high, axis, [(i, (i + 1) % n) for i in range(n)])
        upper = permute(low, axis, [((i + 1) % n, i) for i in range(n)])
        return lower, upper, lax.pmax(top, axis)
    odd = lax.rem(lax.axis_index(axis), 2) == 1
    got_a = permute(with_top(jnp.where(odd, low, high), used, top), axis, pairs_a(n))
    top = got_top(top, got_a)
    if mids is not None:
        mids.append(top)
    got_b = permute(with_top(jnp.where(odd, high, low), used, top), axis, pairs_b(n))
    if n == 4:
        top = got_top(top, got_b)
    else:
        top = top_over(top, axis, 2)
    lower = jnp.where(odd, got_a, got_b)
    upper = jnp.where(odd, got_b, got_a)
    return lower, upper, top


def local(density, velocity, pressure):
    nx, ny, nz = density.shape
    n = nx * ny
    gx = lax.axis_size("gx")
    xeven = gx % 2 == 0
    width = 15 * ny
    S = jax.ShapeDtypeStruct
    density, velocity, pressure = (
        pltpu.with_memory_space_constraint(a, pltpu.HBM)
        for a in (density.reshape(n, nz), velocity.reshape(3, n, nz), pressure.reshape(n, nz))
    )
    q, top = call(
        functools.partial(prepare_kernel, nx, ny, nz),
        (S((5, n + 16, nz), f32), S((8, nz), f32)),
        2000000,
        [pltpu.SemaphoreType.DMA((5,))],
        [HBM] * 3,
    )(density, velocity, pressure)
    qt, xa, xb, ye, ze = call(
        functools.partial(turn_kernel, nx, ny, nz, xeven),
        (
            S((5, nz + 16, n), f32),
            S((width, nz), f32),
            S((width, nz), f32),
            S((2, rup(15 * nx + 1, 8), nz), f32),
            S((2, 16, n), f32),
        ),
        2000000,
        (),
        [VMEM, ANY],
    )(q, top)

    sweep_flops = 16000000

    def inner(source, first, count, more, lanes, length, block, comps, rows_out, after):
        return call(
            functools.partial(inner_kernel, first, count, more, length, block, comps),
            S((5, rows_out, lanes), f32),
            sweep_flops,
            fields(10, 4, 25, r=8 * (count + more) + 16, w=lanes),
            [VMEM, ANY],
        )(source, after)

    if xeven:
        got_b = permute(xb, "gx", pairs_b(gx))
        got_a = permute(xa, "gx", pairs_a(gx))
        top = jnp.maximum(top, permute(top, "gx", pairs_a(gx)))
    else:
        got_a = permute(xa, "gx", [(i, (i + 1) % gx) for i in range(gx)])
        got_b = permute(xb, "gx", [((i + 1) % gx, i) for i in range(gx)])
    ztop = top if n == nz else jnp.full((8, n), jnp.max(top[7]))
    zt = nz // 8
    half = max(zt * 7 // 16, 1)
    fz = [
        inner(qt, 0, half, 1, n, nz, 0, (2, 0, 1), 8 * half + 8, ye),
        inner(qt, half, zt - half, 0, n, nz, 0, (2, 0, 1), 8 * (zt - half) + 8, ztop),
    ]
    zlo, zhi, ztop = edge_trade("gz", ze[0], ze[1], 15, ztop)
    top = ztop if n == nz else jnp.full((8, nz), jnp.max(ztop[7]))
    block = rup(ny + 6, 8)
    fy = inner(q, 0, n // 8, 0, nz, ny, block, (1, 0, 2), nx * block + 16, top)
    mids = []
    ylo, yhi, top = edge_trade("gy", ye[0], ye[1], 15 * nx, top, mids)

    def along_x(first, ys, after):
        return call(
            functools.partial(x_kernel, nx, ny, first, ys, xeven),
            S((5, nx * ys, nz), f32),
            sweep_flops,
            fields(5, 10, 4, 25, 5, r=(nx + 6) * ys + 16, w=nz),
            [VMEM] * 3 + [ANY],
        )(q, got_a, got_b, after)

    split = rup(ny // 2, 8)
    tx = along_x(0, split, mids[0] if mids else top)
    tx_rest = along_x(split, ny - split, top)
    tz = call(
        functools.partial(z_ends_kernel, nz),
        S((5, n, nz), f32),
        sweep_flops // 4,
        fields(5, 10, 4, 25, 5, r=64, w=n) + [pltpu.VMEM((5, nz + 16, n), f32)],
        [VMEM] * 5 + [ANY],
    )(qt, zlo, zhi, *fz, mids[0] if mids else top)
    t = call(
        functools.partial(y_ends_kernel, nx, ny, block),
        S((5, n, nz), f32),
        sweep_flops // 4,
        fields(5, 10, 4, 25, 5, r=8 * rup(2 * nx, 8) + 16, w=nz) + [pltpu.VMEM((5, nx * block + 16, nz), f32)],
        [VMEM] * 5 + [ANY],
    )(q, ylo, yhi, fy, tz, top)
    top = top_over(top, "gx", 2 if xeven else 1)
    out = S((5, nx, ny, nz), f32)
    return call(
        functools.partial(final_kernel, nx, ny, split),
        out,
        1000000,
        [pltpu.VMEM(out.shape, f32), pltpu.SemaphoreType.DMA((nx,))],
        [VMEM] * 5,
        HBM,
    )(q, tx, tx_rest, t, top)


def solution(mesh):
    in_specs = (P("gx", "gy", "gz"), P(None, "gx", "gy", "gz"), P("gx", "gy", "gz"))
    out_specs = P(None, "gx", "gy", "gz")

    return jax.shard_map(local, mesh=mesh, in_specs=in_specs, out_specs=out_specs, check_vma=False)
```

```python
import functools
import math

import jax
import jax.numpy as jnp
from jax import lax
from jax.experimental import pallas as pl
from jax.experimental.pallas import tpu as pltpu
from jax.sharding import PartitionSpec as P


gamma_gas = 1.4
weno_eps = 1e-06
cfl_number = 0.4
f32 = jnp.float32

KX = math.sqrt(13.0 / 12.0)
KT = 0.5 / KX
KB = 1.0 / (6.0 * KX)
VMEM_LIMIT = 24 * 1024 * 1024


def rup(n, m):
    return (n + m - 1) // m * m


def rows(i, offset=0):
    return pl.ds(pl.multiple_of(i * 8, 8) + offset, 8)


def over(count, unroll, body):
    whole = count // unroll
    if whole:

        @pl.loop(0, whole)
        def _(j):
            for u in range(unroll):
                body(j * unroll + u)

    for i in range(whole * unroll, count):
        body(i)


def cell_pass(prim, uf, aux, count, comps, first=0):
    def body(i):
        here, there = rows(i), rows(i + first)
        rho, p = prim[0, there, :], prim[4, there, :]
        un, ut, us = (prim[1 + c, there, :] for c in comps)
        inv = 1.0 / rho
        mn, mt, ms = rho * un, rho * ut, rho * us
        mnun = mn * un
        energy = 2.5 * p + 0.5 * (mnun + mt * ut + ms * us)
        total = energy + p
        values = (rho, mn, mt, ms, energy, mn, mnun + p, mt * un, ms * un, total * un)
        for m in range(10):
            uf[m, here, :] = values[m]
        aux[0, here, :] = total * inv
        aux[1, here, :] = jnp.sqrt(rho)
        aux[3, here, :] = jnp.abs(un) + jnp.sqrt(gamma_gas * p * inv)

    over(count, 4, body)


def diff_pass(uf, aux, cx, count, pairs, s):
    def body(i):
        here = rows(i)
        for m in range(10):
            a, b, c = uf[m, here, :], uf[m, rows(i, s), :], uf[m, rows(i, 2 * s), :]
            second = (0.5 * (a + c) - b) * KX
            cx[m, here, :] = 0.25 * (c - a)
            cx[10 + m, here, :] = second
            if m >= 5:
                cx[15 + m, here, :] = (0.5 / KB) * b - (1.0 / (6.0 * KB * KX)) * second

    def pair(i):
        aux[2, rows(i), :] = jnp.maximum(aux[3, rows(i), :], aux[3, rows(i, s), :])

    over(count, 2, body)
    over(pairs, 8, pair)


def weno_excess(mid, xa, xb, xc, sign, eps):
    tau_a = xa - xb
    tau_c = xb - xc
    if sign > 0:
        mid_a = mid + KT * tau_a
        mid_c = mid + KT * tau_c
    else:
        mid_a = mid - KT * tau_a
        mid_c = mid - KT * tau_c
    sm_a = mid_a * mid_a + (xa * xa + eps)
    sm_b = mid * mid + (xb * xb + eps)
    sm_c = mid_c * mid_c + (xc * xc + eps)
    ga = 3.0 * (sm_a * sm_a)
    gb = sm_b * sm_b
    gc = sm_c * sm_c
    gc = gc + gc
    num = gb * (tau_a * gc + tau_c * ga)
    den = gb * gc + (ga + ga) * (gb + gc)
    return num / den


def characteristic(v, un, ut, us, qh, b1, ic):
    t = (qh * v[0] - un * v[1]) - (ut * v[2] + us * v[3]) + v[4]
    a = b1 * t
    n = (un * v[0] - v[1]) * ic
    return (a + n, v[0] - a, v[2] - ut * v[0], v[3] - us * v[0], a - n)


def face_average(prim, aux, i, s, comps, first):
    def at(ref, k, o):
        return ref[k, rows(i if ref is aux else i + first, o * s), :]

    rl, rr = at(aux, 1, 2), at(aux, 1, 3)
    share = rr / (rl + rr)

    def roe(ref, k):
        left, right = at(ref, k, 2), at(ref, k, 3)
        return left + share * (right - left)

    un, ut, us = (roe(prim, 1 + c) for c in comps)
    enth = roe(aux, 0)
    qh = 0.5 * (un * un + ut * ut + us * us)
    c2 = (gamma_gas - 1.0) * (enth - qh)
    ic = lax.rsqrt(c2)
    b1 = (gamma_gas - 1.0) * (ic * ic)
    alpha = jnp.maximum(jnp.maximum(at(aux, 2, 0), at(aux, 2, 2)), at(aux, 2, 4))
    return un, ut, us, enth, qh, c2 * ic, ic, b1, alpha


def face_values(get_cx, average):
    un, ut, us, enth, qh, c, ic, b1, alpha = average
    args = (un, ut, us, qh, b1, ic)
    mid_p = characteristic([get_cx(5 + m, 2) + alpha * get_cx(m, 2) for m in range(5)], *args)
    mid_m = characteristic([get_cx(5 + m, 3) - alpha * get_cx(m, 3) for m in range(5)], *args)
    xu = {o: [alpha * get_cx(10 + m, o) for m in range(5)] for o in range(1, 5)}
    xp = {}
    xm = {}
    for o in (1, 2, 3, 4):
        xf = [get_cx(15 + m, o) for m in range(5)]
        if o <= 3:
            xp[o] = characteristic([xf[m] + xu[o][m] for m in range(5)], *args)
        if o >= 2:
            xm[o] = characteristic([xf[m] - xu[o][m] for m in range(5)], *args)
    g = []
    for m in range(5):
        eps = 4.0 * weno_eps if m in (0, 4) else weno_eps
        up = weno_excess(mid_p[m], xp[1][m], xp[2][m], xp[3][m], 1, eps)
        down = weno_excess(mid_m[m], xm[4][m], xm[3][m], xm[2][m], -1, eps)
        g.append(up + down)
    h2, h3, h4 = (g[m] + g[m] for m in (1, 2, 3))
    h15 = g[0] + g[4]
    dh = c * (g[4] - g[0])
    rr = h15 + h2
    upd = (
        rr,
        un * rr + dh,
        ut * rr + h3,
        us * rr + h4,
        enth * h15 + un * dh + qh * h2 + ut * h3 + us * h4,
    )
    return [
        (get_cx(20 + m, 2) + get_cx(20 + m, 3)) + (xu[3][m] - xu[2][m]) + upd[m] for m in range(5)
    ]


def face_pass(prim, aux, cx, count, s, comps, put, first=0):
    order = (0, 1 + comps[0], 1 + comps[1], 1 + comps[2], 4)

    def step(i, average):
        ahead = face_average(prim, aux, i + 1, s, comps, first)
        values = face_values(lambda k, o: cx[k, rows(i, (o - 1) * s), :], average)
        for m in range(5):
            put(order[m], i, values[m])
        return ahead

    lax.fori_loop(0, count, step, face_average(prim, aux, 0, s, comps, first))


def prepare_kernel(nx, ny, nz, rho, vel, p, q_ref, top_ref, sems):
    n = nx * ny
    sources = (rho, vel.at[0], vel.at[1], vel.at[2], p)
    copies = [
        pltpu.make_async_copy(src, q_ref.at[k, pl.ds(0, n), :], sems.at[k])
        for k, src in enumerate(sources)
    ]
    for copy in copies:
        copy.start()
    for copy in copies:
        copy.wait()
    top = None
    for i in range(n // 8):
        here = slice(8 * i, 8 * i + 8)
        sound = jnp.sqrt(gamma_gas * q_ref[4, here, :] / q_ref[0, here, :])
        speed = (jnp.abs(q_ref[1, here, :]) + jnp.abs(q_ref[2, here, :])) + (
            jnp.abs(q_ref[3, here, :]) + 3.0 * sound
        )
        top = speed if top is None else jnp.maximum(top, speed)
    top = jnp.broadcast_to(jnp.max(top, keepdims=True), (8, nz))
    top_ref[...] = top


def edge_starts(nx, ny, xeven):
    high = (nx - 3) * ny
    if not xeven:
        return high, 0
    odd = lax.rem(lax.axis_index("gx"), 2)
    return pl.multiple_of((1 - odd) * high, 8), pl.multiple_of(odd * high, 8)


def slots(axis):
    n = lax.axis_size(axis)
    if n % 2 or n < 4:
        return 0, 1
    odd = lax.rem(lax.axis_index(axis), 2)
    return 1 - odd, odd


def turn_kernel(nx, ny, nz, xeven, q_ref, after, qt_ref, xa_ref, xb_ref, y_ref, z_ref, free_ref):
    n = nx * ny
    for k in range(5):
        qt_ref[k, 0:nz, :] = q_ref[k, 0:n, :].T
    size = y_ref.shape[1]
    for slot, side in zip(slots("gy"), (0, 1)):
        y_ref[slot, size - 8 :, :] = jnp.zeros((8, nz), f32)
        for k in range(5):
            for e in range(3):
                at = (3 * k + e) * nx
                row = e + side * (ny - 3)
                y_ref[slot, at : at + nx, :] = q_ref[k, pl.ds(row, nx, stride=ny), :]
    width = 3 * ny
    start_a, start_b = edge_starts(nx, ny, xeven)
    for k in range(5):
        xa_ref[k * width : (k + 1) * width, :] = q_ref[k, pl.ds(start_a, width), :]
        xb_ref[k * width : (k + 1) * width, :] = q_ref[k, pl.ds(start_b, width), :]
    for slot, at in zip(slots("gz"), (0, nz - 3)):
        z_ref[slot, 8:16, :] = jnp.zeros((8, n), f32)
        for k in range(5):
            z_ref[slot, 3 * k : 3 * k + 3, :] = qt_ref[k, at : at + 3, :]
    row = lax.broadcasted_iota(jnp.int32, free_ref.shape, 0)
    free_ref[...] = jnp.where(row == 7, 1.0, 0.0).astype(f32)


def x_kernel(nx, ny, first, ys, xeven, q_ref, a_ref, b_ref, after, out_ref, prim, uf, aux, cx, flux):
    far = (nx + 3) * ys
    if xeven:
        odd = lax.rem(lax.axis_index("gx"), 2)
        at_a = pl.multiple_of((1 - odd) * far, 8)
        at_b = pl.multiple_of(odd * far, 8)
    else:
        at_a, at_b = 0, far
    for k in range(5):
        for e in range(3):
            row = (3 * k + e) * ny + first
            prim[k, pl.ds(pl.multiple_of(at_a + e * ys, 8), ys), :] = a_ref[row : row + ys, :]
            prim[k, pl.ds(pl.multiple_of(at_b + e * ys, 8), ys), :] = b_ref[row : row + ys, :]
        for x in range(nx):
            row = x * ny + first
            prim[k, (3 + x) * ys : (4 + x) * ys, :] = q_ref[k, row : row + ys, :]
    t = ys // 8
    comps = (0, 1, 2)
    cell_pass(prim, uf, aux, (nx + 6) * t, comps)
    diff_pass(uf, aux, cx, (nx + 4) * t, (nx + 5) * t, ys)

    def put(k, i, value):
        flux[k, rows(i), :] = value

    face_pass(prim, aux, cx, (nx + 1) * t, ys, comps, put)
    n = nx * ys
    for k in range(5):
        out_ref[k] = flux[k, ys : ys + n, :] - flux[k, 0:n, :]


def inner_kernel(first, count, more, length, block, comps, q_ref, after, out_ref, uf, aux, cx):
    cell_pass(q_ref, uf, aux, count + more, comps, first)
    diff_pass(uf, aux, cx, count + more, count + more, 1)
    tiles = length // 8

    def put(k, i, value):
        if block:
            i = lax.div(i, tiles) * (block // 8) + lax.rem(i, tiles)
        out_ref[k, rows(i, 3), :] = value

    face_pass(q_ref, aux, cx, count, 1, comps, put, first)


def z_ends_kernel(nz, qt_ref, lo, hi, fz_ref, fz2_ref, after, out_ref, prim, uf, aux, cx, flux, fz):
    for k in range(5):
        prim[k] = jnp.ones(prim.shape[1:], f32)
        for j in range(6):
            if j < 3:
                prim[k, 8 * j : 8 * j + 3 - j, :] = lo[3 * k + j : 3 * k + 3, :]
            if j > 0:
                prim[k, 8 * j + max(3 - j, 0) : 8 * j + 3, :] = qt_ref[k, max(j - 3, 0) : j, :]
            if j < 5:
                prim[k, 8 * j + 3 : 8 * j + 3 + min(5 - j, 3), :] = qt_ref[k, nz - 5 + j : nz - 5 + j + min(5 - j, 3), :]
            if j > 2:
                prim[k, 8 * j + 8 - j : 8 * j + 6, :] = hi[3 * k : 3 * k + j - 2, :]

    def put(k, i, value):
        flux[k, rows(i), :] = value

    comps = (2, 0, 1)
    cell_pass(prim, uf, aux, 6, comps)
    diff_pass(uf, aux, cx, 4, 5, 8)
    face_pass(prim, aux, cx, 1, 8, comps, put)
    a = fz_ref.shape[1] - 8
    b = a + fz2_ref.shape[1] - 8
    count = (nz - b) // 8

    def put_inner(k, i, value):
        fz[k, rows(i + b // 8, 3), :] = value

    cell_pass(qt_ref, uf, aux, count, comps, b // 8)
    diff_pass(uf, aux, cx, count, count, 1)
    face_pass(qt_ref, aux, cx, count, 1, comps, put_inner, b // 8)
    for k in range(5):
        fz[k, 3 : a + 3, :] = fz_ref[k, 3 : a + 3, :]
        fz[k, a + 3 : b + 3, :] = fz2_ref[k, 3 : b - a + 3, :]
        fz[k, 0:3, :] = flux[k, 0:3, :]
        fz[k, nz - 2 : nz + 1, :] = flux[k, 3:6, :]
        out_ref[k] = (fz[k, 1 : nz + 1, :] - fz[k, 0:nz, :]).T


def y_ends_kernel(nx, ny, block, q_ref, lo, hi, fy_ref, tz_ref, after, out_ref, prim, uf, aux, cx, flux, fy):
    sb = rup(2 * nx, 8)
    for k in range(5):
        for e in range(8):
            if e < 3:
                low = lo[(3 * k + e) * nx : (3 * k + e + 1) * nx, :]
            else:
                low = q_ref[k, pl.ds(e - 3, nx, stride=ny), :]
            if e < 5:
                high = q_ref[k, pl.ds(ny - 5 + e, nx, stride=ny), :]
            else:
                high = hi[(3 * k + e - 5) * nx : (3 * k + e - 4) * nx, :]
            prim[k, e * sb : e * sb + nx, :] = low
            prim[k, e * sb + nx : e * sb + 2 * nx, :] = high
    t = sb // 8
    comps = (1, 0, 2)
    cell_pass(prim, uf, aux, 8 * t, comps)
    diff_pass(uf, aux, cx, 6 * t, 7 * t, sb)

    def put(k, i, value):
        flux[k, rows(i), :] = value

    face_pass(prim, aux, cx, 3 * t, sb, comps, put)
    for k in range(5):
        fy[k, 0 : nx * block, :] = fy_ref[k, 0 : nx * block, :]
        for f in range(3):
            fy[k, pl.ds(f, nx, stride=block), :] = flux[k, f * sb : f * sb + nx, :]
            fy[k, pl.ds(ny - 2 + f, nx, stride=block), :] = flux[k, f * sb + nx : f * sb + 2 * nx, :]
        for x in range(nx):
            at = x * block
            here = slice(x * ny, (x + 1) * ny)
            out_ref[k, here, :] = tz_ref[k, here, :] + (fy[k, at + 1 : at + 1 + ny, :] - fy[k, at : at + ny, :])


def final_kernel(nx, ny, split, q_ref, tx_ref, rest_ref, t_ref, top_ref, out_ref, held, sems):
    step = (cfl_number * KB) / top_ref[7:8, :]
    copies = []
    for x in range(nx):
        for lo, hi, part in ((0, split, tx_ref), (split, ny, rest_ref)):
            here = slice(x * ny + lo, x * ny + hi)
            there = slice(x * (hi - lo), (x + 1) * (hi - lo))
            rho, u1, u2, u3, p = (q_ref[k, here, :] for k in range(5))
            m1, m2, m3 = rho * u1, rho * u2, rho * u3
            energy = 2.5 * p + 0.5 * (m1 * u1 + m2 * u2 + m3 * u3)
            for k, value in enumerate((rho, m1, m2, m3, energy)):
                held[k, x, lo:hi] = value - step * (part[k, there, :] + t_ref[k, here, :])
        copies.append(pltpu.make_async_copy(held.at[:, x], out_ref.at[:, x], sems.at[x]))
        copies[-1].start()
    for copy in copies:
        copy.wait()


VMEM = pl.BlockSpec(memory_space=pltpu.VMEM)
HBM = pl.BlockSpec(memory_space=pltpu.HBM)
ANY = pl.BlockSpec(memory_space=pl.ANY)


def call(kernel, outs, flops, scratch=(), in_specs=None, out_specs=None):
    extra = {} if in_specs is None else {"in_specs": in_specs}
    if out_specs is not None:
        extra["out_specs"] = out_specs
    return pl.pallas_call(
        kernel,
        out_shape=outs,
        scratch_shapes=scratch,
        compiler_params=pltpu.CompilerParams(vmem_limit_bytes=VMEM_LIMIT),
        cost_estimate=pl.CostEstimate(flops=flops, bytes_accessed=1000000, transcendentals=0),
        **extra,
    )


def fields(*counts, r, w):
    return [pltpu.VMEM((count, r, w), f32) for count in counts]


def pairs_a(n):
    return [(i, i ^ 1) for i in range(n)]


def pairs_b(n):
    return [(i, (i + 1) % n if i % 2 else (i - 1) % n) for i in range(n)]


def top_over(top, axis, first):
    n = lax.axis_size(axis)
    if n & (n - 1):
        return lax.pmax(top, axis)
    d = first
    while d < n:
        top = jnp.maximum(top, lax.ppermute(top, axis, [(i, i ^ d) for i in range(n)]))
        d *= 2
    return top


def with_top(edges, free, top):
    at = edges.shape[0] - 8
    return jnp.concatenate([edges[:at], edges[at:] + free * top])


def got_top(top, got):
    return jnp.maximum(top, got[got.shape[0] - 8 :])


def edge_trade(axis, edges, free, top, mids=None):
    n = lax.axis_size(axis)
    first, second = edges[0], edges[1]
    size = first.shape[0]
    if n == 1:
        return second, first, top
    if n == 2:
        got = lax.ppermute(with_top(edges.reshape(2 * size, -1), free, top), axis, [(0, 1), (1, 0)])
        return got[size:], got[:size], got_top(top, got)
    if n % 2:
        lower = lax.ppermute(second, axis, [(i, (i + 1) % n) for i in range(n)])
        upper = lax.ppermute(first, axis, [((i + 1) % n, i) for i in range(n)])
        return lower, upper, lax.pmax(top, axis)
    odd = lax.rem(lax.axis_index(axis), 2) == 1
    got_a = lax.ppermute(with_top(first, free, top), axis, pairs_a(n))
    top = got_top(top, got_a)
    if mids is not None:
        mids.append(top)
    got_b = lax.ppermute(with_top(second, free, top), axis, pairs_b(n))
    if n == 4:
        top = got_top(top, got_b)
    else:
        top = top_over(top, axis, 2)
    lower = jnp.where(odd, got_a, got_b)
    upper = jnp.where(odd, got_b, got_a)
    return lower, upper, top


def local(density, velocity, pressure):
    nx, ny, nz = density.shape
    n = nx * ny
    gx = lax.axis_size("gx")
    xeven = gx % 2 == 0
    width = 15 * ny
    S = jax.ShapeDtypeStruct
    density, velocity, pressure = (
        pltpu.with_memory_space_constraint(a, pltpu.HBM)
        for a in (density.reshape(n, nz), velocity.reshape(3, n, nz), pressure.reshape(n, nz))
    )
    q, top = call(
        functools.partial(prepare_kernel, nx, ny, nz),
        (S((5, n + 16, nz), f32), S((8, nz), f32)),
        2000000,
        [pltpu.SemaphoreType.DMA((5,))],
        [HBM] * 3,
    )(density, velocity, pressure)
    qt, xa, xb, ye, ze, free = call(
        functools.partial(turn_kernel, nx, ny, nz, xeven),
        (
            S((5, nz + 16, n), f32),
            S((width, nz), f32),
            S((width, nz), f32),
            S((2, rup(15 * nx + 1, 8), nz), f32),
            S((2, 16, n), f32),
            S((8, nz), f32),
        ),
        2000000,
        (),
        [VMEM, ANY],
    )(q, top)

    sweep_flops = 16000000

    def inner(source, first, count, more, lanes, length, block, comps, rows_out, after):
        return call(
            functools.partial(inner_kernel, first, count, more, length, block, comps),
            S((5, rows_out, lanes), f32),
            sweep_flops,
            fields(10, 4, 25, r=8 * (count + more) + 16, w=lanes),
            [VMEM, ANY],
        )(source, after)

    if xeven:
        got_b = lax.ppermute(xb, "gx", pairs_b(gx))
        got_a = lax.ppermute(xa, "gx", pairs_a(gx))
        top = jnp.maximum(top, lax.ppermute(top, "gx", pairs_a(gx)))
    else:
        got_a = lax.ppermute(xa, "gx", [(i, (i + 1) % gx) for i in range(gx)])
        got_b = lax.ppermute(xb, "gx", [((i + 1) % gx, i) for i in range(gx)])
    ztop = top if n == nz else jnp.full((8, n), jnp.max(top[7]))
    zt = nz // 8
    za, zb = zt * 7 // 16, zt * 6 // 16
    fz = [
        inner(qt, 0, za, 1, n, nz, 0, (2, 0, 1), 8 * za + 8, ye),
        inner(qt, za, zb, 1, n, nz, 0, (2, 0, 1), 8 * zb + 8, ztop),
    ]
    zlo, zhi, ztop = edge_trade("gz", ze, free if n == nz else jnp.broadcast_to(free[:, :1], (8, n)), ztop)
    top = ztop if n == nz else jnp.full((8, nz), jnp.max(ztop[7]))
    block = rup(ny + 6, 8)
    fy = inner(q, 0, n // 8, 0, nz, ny, block, (1, 0, 2), nx * block + 16, top)
    mids = []
    ylo, yhi, top = edge_trade("gy", ye, free, top, mids)

    def along_x(first, ys, after):
        return call(
            functools.partial(x_kernel, nx, ny, first, ys, xeven),
            S((5, nx * ys, nz), f32),
            sweep_flops,
            fields(5, 10, 4, 25, 5, r=(nx + 6) * ys + 16, w=nz),
            [VMEM] * 3 + [ANY],
        )(q, got_a, got_b, after)

    split = rup(ny // 2, 8)
    tx = along_x(0, split, mids[0] if mids else top)
    tx_rest = along_x(split, ny - split, top)
    tz = call(
        functools.partial(z_ends_kernel, nz),
        S((5, n, nz), f32),
        sweep_flops // 4,
        fields(5, 10, 4, 25, 5, r=64, w=n) + [pltpu.VMEM((5, nz + 16, n), f32)],
        [VMEM] * 5 + [ANY],
    )(qt, zlo, zhi, *fz, mids[0] if mids else top)
    t = call(
        functools.partial(y_ends_kernel, nx, ny, block),
        S((5, n, nz), f32),
        sweep_flops // 4,
        fields(5, 10, 4, 25, 5, r=8 * rup(2 * nx, 8) + 16, w=nz) + [pltpu.VMEM((5, nx * block + 16, nz), f32)],
        [VMEM] * 5 + [ANY],
    )(q, ylo, yhi, fy, tz, top)
    top = top_over(top, "gx", 2 if xeven else 1)
    out = S((5, nx, ny, nz), f32)
    return call(
        functools.partial(final_kernel, nx, ny, split),
        out,
        1000000,
        [pltpu.VMEM(out.shape, f32), pltpu.SemaphoreType.DMA((nx,))],
        [VMEM] * 5,
        HBM,
    )(q, tx, tx_rest, t, top)


def solution(mesh):
    in_specs = (P("gx", "gy", "gz"), P(None, "gx", "gy", "gz"), P("gx", "gy", "gz"))
    out_specs = P(None, "gx", "gy", "gz")

    return jax.shard_map(local, mesh=mesh, in_specs=in_specs, out_specs=out_specs, check_vma=False)
```

```python
import functools
import math

import jax
import jax.numpy as jnp
from jax import lax
from jax.experimental import pallas as pl
from jax.experimental.pallas import tpu as pltpu
from jax.sharding import PartitionSpec as P


gamma_gas = 1.4
weno_eps = 1e-06
cfl_number = 0.4
f32 = jnp.float32

KX = math.sqrt(13.0 / 12.0)
KT = 0.5 / KX
KB = 1.0 / (6.0 * KX)
VMEM_LIMIT = 24 * 1024 * 1024


def rup(n, m):
    return (n + m - 1) // m * m


def rows(i, offset=0):
    return pl.ds(pl.multiple_of(i * 8, 8) + offset, 8)


def over(count, unroll, body):
    whole = count // unroll
    if whole:

        @pl.loop(0, whole)
        def _(j):
            for u in range(unroll):
                body(j * unroll + u)

    for i in range(whole * unroll, count):
        body(i)


def cell_pass(prim, uf, aux, count, comps, first=0):
    def body(i):
        here, there = rows(i), rows(i + first)
        rho, p = prim[0, there, :], prim[4, there, :]
        un, ut, us = (prim[1 + c, there, :] for c in comps)
        inv = 1.0 / rho
        mn, mt, ms = rho * un, rho * ut, rho * us
        mnun = mn * un
        energy = 2.5 * p + 0.5 * (mnun + mt * ut + ms * us)
        total = energy + p
        values = (rho, mn, mt, ms, energy, mn, mnun + p, mt * un, ms * un, total * un)
        for m in range(10):
            uf[m, here, :] = values[m]
        aux[0, here, :] = total * inv
        aux[1, here, :] = jnp.sqrt(rho)
        aux[3, here, :] = jnp.abs(un) + jnp.sqrt(gamma_gas * p * inv)

    over(count, 4, body)


def diff_pass(uf, aux, cx, count, pairs, s):
    def body(i):
        here = rows(i)
        for m in range(10):
            a, b, c = uf[m, here, :], uf[m, rows(i, s), :], uf[m, rows(i, 2 * s), :]
            second = (0.5 * (a + c) - b) * KX
            cx[m, here, :] = 0.25 * (c - a)
            cx[10 + m, here, :] = second
            if m >= 5:
                cx[15 + m, here, :] = (0.5 / KB) * b - (1.0 / (6.0 * KB * KX)) * second

    def pair(i):
        aux[2, rows(i), :] = jnp.maximum(aux[3, rows(i), :], aux[3, rows(i, s), :])

    over(count, 2, body)
    over(pairs, 8, pair)


def weno_excess(mid, xa, xb, xc, sign, eps):
    tau_a = xa - xb
    tau_c = xb - xc
    if sign > 0:
        mid_a = mid + KT * tau_a
        mid_c = mid + KT * tau_c
    else:
        mid_a = mid - KT * tau_a
        mid_c = mid - KT * tau_c
    sm_a = mid_a * mid_a + (xa * xa + eps)
    sm_b = mid * mid + (xb * xb + eps)
    sm_c = mid_c * mid_c + (xc * xc + eps)
    ga = 3.0 * (sm_a * sm_a)
    gb = sm_b * sm_b
    gc = sm_c * sm_c
    gc = gc + gc
    num = gb * (tau_a * gc + tau_c * ga)
    den = gb * gc + (ga + ga) * (gb + gc)
    return num / den


def characteristic(v, un, ut, us, qh, b1, ic):
    t = (qh * v[0] - un * v[1]) - (ut * v[2] + us * v[3]) + v[4]
    a = b1 * t
    n = (un * v[0] - v[1]) * ic
    return (a + n, v[0] - a, v[2] - ut * v[0], v[3] - us * v[0], a - n)


def face_average(prim, aux, i, s, comps, first):
    def at(ref, k, o):
        return ref[k, rows(i if ref is aux else i + first, o * s), :]

    rl, rr = at(aux, 1, 2), at(aux, 1, 3)
    share = rr / (rl + rr)

    def roe(ref, k):
        left, right = at(ref, k, 2), at(ref, k, 3)
        return left + share * (right - left)

    un, ut, us = (roe(prim, 1 + c) for c in comps)
    enth = roe(aux, 0)
    qh = 0.5 * (un * un + ut * ut + us * us)
    c2 = (gamma_gas - 1.0) * (enth - qh)
    ic = lax.rsqrt(c2)
    b1 = (gamma_gas - 1.0) * (ic * ic)
    alpha = jnp.maximum(jnp.maximum(at(aux, 2, 0), at(aux, 2, 2)), at(aux, 2, 4))
    return un, ut, us, enth, qh, c2 * ic, ic, b1, alpha


def face_values(get_cx, average):
    un, ut, us, enth, qh, c, ic, b1, alpha = average
    args = (un, ut, us, qh, b1, ic)
    mid_p = characteristic([get_cx(5 + m, 2) + alpha * get_cx(m, 2) for m in range(5)], *args)
    mid_m = characteristic([get_cx(5 + m, 3) - alpha * get_cx(m, 3) for m in range(5)], *args)
    xu = {o: [alpha * get_cx(10 + m, o) for m in range(5)] for o in range(1, 5)}
    xp = {}
    xm = {}
    for o in (1, 2, 3, 4):
        xf = [get_cx(15 + m, o) for m in range(5)]
        if o <= 3:
            xp[o] = characteristic([xf[m] + xu[o][m] for m in range(5)], *args)
        if o >= 2:
            xm[o] = characteristic([xf[m] - xu[o][m] for m in range(5)], *args)
    g = []
    for m in range(5):
        eps = 4.0 * weno_eps if m in (0, 4) else weno_eps
        up = weno_excess(mid_p[m], xp[1][m], xp[2][m], xp[3][m], 1, eps)
        down = weno_excess(mid_m[m], xm[4][m], xm[3][m], xm[2][m], -1, eps)
        g.append(up + down)
    h2, h3, h4 = (g[m] + g[m] for m in (1, 2, 3))
    h15 = g[0] + g[4]
    dh = c * (g[4] - g[0])
    rr = h15 + h2
    upd = (
        rr,
        un * rr + dh,
        ut * rr + h3,
        us * rr + h4,
        enth * h15 + un * dh + qh * h2 + ut * h3 + us * h4,
    )
    return [
        (get_cx(20 + m, 2) + get_cx(20 + m, 3)) + (xu[3][m] - xu[2][m]) + upd[m] for m in range(5)
    ]


def face_pass(prim, aux, cx, count, s, comps, put, first=0):
    order = (0, 1 + comps[0], 1 + comps[1], 1 + comps[2], 4)

    def step(i, average):
        ahead = face_average(prim, aux, i + 1, s, comps, first)
        values = face_values(lambda k, o: cx[k, rows(i, (o - 1) * s), :], average)
        for m in range(5):
            put(order[m], i, values[m])
        return ahead

    def steps(j, average):
        for u in range(2):
            average = step(2 * j + u, average)
        return average

    average = lax.fori_loop(0, count // 2, steps, face_average(prim, aux, 0, s, comps, first))
    if count % 2:
        step(count - 1, average)


def prepare_kernel(nx, ny, nz, rho, vel, p, q_ref, top_ref, sems):
    n = nx * ny
    sources = (rho, vel.at[0], vel.at[1], vel.at[2], p)
    copies = [
        pltpu.make_async_copy(src, q_ref.at[k, pl.ds(0, n), :], sems.at[k])
        for k, src in enumerate(sources)
    ]
    for copy in copies:
        copy.start()
    for copy in copies:
        copy.wait()
    top = None
    for i in range(n // 8):
        here = slice(8 * i, 8 * i + 8)
        sound = jnp.sqrt(gamma_gas * q_ref[4, here, :] / q_ref[0, here, :])
        speed = (jnp.abs(q_ref[1, here, :]) + jnp.abs(q_ref[2, here, :])) + (
            jnp.abs(q_ref[3, here, :]) + 3.0 * sound
        )
        top = speed if top is None else jnp.maximum(top, speed)
    top = jnp.broadcast_to(jnp.max(top, keepdims=True), (8, nz))
    top_ref[...] = top


def edge_starts(nx, ny, xeven):
    high = (nx - 3) * ny
    if not xeven:
        return high, 0
    odd = lax.rem(lax.axis_index("gx"), 2)
    return pl.multiple_of((1 - odd) * high, 8), pl.multiple_of(odd * high, 8)


def slots(axis):
    n = lax.axis_size(axis)
    if n % 2 or n < 4:
        return 0, 1
    odd = lax.rem(lax.axis_index(axis), 2)
    return 1 - odd, odd


def turn_kernel(nx, ny, nz, xeven, q_ref, after, qt_ref, xa_ref, xb_ref, y_ref, z_ref, free_ref):
    n = nx * ny
    for k in range(5):
        qt_ref[k, 0:nz, :] = q_ref[k, 0:n, :].T
    size = y_ref.shape[1]
    for slot, side in zip(slots("gy"), (0, 1)):
        y_ref[slot, size - 8 :, :] = jnp.zeros((8, nz), f32)
        for k in range(5):
            for e in range(3):
                at = (3 * k + e) * nx
                row = e + side * (ny - 3)
                y_ref[slot, at : at + nx, :] = q_ref[k, pl.ds(row, nx, stride=ny), :]
    width = 3 * ny
    start_a, start_b = edge_starts(nx, ny, xeven)
    for k in range(5):
        xa_ref[k * width : (k + 1) * width, :] = q_ref[k, pl.ds(start_a, width), :]
        xb_ref[k * width : (k + 1) * width, :] = q_ref[k, pl.ds(start_b, width), :]
    for slot, at in zip(slots("gz"), (0, nz - 3)):
        z_ref[slot, 8:16, :] = jnp.zeros((8, n), f32)
        for k in range(5):
            z_ref[slot, 3 * k : 3 * k + 3, :] = qt_ref[k, at : at + 3, :]
    row = lax.broadcasted_iota(jnp.int32, free_ref.shape, 0)
    free_ref[...] = jnp.where(row == 7, 1.0, 0.0).astype(f32)


def x_kernel(nx, ny, first, ys, xeven, q_ref, a_ref, b_ref, after, out_ref, prim, uf, aux, cx, flux):
    far = (nx + 3) * ys
    if xeven:
        odd = lax.rem(lax.axis_index("gx"), 2)
        at_a = pl.multiple_of((1 - odd) * far, 8)
        at_b = pl.multiple_of(odd * far, 8)
    else:
        at_a, at_b = 0, far
    for k in range(5):
        for e in range(3):
            row = (3 * k + e) * ny + first
            prim[k, pl.ds(pl.multiple_of(at_a + e * ys, 8), ys), :] = a_ref[row : row + ys, :]
            prim[k, pl.ds(pl.multiple_of(at_b + e * ys, 8), ys), :] = b_ref[row : row + ys, :]
        for x in range(nx):
            row = x * ny + first
            prim[k, (3 + x) * ys : (4 + x) * ys, :] = q_ref[k, row : row + ys, :]
    t = ys // 8
    comps = (0, 1, 2)
    cell_pass(prim, uf, aux, (nx + 6) * t, comps)
    diff_pass(uf, aux, cx, (nx + 4) * t, (nx + 5) * t, ys)

    def put(k, i, value):
        flux[k, rows(i), :] = value

    face_pass(prim, aux, cx, (nx + 1) * t, ys, comps, put)
    n = nx * ys
    for k in range(5):
        out_ref[k] = flux[k, ys : ys + n, :] - flux[k, 0:n, :]


def inner_kernel(first, count, more, length, block, comps, q_ref, after, out_ref, uf, aux, cx):
    cell_pass(q_ref, uf, aux, count + more, comps, first)
    diff_pass(uf, aux, cx, count + more, count + more, 1)
    tiles = length // 8

    def put(k, i, value):
        if block:
            i = lax.div(i, tiles) * (block // 8) + lax.rem(i, tiles)
        out_ref[k, rows(i, 3), :] = value

    face_pass(q_ref, aux, cx, count, 1, comps, put, first)


def z_ends_kernel(nz, qt_ref, lo, hi, fz_ref, fz2_ref, after, out_ref, prim, uf, aux, cx, flux, fz):
    for k in range(5):
        prim[k] = jnp.ones(prim.shape[1:], f32)
        for j in range(6):
            if j < 3:
                prim[k, 8 * j : 8 * j + 3 - j, :] = lo[3 * k + j : 3 * k + 3, :]
            if j > 0:
                prim[k, 8 * j + max(3 - j, 0) : 8 * j + 3, :] = qt_ref[k, max(j - 3, 0) : j, :]
            if j < 5:
                prim[k, 8 * j + 3 : 8 * j + 3 + min(5 - j, 3), :] = qt_ref[k, nz - 5 + j : nz - 5 + j + min(5 - j, 3), :]
            if j > 2:
                prim[k, 8 * j + 8 - j : 8 * j + 6, :] = hi[3 * k : 3 * k + j - 2, :]

    def put(k, i, value):
        flux[k, rows(i), :] = value

    comps = (2, 0, 1)
    cell_pass(prim, uf, aux, 6, comps)
    diff_pass(uf, aux, cx, 4, 5, 8)
    face_pass(prim, aux, cx, 1, 8, comps, put)
    a = fz_ref.shape[1] - 8
    b = a + fz2_ref.shape[1] - 8
    count = (nz - b) // 8

    def put_inner(k, i, value):
        fz[k, rows(i + b // 8, 3), :] = value

    cell_pass(qt_ref, uf, aux, count, comps, b // 8)
    diff_pass(uf, aux, cx, count, count, 1)
    face_pass(qt_ref, aux, cx, count, 1, comps, put_inner, b // 8)
    for k in range(5):
        fz[k, 3 : a + 3, :] = fz_ref[k, 3 : a + 3, :]
        fz[k, a + 3 : b + 3, :] = fz2_ref[k, 3 : b - a + 3, :]
        fz[k, 0:3, :] = flux[k, 0:3, :]
        fz[k, nz - 2 : nz + 1, :] = flux[k, 3:6, :]
        out_ref[k] = (fz[k, 1 : nz + 1, :] - fz[k, 0:nz, :]).T


def y_ends_kernel(nx, ny, block, q_ref, lo, hi, fy_ref, tz_ref, after, out_ref, prim, uf, aux, cx, flux, fy):
    sb = rup(2 * nx, 8)
    for k in range(5):
        for e in range(8):
            if e < 3:
                low = lo[(3 * k + e) * nx : (3 * k + e + 1) * nx, :]
            else:
                low = q_ref[k, pl.ds(e - 3, nx, stride=ny), :]
            if e < 5:
                high = q_ref[k, pl.ds(ny - 5 + e, nx, stride=ny), :]
            else:
                high = hi[(3 * k + e - 5) * nx : (3 * k + e - 4) * nx, :]
            prim[k, e * sb : e * sb + nx, :] = low
            prim[k, e * sb + nx : e * sb + 2 * nx, :] = high
    t = sb // 8
    comps = (1, 0, 2)
    cell_pass(prim, uf, aux, 8 * t, comps)
    diff_pass(uf, aux, cx, 6 * t, 7 * t, sb)

    def put(k, i, value):
        flux[k, rows(i), :] = value

    face_pass(prim, aux, cx, 3 * t, sb, comps, put)
    for k in range(5):
        fy[k, 0 : nx * block, :] = fy_ref[k, 0 : nx * block, :]
        for f in range(3):
            fy[k, pl.ds(f, nx, stride=block), :] = flux[k, f * sb : f * sb + nx, :]
            fy[k, pl.ds(ny - 2 + f, nx, stride=block), :] = flux[k, f * sb + nx : f * sb + 2 * nx, :]
        for x in range(nx):
            at = x * block
            here = slice(x * ny, (x + 1) * ny)
            out_ref[k, here, :] = tz_ref[k, here, :] + (fy[k, at + 1 : at + 1 + ny, :] - fy[k, at : at + ny, :])


def final_kernel(nx, ny, split, q_ref, tx_ref, rest_ref, t_ref, top_ref, out_ref, held, sems):
    step = (cfl_number * KB) / top_ref[7:8, :]
    copies = []
    for x in range(nx):
        for lo, hi, part in ((0, split, tx_ref), (split, ny, rest_ref)):
            here = slice(x * ny + lo, x * ny + hi)
            there = slice(x * (hi - lo), (x + 1) * (hi - lo))
            rho, u1, u2, u3, p = (q_ref[k, here, :] for k in range(5))
            m1, m2, m3 = rho * u1, rho * u2, rho * u3
            energy = 2.5 * p + 0.5 * (m1 * u1 + m2 * u2 + m3 * u3)
            for k, value in enumerate((rho, m1, m2, m3, energy)):
                held[k, x, lo:hi] = value - step * (part[k, there, :] + t_ref[k, here, :])
        copies.append(pltpu.make_async_copy(held.at[:, x], out_ref.at[:, x], sems.at[x]))
        copies[-1].start()
    for copy in copies:
        copy.wait()


VMEM = pl.BlockSpec(memory_space=pltpu.VMEM)
HBM = pl.BlockSpec(memory_space=pltpu.HBM)
ANY = pl.BlockSpec(memory_space=pl.ANY)


def call(kernel, outs, flops, scratch=(), in_specs=None, out_specs=None):
    extra = {} if in_specs is None else {"in_specs": in_specs}
    if out_specs is not None:
        extra["out_specs"] = out_specs
    return pl.pallas_call(
        kernel,
        out_shape=outs,
        scratch_shapes=scratch,
        compiler_params=pltpu.CompilerParams(vmem_limit_bytes=VMEM_LIMIT),
        cost_estimate=pl.CostEstimate(flops=flops, bytes_accessed=1000000, transcendentals=0),
        **extra,
    )


def permute(value, axis, pairs):
    return lax.ppermute(value, axis, pairs)


def fields(*counts, r, w):
    return [pltpu.VMEM((count, r, w), f32) for count in counts]


def pairs_a(n):
    return [(i, i ^ 1) for i in range(n)]


def pairs_b(n):
    return [(i, (i + 1) % n if i % 2 else (i - 1) % n) for i in range(n)]


def top_over(top, axis, first):
    n = lax.axis_size(axis)
    if n & (n - 1):
        return lax.pmax(top, axis)
    d = first
    while d < n:
        top = jnp.maximum(top, permute(top, axis, [(i, i ^ (d | (first > 1))) for i in range(n)]))
        d *= 2
    return top


def with_top(edges, free, top):
    at = edges.shape[0] - 8
    return jnp.concatenate([edges[:at], edges[at:] + free * top])


def got_top(top, got):
    return jnp.maximum(top, got[got.shape[0] - 8 :])


def edge_trade(axis, edges, free, top, mids=None):
    n = lax.axis_size(axis)
    first, second = edges[0], edges[1]
    size = first.shape[0]
    if n == 1:
        return second, first, top
    if n == 2:
        got = permute(with_top(edges.reshape(2 * size, -1), free, top), axis, [(0, 1), (1, 0)])
        return got[size:], got[:size], got_top(top, got)
    if n % 2:
        lower = permute(second, axis, [(i, (i + 1) % n) for i in range(n)])
        upper = permute(first, axis, [((i + 1) % n, i) for i in range(n)])
        return lower, upper, lax.pmax(top, axis)
    odd = lax.rem(lax.axis_index(axis), 2) == 1
    got_a = permute(with_top(first, free, top), axis, pairs_a(n))
    top = got_top(top, got_a)
    if mids is not None:
        mids.append(top)
    got_b = permute(with_top(second, free, top), axis, pairs_b(n))
    if n == 4:
        top = got_top(top, got_b)
    else:
        top = top_over(top, axis, 2)
    lower = jnp.where(odd, got_a, got_b)
    upper = jnp.where(odd, got_b, got_a)
    return lower, upper, top


def local(density, velocity, pressure):
    nx, ny, nz = density.shape
    n = nx * ny
    gx = lax.axis_size("gx")
    xeven = gx % 2 == 0
    width = 15 * ny
    S = jax.ShapeDtypeStruct
    density, velocity, pressure = (
        pltpu.with_memory_space_constraint(a, pltpu.HBM)
        for a in (density.reshape(n, nz), velocity.reshape(3, n, nz), pressure.reshape(n, nz))
    )
    q, top = call(
        functools.partial(prepare_kernel, nx, ny, nz),
        (S((5, n + 16, nz), f32), S((8, nz), f32)),
        2000000,
        [pltpu.SemaphoreType.DMA((5,))],
        [HBM] * 3,
    )(density, velocity, pressure)
    qt, xa, xb, ye, ze, free = call(
        functools.partial(turn_kernel, nx, ny, nz, xeven),
        (
            S((5, nz + 16, n), f32),
            S((width, nz), f32),
            S((width, nz), f32),
            S((2, rup(15 * nx + 1, 8), nz), f32),
            S((2, 16, n), f32),
            S((8, nz), f32),
        ),
        2000000,
        (),
        [VMEM, ANY],
    )(q, top)

    sweep_flops = 16000000

    def inner(source, first, count, more, lanes, length, block, comps, rows_out, after):
        return call(
            functools.partial(inner_kernel, first, count, more, length, block, comps),
            S((5, rows_out, lanes), f32),
            sweep_flops,
            fields(10, 4, 25, r=8 * (count + more) + 16, w=lanes),
            [VMEM, ANY],
        )(source, after)

    if xeven:
        got_b = permute(xb, "gx", pairs_b(gx))
        got_a = permute(xa, "gx", pairs_a(gx))
        top = jnp.maximum(top, permute(top, "gx", pairs_a(gx)))
    else:
        got_a = permute(xa, "gx", [(i, (i + 1) % gx) for i in range(gx)])
        got_b = permute(xb, "gx", [((i + 1) % gx, i) for i in range(gx)])
    ztop = top if n == nz else jnp.full((8, n), jnp.max(top[7]))
    zt = nz // 8
    za, zb = zt * 7 // 16, zt * 4 // 16
    fz = [
        inner(qt, 0, za, 1, n, nz, 0, (2, 0, 1), 8 * za + 8, ye),
        inner(qt, za, zb, 1, n, nz, 0, (2, 0, 1), 8 * zb + 8, ztop),
    ]
    zlo, zhi, ztop = edge_trade("gz", ze, free if n == nz else jnp.broadcast_to(free[:, :1], (8, n)), ztop)
    top = ztop if n == nz else jnp.full((8, nz), jnp.max(ztop[7]))
    block = rup(ny + 6, 8)
    fy = inner(q, 0, n // 8, 0, nz, ny, block, (1, 0, 2), nx * block + 16, top)
    mids = []
    ylo, yhi, top = edge_trade("gy", ye, free, top, mids)

    def along_x(first, ys, after):
        return call(
            functools.partial(x_kernel, nx, ny, first, ys, xeven),
            S((5, nx * ys, nz), f32),
            sweep_flops,
            fields(5, 10, 4, 25, 5, r=(nx + 6) * ys + 16, w=nz),
            [VMEM] * 3 + [ANY],
        )(q, got_a, got_b, after)

    split = rup(ny // 4, 8)
    tx = along_x(0, split, mids[0] if mids else top)
    tx_rest = along_x(split, ny - split, top)
    tz = call(
        functools.partial(z_ends_kernel, nz),
        S((5, n, nz), f32),
        sweep_flops // 4,
        fields(5, 10, 4, 25, 5, r=64, w=n) + [pltpu.VMEM((5, nz + 16, n), f32)],
        [VMEM] * 5 + [ANY],
    )(qt, zlo, zhi, *fz, mids[0] if mids else top)
    t = call(
        functools.partial(y_ends_kernel, nx, ny, block),
        S((5, n, nz), f32),
        sweep_flops // 4,
        fields(5, 10, 4, 25, 5, r=8 * rup(2 * nx, 8) + 16, w=nz) + [pltpu.VMEM((5, nx * block + 16, nz), f32)],
        [VMEM] * 5 + [ANY],
    )(q, ylo, yhi, fy, tz, top)
    top = top_over(top, "gx", 2 if xeven else 1)
    out = S((5, nx, ny, nz), f32)
    return call(
        functools.partial(final_kernel, nx, ny, split),
        out,
        1000000,
        [pltpu.VMEM(out.shape, f32), pltpu.SemaphoreType.DMA((nx,))],
        [VMEM] * 5,
        HBM,
    )(q, tx, tx_rest, t, top)


def solution(mesh):
    in_specs = (P("gx", "gy", "gz"), P(None, "gx", "gy", "gz"), P("gx", "gy", "gz"))
    out_specs = P(None, "gx", "gy", "gz")

    return jax.shard_map(local, mesh=mesh, in_specs=in_specs, out_specs=out_specs, check_vma=False)
```

```python
import functools
import math

import jax
import jax.numpy as jnp
from jax import lax
from jax.experimental import pallas as pl
from jax.experimental.pallas import tpu as pltpu
from jax.sharding import PartitionSpec as P


gamma_gas = 1.4
weno_eps = 1e-06
cfl_number = 0.4
f32 = jnp.float32

KX = math.sqrt(13.0 / 12.0)
KT = 0.5 / KX
KB = 1.0 / (6.0 * KX)
VMEM_LIMIT = 24 * 1024 * 1024


def rup(n, m):
    return (n + m - 1) // m * m


def rows(i, offset=0):
    return pl.ds(pl.multiple_of(i * 8, 8) + offset, 8)


def over(count, unroll, body):
    whole = count // unroll
    if whole:

        @pl.loop(0, whole)
        def _(j):
            for u in range(unroll):
                body(j * unroll + u)

    for i in range(whole * unroll, count):
        body(i)


def cell_pass(prim, uf, aux, count, comps, first=0):
    def body(i):
        here, there = rows(i), rows(i + first)
        rho, p = prim[0, there, :], prim[4, there, :]
        un, ut, us = (prim[1 + c, there, :] for c in comps)
        inv = 1.0 / rho
        mn, mt, ms = rho * un, rho * ut, rho * us
        mnun = mn * un
        energy = 2.5 * p + 0.5 * (mnun + mt * ut + ms * us)
        total = energy + p
        values = (rho, mn, mt, ms, energy, mn, mnun + p, mt * un, ms * un, total * un)
        for m in range(10):
            uf[m, here, :] = values[m]
        aux[0, here, :] = total * inv
        aux[1, here, :] = jnp.sqrt(rho)
        aux[3, here, :] = jnp.abs(un) + jnp.sqrt(gamma_gas * p * inv)

    over(count, 4, body)


def diff_pass(uf, aux, cx, count, pairs, s):
    def body(i):
        here = rows(i)
        for m in range(10):
            a, b, c = uf[m, here, :], uf[m, rows(i, s), :], uf[m, rows(i, 2 * s), :]
            second = (0.5 * (a + c) - b) * KX
            cx[m, here, :] = 0.25 * (c - a)
            cx[10 + m, here, :] = second
            if m >= 5:
                cx[15 + m, here, :] = (0.5 / KB) * b - (1.0 / (6.0 * KB * KX)) * second

    def pair(i):
        aux[2, rows(i), :] = jnp.maximum(aux[3, rows(i), :], aux[3, rows(i, s), :])

    over(count, 4, body)
    over(pairs, 8, pair)


def weno_excess(mid, xa, xb, xc, sign, eps):
    tau_a = xa - xb
    tau_c = xb - xc
    if sign > 0:
        mid_a = mid + KT * tau_a
        mid_c = mid + KT * tau_c
    else:
        mid_a = mid - KT * tau_a
        mid_c = mid - KT * tau_c
    sm_a = mid_a * mid_a + (xa * xa + eps)
    sm_b = mid * mid + (xb * xb + eps)
    sm_c = mid_c * mid_c + (xc * xc + eps)
    ga = 3.0 * (sm_a * sm_a)
    gb = sm_b * sm_b
    gc = sm_c * sm_c
    gc = gc + gc
    num = gb * (tau_a * gc + tau_c * ga)
    den = gb * gc + (ga + ga) * (gb + gc)
    return num / den


def characteristic(v, un, ut, us, qh, b1, ic):
    t = (qh * v[0] - un * v[1]) - (ut * v[2] + us * v[3]) + v[4]
    a = b1 * t
    n = (un * v[0] - v[1]) * ic
    return (a + n, v[0] - a, v[2] - ut * v[0], v[3] - us * v[0], a - n)


def face_average(prim, aux, i, s, comps, first):
    def at(ref, k, o):
        return ref[k, rows(i if ref is aux else i + first, o * s), :]

    rl, rr = at(aux, 1, 2), at(aux, 1, 3)
    share = rr / (rl + rr)

    def roe(ref, k):
        left, right = at(ref, k, 2), at(ref, k, 3)
        return left + share * (right - left)

    un, ut, us = (roe(prim, 1 + c) for c in comps)
    enth = roe(aux, 0)
    qh = 0.5 * (un * un + ut * ut + us * us)
    c2 = (gamma_gas - 1.0) * (enth - qh)
    ic = lax.rsqrt(c2)
    b1 = (gamma_gas - 1.0) * (ic * ic)
    alpha = jnp.maximum(jnp.maximum(at(aux, 2, 0), at(aux, 2, 2)), at(aux, 2, 4))
    return un, ut, us, enth, qh, c2 * ic, ic, b1, alpha


def face_values(get_cx, average):
    un, ut, us, enth, qh, c, ic, b1, alpha = average
    args = (un, ut, us, qh, b1, ic)
    mid_p = characteristic([get_cx(5 + m, 2) + alpha * get_cx(m, 2) for m in range(5)], *args)
    mid_m = characteristic([get_cx(5 + m, 3) - alpha * get_cx(m, 3) for m in range(5)], *args)
    xu = {o: [alpha * get_cx(10 + m, o) for m in range(5)] for o in range(1, 5)}
    xp = {}
    xm = {}
    for o in (1, 2, 3, 4):
        xf = [get_cx(15 + m, o) for m in range(5)]
        if o <= 3:
            xp[o] = characteristic([xf[m] + xu[o][m] for m in range(5)], *args)
        if o >= 2:
            xm[o] = characteristic([xf[m] - xu[o][m] for m in range(5)], *args)
    g = []
    for m in range(5):
        eps = 4.0 * weno_eps if m in (0, 4) else weno_eps
        up = weno_excess(mid_p[m], xp[1][m], xp[2][m], xp[3][m], 1, eps)
        down = weno_excess(mid_m[m], xm[4][m], xm[3][m], xm[2][m], -1, eps)
        g.append(up + down)
    h2, h3, h4 = (g[m] + g[m] for m in (1, 2, 3))
    h15 = g[0] + g[4]
    dh = c * (g[4] - g[0])
    rr = h15 + h2
    upd = (
        rr,
        un * rr + dh,
        ut * rr + h3,
        us * rr + h4,
        enth * h15 + un * dh + qh * h2 + ut * h3 + us * h4,
    )
    return [
        (get_cx(20 + m, 2) + get_cx(20 + m, 3)) + (xu[3][m] - xu[2][m]) + upd[m] for m in range(5)
    ]


def face_pass(prim, aux, cx, count, s, comps, put, first=0):
    order = (0, 1 + comps[0], 1 + comps[1], 1 + comps[2], 4)

    def step(i, average):
        ahead = face_average(prim, aux, i + 1, s, comps, first)
        values = face_values(lambda k, o: cx[k, rows(i, (o - 1) * s), :], average)
        for m in range(5):
            put(order[m], i, values[m])
        return ahead

    def steps(j, average):
        for u in range(2):
            average = step(2 * j + u, average)
        return average

    average = lax.fori_loop(0, count // 2, steps, face_average(prim, aux, 0, s, comps, first))
    if count % 2:
        step(count - 1, average)


def prepare_kernel(nx, ny, nz, rho, vel, p, q_ref, top_ref, sems):
    n = nx * ny
    sources = (rho, vel.at[0], vel.at[1], vel.at[2], p)
    copies = [
        pltpu.make_async_copy(src, q_ref.at[k, pl.ds(0, n), :], sems.at[k])
        for k, src in enumerate(sources)
    ]
    for copy in copies:
        copy.start()
    for copy in copies:
        copy.wait()
    top = None
    for i in range(n // 8):
        here = slice(8 * i, 8 * i + 8)
        sound = jnp.sqrt(gamma_gas * q_ref[4, here, :] / q_ref[0, here, :])
        speed = (jnp.abs(q_ref[1, here, :]) + jnp.abs(q_ref[2, here, :])) + (
            jnp.abs(q_ref[3, here, :]) + 3.0 * sound
        )
        top = speed if top is None else jnp.maximum(top, speed)
    top = jnp.broadcast_to(jnp.max(top, keepdims=True), (8, nz))
    top_ref[...] = top


def edge_starts(nx, ny, xeven):
    high = (nx - 3) * ny
    if not xeven:
        return high, 0
    odd = lax.rem(lax.axis_index("gx"), 2)
    return pl.multiple_of((1 - odd) * high, 8), pl.multiple_of(odd * high, 8)


def slots(axis):
    n = lax.axis_size(axis)
    if n % 2 or n < 4:
        return 0, 1
    odd = lax.rem(lax.axis_index(axis), 2)
    return 1 - odd, odd


def turn_kernel(nx, ny, nz, xeven, q_ref, after, qt_ref, xa_ref, xb_ref, y_ref, z_ref, free_ref):
    n = nx * ny
    for k in range(5):
        qt_ref[k, 0:nz, :] = q_ref[k, 0:n, :].T
    size = y_ref.shape[1]
    for slot, side in zip(slots("gy"), (0, 1)):
        y_ref[slot, size - 8 :, :] = jnp.zeros((8, nz), f32)
        for k in range(5):
            for e in range(3):
                at = (3 * k + e) * nx
                row = e + side * (ny - 3)
                y_ref[slot, at : at + nx, :] = q_ref[k, pl.ds(row, nx, stride=ny), :]
    width = 3 * ny
    start_a, start_b = edge_starts(nx, ny, xeven)
    for k in range(5):
        xa_ref[k * width : (k + 1) * width, :] = q_ref[k, pl.ds(start_a, width), :]
        xb_ref[k * width : (k + 1) * width, :] = q_ref[k, pl.ds(start_b, width), :]
    for slot, at in zip(slots("gz"), (0, nz - 3)):
        z_ref[slot, 8:16, :] = jnp.zeros((8, n), f32)
        for k in range(5):
            z_ref[slot, 3 * k : 3 * k + 3, :] = qt_ref[k, at : at + 3, :]
    row = lax.broadcasted_iota(jnp.int32, free_ref.shape, 0)
    free_ref[...] = jnp.where(row == 7, 1.0, 0.0).astype(f32)


def x_kernel(nx, ny, first, ys, xeven, q_ref, a_ref, b_ref, after, out_ref, prim, uf, aux, cx, flux):
    far = (nx + 3) * ys
    if xeven:
        odd = lax.rem(lax.axis_index("gx"), 2)
        at_a = pl.multiple_of((1 - odd) * far, 8)
        at_b = pl.multiple_of(odd * far, 8)
    else:
        at_a, at_b = 0, far
    for k in range(5):
        for e in range(3):
            row = (3 * k + e) * ny + first
            prim[k, pl.ds(pl.multiple_of(at_a + e * ys, 8), ys), :] = a_ref[row : row + ys, :]
            prim[k, pl.ds(pl.multiple_of(at_b + e * ys, 8), ys), :] = b_ref[row : row + ys, :]
        for x in range(nx):
            row = x * ny + first
            prim[k, (3 + x) * ys : (4 + x) * ys, :] = q_ref[k, row : row + ys, :]
    t = ys // 8
    comps = (0, 1, 2)
    cell_pass(prim, uf, aux, (nx + 6) * t, comps)
    diff_pass(uf, aux, cx, (nx + 4) * t, (nx + 5) * t, ys)

    def put(k, i, value):
        flux[k, rows(i), :] = value

    face_pass(prim, aux, cx, (nx + 1) * t, ys, comps, put)
    n = nx * ys
    for k in range(5):
        out_ref[k] = flux[k, ys : ys + n, :] - flux[k, 0:n, :]


def inner_kernel(first, count, more, length, block, comps, q_ref, after, out_ref, uf, aux, cx):
    cell_pass(q_ref, uf, aux, count + more, comps, first)
    diff_pass(uf, aux, cx, count + more, count + more, 1)
    tiles = length // 8

    def put(k, i, value):
        if block:
            i = lax.div(i, tiles) * (block // 8) + lax.rem(i, tiles)
        out_ref[k, rows(i, 3), :] = value

    face_pass(q_ref, aux, cx, count, 1, comps, put, first)


def z_ends_kernel(nz, qt_ref, lo, hi, fz_ref, fz2_ref, after, out_ref, prim, uf, aux, cx, flux, fz):
    for k in range(5):
        prim[k] = jnp.ones(prim.shape[1:], f32)
        for j in range(6):
            if j < 3:
                prim[k, 8 * j : 8 * j + 3 - j, :] = lo[3 * k + j : 3 * k + 3, :]
            if j > 0:
                prim[k, 8 * j + max(3 - j, 0) : 8 * j + 3, :] = qt_ref[k, max(j - 3, 0) : j, :]
            if j < 5:
                prim[k, 8 * j + 3 : 8 * j + 3 + min(5 - j, 3), :] = qt_ref[k, nz - 5 + j : nz - 5 + j + min(5 - j, 3), :]
            if j > 2:
                prim[k, 8 * j + 8 - j : 8 * j + 6, :] = hi[3 * k : 3 * k + j - 2, :]

    def put(k, i, value):
        flux[k, rows(i), :] = value

    comps = (2, 0, 1)
    cell_pass(prim, uf, aux, 6, comps)
    diff_pass(uf, aux, cx, 4, 5, 8)
    face_pass(prim, aux, cx, 1, 8, comps, put)
    a = fz_ref.shape[1] - 8
    b = a + fz2_ref.shape[1] - 8
    count = (nz - b) // 8

    def put_inner(k, i, value):
        fz[k, rows(i + b // 8, 3), :] = value

    cell_pass(qt_ref, uf, aux, count, comps, b // 8)
    diff_pass(uf, aux, cx, count, count, 1)
    face_pass(qt_ref, aux, cx, count, 1, comps, put_inner, b // 8)
    for k in range(5):
        fz[k, 3 : a + 3, :] = fz_ref[k, 3 : a + 3, :]
        fz[k, a + 3 : b + 3, :] = fz2_ref[k, 3 : b - a + 3, :]
        fz[k, 0:3, :] = flux[k, 0:3, :]
        fz[k, nz - 2 : nz + 1, :] = flux[k, 3:6, :]
        out_ref[k] = (fz[k, 1 : nz + 1, :] - fz[k, 0:nz, :]).T


def y_ends_kernel(nx, ny, block, q_ref, lo, hi, fy_ref, tz_ref, after, out_ref, prim, uf, aux, cx, flux, fy):
    sb = rup(2 * nx, 8)
    for k in range(5):
        for e in range(8):
            if e < 3:
                low = lo[(3 * k + e) * nx : (3 * k + e + 1) * nx, :]
            else:
                low = q_ref[k, pl.ds(e - 3, nx, stride=ny), :]
            if e < 5:
                high = q_ref[k, pl.ds(ny - 5 + e, nx, stride=ny), :]
            else:
                high = hi[(3 * k + e - 5) * nx : (3 * k + e - 4) * nx, :]
            prim[k, e * sb : e * sb + nx, :] = low
            prim[k, e * sb + nx : e * sb + 2 * nx, :] = high
    t = sb // 8
    comps = (1, 0, 2)
    cell_pass(prim, uf, aux, 8 * t, comps)
    diff_pass(uf, aux, cx, 6 * t, 7 * t, sb)

    def put(k, i, value):
        flux[k, rows(i), :] = value

    face_pass(prim, aux, cx, 3 * t, sb, comps, put)
    for k in range(5):
        fy[k, 0 : nx * block, :] = fy_ref[k, 0 : nx * block, :]
        for f in range(3):
            fy[k, pl.ds(f, nx, stride=block), :] = flux[k, f * sb : f * sb + nx, :]
            fy[k, pl.ds(ny - 2 + f, nx, stride=block), :] = flux[k, f * sb + nx : f * sb + 2 * nx, :]
        for x in range(nx):
            at = x * block
            here = slice(x * ny, (x + 1) * ny)
            out_ref[k, here, :] = tz_ref[k, here, :] + (fy[k, at + 1 : at + 1 + ny, :] - fy[k, at : at + ny, :])


def final_kernel(nx, ny, split, q_ref, tx_ref, rest_ref, t_ref, top_ref, out_ref, held, sems):
    step = (cfl_number * KB) / top_ref[7:8, :]
    copies = []
    for x in range(nx):
        for lo, hi, part in ((0, split, tx_ref), (split, ny, rest_ref)):
            here = slice(x * ny + lo, x * ny + hi)
            there = slice(x * (hi - lo), (x + 1) * (hi - lo))
            rho, u1, u2, u3, p = (q_ref[k, here, :] for k in range(5))
            m1, m2, m3 = rho * u1, rho * u2, rho * u3
            energy = 2.5 * p + 0.5 * (m1 * u1 + m2 * u2 + m3 * u3)
            for k, value in enumerate((rho, m1, m2, m3, energy)):
                held[k, x, lo:hi] = value - step * (part[k, there, :] + t_ref[k, here, :])
        copies.append(pltpu.make_async_copy(held.at[:, x], out_ref.at[:, x], sems.at[x]))
        copies[-1].start()
    for copy in copies:
        copy.wait()


VMEM = pl.BlockSpec(memory_space=pltpu.VMEM)
HBM = pl.BlockSpec(memory_space=pltpu.HBM)
ANY = pl.BlockSpec(memory_space=pl.ANY)


def call(kernel, outs, flops, scratch=(), in_specs=None, out_specs=None):
    extra = {} if in_specs is None else {"in_specs": in_specs}
    if out_specs is not None:
        extra["out_specs"] = out_specs
    return pl.pallas_call(
        kernel,
        out_shape=outs,
        scratch_shapes=scratch,
        compiler_params=pltpu.CompilerParams(vmem_limit_bytes=VMEM_LIMIT),
        cost_estimate=pl.CostEstimate(flops=flops, bytes_accessed=1000000, transcendentals=0),
        **extra,
    )


def permute(value, axis, pairs):
    return lax.ppermute(value, axis, pairs)


def fields(*counts, r, w):
    return [pltpu.VMEM((count, r, w), f32) for count in counts]


def pairs_a(n):
    return [(i, i ^ 1) for i in range(n)]


def pairs_b(n):
    return [(i, (i + 1) % n if i % 2 else (i - 1) % n) for i in range(n)]


def top_over(top, axis, first):
    n = lax.axis_size(axis)
    if n & (n - 1):
        return lax.pmax(top, axis)
    d = first
    while d < n:
        top = jnp.maximum(top, permute(top, axis, [(i, i ^ (d | (first > 1))) for i in range(n)]))
        d *= 2
    return top


def with_top(edges, free, top):
    at = edges.shape[0] - 8
    return jnp.concatenate([edges[:at], edges[at:] + free * top])


def got_top(top, got):
    return jnp.maximum(top, got[got.shape[0] - 8 :])


def edge_trade(axis, edges, free, top, mids=None):
    n = lax.axis_size(axis)
    first, second = edges[0], edges[1]
    size = first.shape[0]
    if n == 1:
        return second, first, top
    if n == 2:
        got = permute(with_top(edges.reshape(2 * size, -1), free, top), axis, [(0, 1), (1, 0)])
        return got[size:], got[:size], got_top(top, got)
    if n % 2:
        lower = permute(second, axis, [(i, (i + 1) % n) for i in range(n)])
        upper = permute(first, axis, [((i + 1) % n, i) for i in range(n)])
        return lower, upper, lax.pmax(top, axis)
    odd = lax.rem(lax.axis_index(axis), 2) == 1
    got_a = permute(with_top(first, free, top), axis, pairs_a(n))
    top = got_top(top, got_a)
    if mids is not None:
        mids.append(top)
    got_b = permute(with_top(second, free, top), axis, pairs_b(n))
    if n == 4:
        top = got_top(top, got_b)
    else:
        top = top_over(top, axis, 2)
    lower = jnp.where(odd, got_a, got_b)
    upper = jnp.where(odd, got_b, got_a)
    return lower, upper, top


def local(density, velocity, pressure):
    nx, ny, nz = density.shape
    n = nx * ny
    gx = lax.axis_size("gx")
    xeven = gx % 2 == 0
    width = 15 * ny
    S = jax.ShapeDtypeStruct
    density, velocity, pressure = (
        pltpu.with_memory_space_constraint(a, pltpu.HBM)
        for a in (density.reshape(n, nz), velocity.reshape(3, n, nz), pressure.reshape(n, nz))
    )
    q, top = call(
        functools.partial(prepare_kernel, nx, ny, nz),
        (S((5, n + 16, nz), f32), S((8, nz), f32)),
        2000000,
        [pltpu.SemaphoreType.DMA((5,))],
        [HBM] * 3,
    )(density, velocity, pressure)
    qt, xa, xb, ye, ze, free = call(
        functools.partial(turn_kernel, nx, ny, nz, xeven),
        (
            S((5, nz + 16, n), f32),
            S((width, nz), f32),
            S((width, nz), f32),
            S((2, rup(15 * nx + 1, 8), nz), f32),
            S((2, 16, n), f32),
            S((8, nz), f32),
        ),
        2000000,
        (),
        [VMEM, ANY],
    )(q, top)

    sweep_flops = 16000000

    def inner(source, first, count, more, lanes, length, block, comps, rows_out, after):
        return call(
            functools.partial(inner_kernel, first, count, more, length, block, comps),
            S((5, rows_out, lanes), f32),
            sweep_flops,
            fields(10, 4, 25, r=8 * (count + more) + 16, w=lanes),
            [VMEM, ANY],
        )(source, after)

    if xeven:
        got_b = permute(xb, "gx", pairs_b(gx))
        got_a = permute(xa, "gx", pairs_a(gx))
        top = jnp.maximum(top, permute(top, "gx", pairs_a(gx)))
    else:
        got_a = permute(xa, "gx", [(i, (i + 1) % gx) for i in range(gx)])
        got_b = permute(xb, "gx", [((i + 1) % gx, i) for i in range(gx)])
    ztop = top if n == nz else jnp.full((8, n), jnp.max(top[7]))
    zt = nz // 8
    za, zb = zt * 7 // 16, zt * 7 // 16
    fz = [
        inner(qt, 0, za, 1, n, nz, 0, (2, 0, 1), 8 * za + 8, ye),
        inner(qt, za, zb, 1, n, nz, 0, (2, 0, 1), 8 * zb + 8, ztop),
    ]
    zlo, zhi, ztop = edge_trade("gz", ze, free if n == nz else jnp.broadcast_to(free[:, :1], (8, n)), ztop)
    top = ztop if n == nz else jnp.full((8, nz), jnp.max(ztop[7]))
    block = rup(ny + 6, 8)
    fy = inner(q, 0, n // 8, 0, nz, ny, block, (1, 0, 2), nx * block + 16, top)
    mids = []
    ylo, yhi, top = edge_trade("gy", ye, free, top, mids)

    def along_x(first, ys, after):
        return call(
            functools.partial(x_kernel, nx, ny, first, ys, xeven),
            S((5, nx * ys, nz), f32),
            sweep_flops,
            fields(5, 10, 4, 25, 5, r=(nx + 6) * ys + 16, w=nz),
            [VMEM] * 3 + [ANY],
        )(q, got_a, got_b, after)

    split = rup(ny // 2, 8)
    tx = along_x(0, split, mids[0] if mids else top)
    tx_rest = along_x(split, ny - split, top)
    tz = call(
        functools.partial(z_ends_kernel, nz),
        S((5, n, nz), f32),
        sweep_flops // 4,
        fields(5, 10, 4, 25, 5, r=64, w=n) + [pltpu.VMEM((5, nz + 16, n), f32)],
        [VMEM] * 5 + [ANY],
    )(qt, zlo, zhi, *fz, mids[0] if mids else top)
    t = call(
        functools.partial(y_ends_kernel, nx, ny, block),
        S((5, n, nz), f32),
        sweep_flops // 4,
        fields(5, 10, 4, 25, 5, r=8 * rup(2 * nx, 8) + 16, w=nz) + [pltpu.VMEM((5, nx * block + 16, nz), f32)],
        [VMEM] * 5 + [ANY],
    )(q, ylo, yhi, fy, tz, top)
    top = top_over(top, "gx", 2 if xeven else 1)
    out = S((5, nx, ny, nz), f32)
    return call(
        functools.partial(final_kernel, nx, ny, split),
        out,
        1000000,
        [pltpu.VMEM(out.shape, f32), pltpu.SemaphoreType.DMA((nx,))],
        [VMEM] * 5,
        HBM,
    )(q, tx, tx_rest, t, top)


def solution(mesh):
    in_specs = (P("gx", "gy", "gz"), P(None, "gx", "gy", "gz"), P("gx", "gy", "gz"))
    out_specs = P(None, "gx", "gy", "gz")

    return jax.shard_map(local, mesh=mesh, in_specs=in_specs, out_specs=out_specs, check_vma=False)
```
